32 devices in a mesh: dp: 4 (over z), seq: 4 (over y, x), tensor: 2 (over core).
Axes of the slice: x: 2, y: 2, z: 4, core: 2. Of those that a mesh axis runs over, the one named last changes fastest.
Arguments:
- block_input: float32 [8, 1024, 768], P(('dp', 'tensor'), 'seq'), may hold values from -6 to 6
- segments: int32 [8, 1024], P(('dp', 'tensor')), may hold values from 0 to 7, never falling along the last dimension, each value on 1 to 512 neighbouring positions
- routes: int32 [2, 8, 1024, 2], P(None, 'dp', 'seq'), may hold values from 0 to 3, all different within a row
- distance_bucket: int32 [1024], replicated, may hold values from 0 to 31
- first_gain: bfloat16 [2, 768], P(None, 'dp'), may hold values from 0.5 to 1.5
- query_key_value: bfloat16 [2, 768, 2304], P(None, 'dp'), may hold values from -0.21875 to 0.21875
- attention_out: bfloat16 [2, 768, 768], P(None, 'dp'), may hold values from -0.875 to 0.875
- bias_table: bfloat16 [2, 32, 12], P(None, 'dp'), may hold values from -4 to 4
- second_gain: bfloat16 [2, 768], P(None, 'dp'), may hold values from 0.5 to 1.5
- router_weights: bfloat16 [2, 768, 4], P(None, 'dp'), may hold values from -0.4375 to 0.4375
- expert_up: bfloat16 [2, 4, 768, 3072], P(None, None, 'dp', 'tensor'), may hold values from -0.21875 to 0.21875
- expert_down: bfloat16 [2, 4, 3072, 768], P(None, None, 'tensor', 'dp'), may hold values from -0.109375 to 0.109375
- cotangent: float32 [8, 1024, 768], P(('dp', 'tensor'), 'seq'), may hold values from -6 to 6
Outputs:
- block_output: float32 [8, 1024, 768], P(('dp', 'tensor'), 'seq')
- input_grad: float32 [8, 1024, 768], P(('dp', 'tensor'), 'seq')
- first_gain_grad: float32 [2, 768], P(None, 'dp')
- query_key_value_grad: float32 [2, 768, 2304], P(None, 'dp')
- attention_out_grad: float32 [2, 768, 768], P(None, 'dp')
- bias_table_grad: float32 [2, 32, 12], P(None, 'dp')
- second_gain_grad: float32 [2, 768], P(None, 'dp')
- router_weights_grad: float32 [2, 768, 4], P(None, 'dp')
- expert_up_grad: float32 [2, 4, 768, 3072], P(None, None, 'dp', 'tensor')
- expert_down_grad: float32 [2, 4, 3072, 768], P(None, None, 'tensor', 'dp')
The draws below stay inside these ranges and needn't reach their ends.
Inputs may be any that keep to these rules, and one draw needn't show every extreme that they name: `segments`: within each sequence the numbers never fall; every document holds 1 to 512 positions, one exactly 512. `routes`: each token names 2 different experts.
All inputs are finite; a program needn't handle non-finite values.
Results may differ from the reference program's by a relative error of at most 0.025.
Values may be sent and summed in bfloat16 or wider, within the bound.
A program may use at most 256 MiB of HBM per device.

```python
import math
import jax
import jax.numpy as jnp
import numpy as np
from jax import lax

D = 768
HEADS = 12
HD = 64
FF = 3072
EXPERTS = 4
TOP = 2
BUCKETS = 32
LAYERS = 2
LEN = 1024
SEG = 8
SEQ_DEV = 1
SEQS = 8
PIECE = 256
GROUP = 512
CAP = 256
N_DP = 4
N_SEQ = 4
N_TENSOR = 2


def touch_ends(drawn, rng, smallest, largest):
    shape = drawn.shape
    spot = [jax.random.randint(jax.random.fold_in(rng, axis), (), 0, shape[axis]) for axis in range(len(shape))]
    drawn = drawn.at[tuple(spot)].set(smallest)
    longest = shape.index(max(shape))
    spot[longest] = (spot[longest] + 1) % shape[longest]
    return drawn.at[tuple(spot)].set(largest)


def block_scale(rng, extent, shards, smallest, high):
    def one(dim, shards_of):
        draws = jax.random.uniform(jax.random.fold_in(jax.random.fold_in(rng, 6), dim), (shards_of,), jnp.float32, smallest / len(shards), high / len(shards))
        return jnp.repeat(jnp.exp(draws), extent[dim] // shards_of).reshape((-1,) + (1,) * (len(extent) - dim - 1))

    level = one(*shards[0])
    for cut in shards[1:]:
        level = level * one(*cut)
    return level


def different_ones(rng, rows, number_of, top, lift):
    order = jax.random.permutation(jax.random.fold_in(rng, 1), number_of)
    pull = order
    for power in range(3):
        pull = pull * pull // number_of
    pull = pull * lift // number_of
    lots = jax.random.randint(jax.random.fold_in(rng, 2), (rows, number_of), 0, 4096) + pull
    holders = jax.random.permutation(jax.random.fold_in(rng, 3), rows)[jnp.arange(number_of) % rows]
    lots = jnp.where(jnp.arange(rows)[:, None] == holders[None, :], 1 << 14, lots)
    merit = lots * number_of + jnp.arange(number_of)
    return lax.top_k(merit.astype(jnp.int32), top)[1].astype(jnp.int32)


def length_profile(count, total, reach, skew):
    portions = [(1 << 20) // math.isqrt(rank ** skew) + 1 for rank in range(2, count + 1)]
    rest, counts = total - reach - (count - 1), [1] * (count - 1)
    while rest > 0:
        movable = [i for i in range(count - 1) if counts[i] < reach]
        mass, remaining = sum([portions[i] for i in movable]), rest
        for i in movable:
            extra = min(reach - counts[i], max(1, remaining * portions[i] // mass), rest)
            counts[i] = counts[i] + extra
            rest = rest - extra
    return np.array([reach] + counts)


def uneven_parts(stream_key, count, total, bound, lean):
    if count == 2:
        one = jax.random.randint(stream_key, (), max(1, total - bound), min(bound, total - 1) + 1)
        return jnp.stack([one, total - one])
    lengths = jnp.asarray(length_profile(count, total, bound, lean), jnp.int32)
    couples = (count - 1) // 2
    giver, taker = lengths[1:1 + 2 * couples:2], lengths[2:2 + 2 * couples:2]
    room = jnp.minimum(giver - 1, bound - taker)
    passed = jax.random.randint(jax.random.fold_in(stream_key, 1), (couples,), 0, 1 << 20) % (room + 1)
    lengths = lengths.at[1:1 + 2 * couples:2].set(giver - passed).at[2:2 + 2 * couples:2].set(taker + passed)
    return lengths[jax.random.permutation(jax.random.fold_in(stream_key, 2), count)]


def centred(key, extent, scale, most, pieces=(), kind=jnp.bfloat16):
    level = block_scale(key, extent, pieces, -0.22, 0.18) if pieces else 1.0
    array = jax.random.normal(key, extent, jnp.float32) * scale * level
    return jnp.minimum(jnp.maximum(array, -most), most).astype(kind)


def setup_inputs(seed: int = 0) -> dict:
    splits = jax.random.split(jax.random.key(seed), 14)
    block_input = centred(splits[0], (SEQS, LEN, D), 1.0, 6.0, ((0, 8), (1, 4)), jnp.float32)
    segments = jax.vmap(lambda own: jnp.searchsorted(jnp.cumsum(uneven_parts(own, SEG, LEN, LEN // 2, 3)), jnp.arange(LEN), side="right"))(jax.random.split(splits[1], SEQS)).reshape((SEQS, LEN)).astype(jnp.int32)
    routes = different_ones(splits[2], LAYERS * SEQS * LEN, EXPERTS, TOP, 4096).reshape((LAYERS, SEQS, LEN, TOP))
    distance_bucket = touch_ends(jax.random.randint(splits[3], (LEN,), 0, BUCKETS), jax.random.fold_in(splits[3], 1), 0, BUCKETS - 1).astype(jnp.int32)
    first_gain = jnp.clip(1.0 + 0.1 * jax.random.normal(splits[4], (LAYERS, D), jnp.float32), 0.5, 1.5).astype(jnp.bfloat16)
    query_key_value = centred(splits[5], (LAYERS, D, 3 * D), D ** -0.5, 0.21875, ((1, 4),))
    attention_out = centred(splits[6], (LAYERS, D, D), (D // 16) ** -0.5, 0.875, ((1, 4),))
    bias_table = centred(splits[7], (LAYERS, BUCKETS, HEADS), 1.0, 4.0, ((1, 4),))
    second_gain = jnp.clip(1.0 + 0.1 * jax.random.normal(splits[8], (LAYERS, D), jnp.float32), 0.5, 1.5).astype(jnp.bfloat16)
    router_weights = centred(splits[9], (LAYERS, D, EXPERTS), (D // 4) ** -0.5, 0.4375, ((1, 4),))
    expert_up = centred(splits[10], (LAYERS, EXPERTS, D, FF), D ** -0.5, 0.21875, ((2, 4), (3, 2)))
    expert_down = centred(splits[11], (LAYERS, EXPERTS, FF, D), FF ** -0.5, 0.109375, ((2, 2), (3, 4)))
    cotangent = centred(splits[12], (SEQS, LEN, D), 1.0, 6.0, ((0, 8), (1, 4)), jnp.float32)
    return {"block_input": block_input, "segments": segments, "routes": routes, "distance_bucket": distance_bucket, "first_gain": first_gain, "query_key_value": query_key_value, "attention_out": attention_out, "bias_table": bias_table, "second_gain": second_gain, "router_weights": router_weights, "expert_up": expert_up, "expert_down": expert_down, "cotangent": cotangent}


epsilon = 1e-06
negative = -1e+30
highest_precision = lax.Precision.HIGHEST

@jax.custom_vjp
def lower_precision(v):
    return lax.optimization_barrier(v.astype(jnp.bfloat16)).astype(jnp.float32)

@jax.custom_vjp
def lower_precision_back(v):
    return v

def low_keep(v):
    return (lower_precision(v), None)

def low_pass(kept, grad):
    return (grad,)

def back_keep(v):
    return (v, None)

def back_low(kept, grad):
    return (lower_precision(grad),)
lower_precision.defvjp(low_keep, low_pass)
lower_precision_back.defvjp(back_keep, back_low)

def scaled(values, gain_vec):
    return values * lax.rsqrt(lax.optimization_barrier(jnp.mean(values * values, axis=-1, keepdims=True)) + epsilon) * gain_vec

def regroup(values):
    inner = SEQ_DEV * N_TENSOR
    shaped = values.reshape((N_DP, inner, N_SEQ, PIECE) + values.shape[2:])
    order = (0, 2, 1, 3) + tuple(range(4, shaped.ndim))
    return jnp.transpose(shaped, order).reshape((N_DP * N_SEQ, inner * PIECE) + values.shape[2:])

def ungroup(values):
    inner = SEQ_DEV * N_TENSOR
    shaped = values.reshape((N_DP, N_SEQ, inner, PIECE) + values.shape[2:])
    order = (0, 2, 1, 3) + tuple(range(4, shaped.ndim))
    return jnp.transpose(shaped, order).reshape((SEQS, LEN) + values.shape[2:])

def attend_one(bias_full, inputs):
    queries, key_seq, value_seq, seg_seq = inputs
    score_logits = jnp.einsum('qhd,khd->hqk', queries, key_seq, precision=highest_precision) * 0.125 + bias_full
    score_logits = lower_precision_back(score_logits)
    row_index = lax.iota(jnp.int32, LEN)
    allowed = (seg_seq[:, None] == seg_seq[None, :]) & (row_index[None, :] <= row_index[:, None])
    probs = lower_precision(jax.nn.softmax(jnp.where(allowed[None], score_logits, negative), axis=-1))
    mixed = jnp.einsum('hqk,khd->qhd', probs, value_seq, precision=highest_precision)
    return (bias_full, lower_precision(lower_precision_back(mixed)).reshape(LEN, D))

def expert_block(weights, inputs):
    first_proj, second_proj = weights
    token_rows, picks, shares = inputs
    flat_picks = picks.reshape(-1).astype(jnp.int32)
    onehot = (flat_picks[:, None] == jnp.arange(EXPERTS, dtype=jnp.int32)[None, :]).astype(jnp.int32)
    places = lax.optimization_barrier(jnp.sum((jnp.cumsum(onehot, axis=0).astype(jnp.int32) - 1) * onehot, axis=1)).astype(jnp.int32)
    target = jnp.where(places < CAP, flat_picks * CAP + places, EXPERTS * CAP).astype(jnp.int32)
    pair_total = flat_picks.shape[0]
    source = jnp.full((EXPERTS * CAP + 1,), pair_total, jnp.int32).at[target].set(jnp.arange(pair_total, dtype=jnp.int32))
    token_of_slot = (source[:EXPERTS * CAP] // TOP).astype(jnp.int32)
    padded = jnp.concatenate([token_rows, jnp.zeros((1, D), jnp.float32)], axis=0)
    slots = padded[token_of_slot].reshape(EXPERTS, CAP, D)
    hidden_pre = lower_precision_back(jnp.einsum('ecd,edf->ecf', slots, first_proj, precision=highest_precision))
    hidden = lower_precision(jax.nn.gelu(hidden_pre, approximate=True))
    result = lower_precision_back(jnp.einsum('ecf,efd->ecd', hidden, second_proj, precision=highest_precision))
    spread = jnp.concatenate([result.reshape(EXPERTS * CAP, D), jnp.zeros((1, D), jnp.float32)], axis=0)
    per_pair = spread[target].reshape(GROUP, TOP, D)
    return (weights, lax.optimization_barrier(jnp.sum(shares[:, :, None] * per_pair, axis=1)))

def forward(residual_state, params, segments, routes, distance_bucket):
    gain_one, query_key_value_weight, output_projection, table, gain_two, router_weight, up_proj, down_proj = params
    distance = lax.iota(jnp.int32, LEN)[:, None] - lax.iota(jnp.int32, LEN)[None, :]
    index = jnp.clip(distance, 0, LEN - 1).astype(jnp.int32)
    for decoder_layer in range(LAYERS):
        normalized_input = lower_precision(scaled(residual_state, gain_one[decoder_layer]))
        projected_rows = lower_precision(lower_precision_back(jnp.einsum('uxk,kb->uxb', normalized_input, query_key_value_weight[decoder_layer], precision=highest_precision)))
        projected_rows = projected_rows.reshape(SEQS, LEN, 3, HEADS, HD)
        by_distance = table[decoder_layer][distance_bucket]
        bias_full = jnp.transpose(by_distance[index], (2, 0, 1))
        _, attention_part = lax.scan(jax.checkpoint(attend_one), bias_full, (projected_rows[:, :, 0], projected_rows[:, :, 1], projected_rows[:, :, 2], segments))
        middle_state = residual_state + lower_precision_back(jnp.einsum('uxk,kb->uxb', attention_part, output_projection[decoder_layer], precision=highest_precision))
        normalized_second = lower_precision(scaled(middle_state, gain_two[decoder_layer]))
        score_logits = lower_precision_back(jnp.einsum('uxk,kb->uxb', normalized_second, router_weight[decoder_layer], precision=highest_precision))
        probs = jax.nn.softmax(score_logits, axis=-1)
        chosen = jnp.take_along_axis(probs, routes[decoder_layer], axis=-1)
        shares = chosen / lax.optimization_barrier(jnp.sum(chosen, axis=-1, keepdims=True))
        _, mixed = lax.scan(jax.checkpoint(expert_block), (up_proj[decoder_layer], down_proj[decoder_layer]), (regroup(normalized_second), regroup(routes[decoder_layer]), regroup(shares)))
        residual_state = middle_state + ungroup(mixed)
    return residual_state

def reference(block_input, segments, routes, distance_bucket, first_gain, query_key_value, attention_out, bias_table, second_gain, router_weights, expert_up, expert_down, cotangent):
    params = (first_gain.astype(jnp.float32), query_key_value.astype(jnp.float32), attention_out.astype(jnp.float32), bias_table.astype(jnp.float32), second_gain.astype(jnp.float32), router_weights.astype(jnp.float32), expert_up.astype(jnp.float32), expert_down.astype(jnp.float32))

    def wrapped(residual_state, params_in):
        return forward(residual_state, params_in, segments, routes, distance_bucket)
    result, puller = jax.vjp(wrapped, block_input, params)
    stream_grad, param_grads = puller(cotangent)
    return (result, stream_grad, param_grads[0], param_grads[1], param_grads[2], param_grads[3], param_grads[4], param_grads[5], param_grads[6], param_grads[7])
```

```python
import functools

import jax
import jax.numpy as jnp
from jax import lax
from jax.experimental import pallas as pl
from jax.experimental.pallas import tpu as pltpu
from jax.sharding import PartitionSpec as P

HEADS = 12
LAYERS = 2
epsilon = 1e-06
negative = -1e30
highest_precision = lax.Precision.HIGHEST


def scaled(values, gain_vec):
    return values * lax.rsqrt(jnp.mean(values * values, axis=-1, keepdims=True) + epsilon) * gain_vec


HD = 64
ROWS = 128
NT = (((1,), (1,)), ((), ()))
TN = (((0,), (0,)), ((), ()))


def visit_blocks(length, span, one_block):
    full = span // ROWS
    for i in range(min(full - 1, length // ROWS)):
        one_block(i * ROWS, 0, (i + 1) * ROWS)

    def step(i, carry):
        start = pl.multiple_of(i * ROWS, ROWS)
        one_block(start, pl.multiple_of(start + ROWS - span, ROWS), span)
        return carry

    lax.fori_loop(full - 1, length // ROWS, step, 0)


def fill_mask(mask_ref, segr_ref, segc_ref, start, low, width):
    same = segc_ref[pl.ds(start, ROWS), :] == segr_ref[:, pl.ds(low, width)]
    back = lax.broadcasted_iota(jnp.int32, (ROWS, width), 0) + (width - ROWS)
    allowed = same & (back >= lax.broadcasted_iota(jnp.int32, (ROWS, width), 1))
    mask_ref[:, :width] = jnp.where(allowed, 0.0, -1e30)


def fill_slab(slab_ref, line_ref, heads, span):
    for h in range(heads):
        spread = jnp.broadcast_to(line_ref[h : h + 1, :], (ROWS, span))
        slab_ref[h] = pltpu.roll(spread, 0, 1, stride=1, stride_axis=0)


def split_heads(qkv_ref, parts_ref, heads):
    for h in range(3 * heads):
        part = qkv_ref[:, h * HD : (h + 1) * HD]
        parts_ref[h] = part * jnp.bfloat16(0.125) if h < heads else part


def attn_fwd_kernel(heads, span, qkv_ref, segr_ref, segc_ref, line_ref, out_ref, lse_ref, parts_ref, mixed_ref, slab_ref, mask_ref):
    length = qkv_ref.shape[0]
    fill_slab(slab_ref, line_ref, heads, span)
    split_heads(qkv_ref, parts_ref, heads)

    def one_block(start, low, width):
        fill_mask(mask_ref, segr_ref, segc_ref, start, low, width)

        def one_head(h, carry):
            q = parts_ref[h, pl.ds(start, ROWS), :]
            k = parts_ref[heads + h, pl.ds(low, width), :]
            v = parts_ref[2 * heads + h, pl.ds(low, width), :]
            s = lax.dot_general(q, k, NT, preferred_element_type=jnp.float32)
            s = s + slab_ref[h, :, span - width :] + mask_ref[:, :width]
            top = jnp.max(s, axis=1, keepdims=True)
            e = jnp.exp(s - top)
            total = jnp.sum(e, axis=1, keepdims=True)
            mixed = jnp.dot(e.astype(jnp.bfloat16), v, preferred_element_type=jnp.float32)
            mixed_ref[h, pl.ds(start, ROWS), :] = (mixed / total).astype(jnp.bfloat16)
            lse_ref[h, pl.ds(start, ROWS), :] = top + jnp.log(total)
            return carry

        lax.fori_loop(0, heads, one_head, 0)

    visit_blocks(length, span, one_block)
    out_ref[...] = jnp.concatenate([mixed_ref[h] for h in range(heads)], axis=1)


def attn_bwd_kernel(heads, span, qkv_ref, segr_ref, segc_ref, line_ref, lse_ref, grad_ref, out_ref, band_ref,
                    parts_ref, gparts_ref, qgrad_ref, kgrad_ref, vgrad_ref, slab_ref, mask_ref, band_acc):
    length = qkv_ref.shape[0]
    fill_slab(slab_ref, line_ref, heads, span)
    split_heads(qkv_ref, parts_ref, heads)
    for h in range(heads):
        gparts_ref[h] = grad_ref[:, h * HD : (h + 1) * HD]
    kgrad_ref[...] = jnp.zeros_like(kgrad_ref)
    vgrad_ref[...] = jnp.zeros_like(vgrad_ref)
    band_acc[...] = jnp.zeros_like(band_acc)

    def one_block(start, low, width):
        fill_mask(mask_ref, segr_ref, segc_ref, start, low, width)

        def one_head(h, carry):
            rows = pl.ds(start, ROWS)
            window = pl.ds(low, width)
            q = parts_ref[h, rows, :]
            k = parts_ref[heads + h, window, :]
            v = parts_ref[2 * heads + h, window, :]
            grad = gparts_ref[h, rows, :]
            s = lax.dot_general(q, k, NT, preferred_element_type=jnp.float32)
            s = s + slab_ref[h, :, span - width :] + mask_ref[:, :width]
            p = jnp.exp(s - lse_ref[h, rows, :])
            dp = lax.dot_general(grad, v, NT, preferred_element_type=jnp.float32)
            inner = jnp.sum(p * dp, axis=1, keepdims=True)
            ds = p * (dp - inner)
            band_acc[h, :, span - width :] += ds
            ds = ds.astype(jnp.bfloat16)
            qgrad = jnp.dot(ds, k, preferred_element_type=jnp.float32)
            qgrad_ref[h, rows, :] = (qgrad * 0.125).astype(jnp.bfloat16)
            kgrad_ref[h, window, :] += lax.dot_general(ds, q, TN, preferred_element_type=jnp.float32)
            vgrad_ref[h, window, :] += lax.dot_general(p.astype(jnp.bfloat16), grad, TN, preferred_element_type=jnp.float32)
            return carry

        lax.fori_loop(0, heads, one_head, 0)

    visit_blocks(length, span, one_block)
    parts = [qgrad_ref[h] for h in range(heads)]
    parts += [kgrad_ref[h].astype(jnp.bfloat16) for h in range(heads)]
    parts += [vgrad_ref[h].astype(jnp.bfloat16) for h in range(heads)]
    out_ref[...] = jnp.concatenate(parts, axis=1)
    row = lax.broadcasted_iota(jnp.int32, (ROWS, span), 0)
    for h in range(heads):
        acc = band_acc[h]
        bit = 1
        while bit < ROWS:
            acc = jnp.where((row & bit) != 0, pltpu.roll(acc, span - bit, 1), acc)
            bit *= 2
        band_ref[h : h + 1, :] = jnp.sum(acc, axis=0, keepdims=True)


def vmem(count):
    return [pl.BlockSpec(memory_space=pltpu.VMEM)] * count


def attend(qkv, seg_row, seg_col, line):
    length, width = qkv.shape
    heads, span = line.shape
    return pl.pallas_call(
        functools.partial(attn_fwd_kernel, heads, span),
        out_shape=(
            jax.ShapeDtypeStruct((length, heads * HD), jnp.bfloat16),
            jax.ShapeDtypeStruct((heads, length, 1), jnp.float32),
        ),
        in_specs=vmem(4),
        out_specs=tuple(vmem(2)),
        scratch_shapes=[
            pltpu.VMEM((3 * heads, length, HD), jnp.bfloat16),
            pltpu.VMEM((heads, length, HD), jnp.bfloat16),
            pltpu.VMEM((heads, ROWS, span), jnp.float32),
            pltpu.VMEM((ROWS, span), jnp.float32),
        ],
        name="attend",
    )(qkv, seg_row, seg_col, line)


def attend_back(qkv, seg_row, seg_col, line, lse, grad):
    length, width = qkv.shape
    heads, span = line.shape
    return pl.pallas_call(
        functools.partial(attn_bwd_kernel, heads, span),
        out_shape=(
            jax.ShapeDtypeStruct((length, width), jnp.bfloat16),
            jax.ShapeDtypeStruct((heads, span), jnp.float32),
        ),
        in_specs=vmem(6),
        out_specs=tuple(vmem(2)),
        scratch_shapes=[
            pltpu.VMEM((3 * heads, length, HD), jnp.bfloat16),
            pltpu.VMEM((heads, length, HD), jnp.bfloat16),
            pltpu.VMEM((heads, length, HD), jnp.bfloat16),
            pltpu.VMEM((heads, length, HD), jnp.float32),
            pltpu.VMEM((heads, length, HD), jnp.float32),
            pltpu.VMEM((heads, ROWS, span), jnp.float32),
            pltpu.VMEM((ROWS, span), jnp.float32),
            pltpu.VMEM((heads, ROWS, span), jnp.float32),
        ],
        name="attend_back",
    )(qkv, seg_row, seg_col, line, lse, grad)


def plane_gather(values):
    return lax.all_gather(values, ("seq", "tensor"), axis=0, tiled=True)


def plane_sum(values):
    return lax.psum_scatter(values, ("seq", "tensor"), scatter_dimension=0, tiled=True)


def seq_gather(values):
    return lax.all_gather(values, "seq", axis=0, tiled=True)


def seq_sum(values):
    return lax.psum_scatter(values, "seq", scatter_dimension=0, tiled=True)


def heads_to_tokens(values):
    return lax.all_to_all(values, "seq", split_axis=0, concat_axis=1, tiled=True)


def tokens_to_heads(values):
    return lax.all_to_all(values, "seq", split_axis=1, concat_axis=0, tiled=True)


def norm_back(values, gain_vec, grad):
    inverse = lax.rsqrt(jnp.mean(values * values, axis=-1, keepdims=True) + epsilon)
    unit = values * inverse
    scaled_grad = grad * gain_vec
    gain_grad = jnp.sum(grad * unit, axis=0)
    return inverse * (scaled_grad - unit * jnp.mean(scaled_grad * unit, axis=-1, keepdims=True)), gain_grad


def gelu_parts(values):
    cubic = values * values * 0.044715
    inner = jnp.tanh(0.7978845608028654 * values * (1.0 + cubic))
    slope = 0.5 * (1.0 + inner) + 0.5 * values * (1.0 - inner * inner) * 0.7978845608028654 * (1.0 + 3.0 * cubic)
    return 0.5 * values * (1.0 + inner), slope


def dot(left, right):
    return jnp.dot(left, right, preferred_element_type=jnp.float32)


def dot_nt(left, right):
    return lax.dot_general(left, right, NT, preferred_element_type=jnp.float32)


def dot_tn(left, right):
    return lax.dot_general(left, right, TN, preferred_element_type=jnp.float32)


def body(
    block_input,
    segments,
    routes,
    distance_bucket,
    first_gain,
    query_key_value,
    attention_out,
    bias_table,
    second_gain,
    router_weights,
    expert_up,
    expert_down,
    cotangent,
):
    low = jnp.bfloat16
    seq_count, piece, width = block_input.shape
    n_dp, n_seq, n_tensor = (lax.axis_size(name) for name in ("dp", "seq", "tensor"))
    n_plane = n_seq * n_tensor
    length = piece * n_seq
    local_heads = HEADS // n_seq
    head_width = local_heads * HD
    experts = expert_up.shape[1]
    assert seq_count == 1 and experts == n_seq
    shard = width // n_dp
    bucket_count = bias_table.shape[1] * n_dp
    bucket_shard = bias_table.shape[1]
    group_rows = n_tensor * piece
    capacity = group_rows * routes.shape[-1] // experts
    seq_index = lax.axis_index("seq")
    plane_index = seq_index * n_tensor + lax.axis_index("tensor")
    span = ROWS + length // 2

    small = jnp.concatenate(
        [
            first_gain.reshape(LAYERS, -1),
            second_gain.reshape(LAYERS, -1),
            bias_table.reshape(LAYERS, -1),
            router_weights.reshape(LAYERS, -1),
        ],
        axis=1,
    )
    small = lax.all_gather(small, "dp", axis=0)
    cuts = [shard, 2 * shard, 2 * shard + bucket_shard * HEADS]
    gains_one, gains_two, tables, routers = jnp.split(small, cuts, axis=2)

    def whole(values, trailing):
        return jnp.moveaxis(values, 1, 0).reshape((LAYERS, -1) + trailing)

    gains_one = whole(gains_one, ()).astype(jnp.float32)
    gains_two = whole(gains_two, ()).astype(jnp.float32)
    tables = whole(tables, (HEADS,)).astype(jnp.float32)
    routers = whole(routers, (experts,))

    own_qkv = lax.dynamic_index_in_dim(
        query_key_value.reshape(LAYERS, shard, 3, n_seq, head_width), seq_index, 3, keepdims=False
    ).reshape(LAYERS, shard, 3 * head_width)
    out_columns = width // n_plane
    own_out = lax.dynamic_index_in_dim(
        attention_out.reshape(LAYERS, shard, n_plane, out_columns), plane_index, 2, keepdims=False
    )
    own_up = lax.dynamic_index_in_dim(expert_up, seq_index, 1, keepdims=False)
    own_down = lax.dynamic_index_in_dim(expert_down, seq_index, 1, keepdims=False).swapaxes(1, 2)

    def attention_weights(layer):
        qkv = lax.all_gather(own_qkv[layer], "dp", axis=0, tiled=True)
        out = lax.all_gather(own_out[layer], ("dp", "seq", "tensor"), axis=0)
        out = out.reshape(n_dp, n_plane, shard, out_columns)
        return qkv, jnp.moveaxis(out, 1, 2).reshape(width, width)

    def expert_weights(layer):
        up = lax.all_gather(own_up[layer], "dp", axis=0, tiled=True)
        down = lax.all_gather(own_down[layer], "dp", axis=0, tiled=True)
        return up, down

    routes_all = lax.all_gather(routes, "seq", axis=0)
    routes_all = jnp.moveaxis(routes_all, 0, 1).reshape(LAYERS, n_seq, group_rows, -1)
    seg_row = segments
    seg_col = segments.reshape(length, 1)
    bucket_line = distance_bucket[length // 2 - 1 :: -1][: length // 2]
    bucket_line = jnp.concatenate(
        [jnp.full((1,), -1, jnp.int32), bucket_line, jnp.full((span - 1 - length // 2,), -1, jnp.int32)]
    )
    line_hot = (bucket_line[None, :] == lax.iota(jnp.int32, bucket_count)[:, None]).astype(jnp.float32)
    strict_upper = (
        lax.iota(jnp.int32, group_rows)[:, None] < lax.iota(jnp.int32, group_rows)[None, :]
    ).astype(low)

    def routing(layer):
        layer_routes = routes_all[layer]
        mine = jnp.any(layer_routes == seq_index, axis=-1)
        slot = dot(mine.astype(low), strict_upper).astype(jnp.int32)
        slot = jnp.where(mine & (slot < capacity), slot, -1)
        hot = (slot[:, None, :] == lax.iota(jnp.int32, capacity)[None, :, None]).astype(low)
        chosen = jnp.any(layer_routes[..., None] == lax.iota(jnp.int32, experts), axis=2)
        return hot, chosen.reshape(n_seq * group_rows, experts)

    def to_slots(hot, rows):
        rows = rows.reshape(n_seq, group_rows, width)
        out = jnp.einsum("gct,gtd->gcd", hot, rows, preferred_element_type=jnp.float32)
        return out.astype(low).reshape(n_seq * capacity, width)

    def from_slots(hot, rows):
        rows = rows.reshape(n_seq, capacity, -1)
        out = jnp.einsum("gct,gcd->gtd", hot, rows, preferred_element_type=jnp.float32)
        return out.reshape(n_seq * group_rows, -1)

    current = block_input[0]
    grad = cotangent[0]
    saved = []
    for layer in range(LAYERS):
        qkv_weight, out_weight = attention_weights(layer)
        up, down = expert_weights(layer)
        normed = scaled(current, gains_one[layer]).astype(low)
        normed_all = seq_gather(normed)
        qkv = dot(normed_all, qkv_weight).astype(low)
        own_table = lax.dynamic_slice_in_dim(tables[layer], seq_index * local_heads, local_heads, 1)
        line = jnp.dot(own_table.T, line_hot, precision=highest_precision)
        mixed, log_total = attend(qkv, seg_row, seg_col, line)
        merged = heads_to_tokens(mixed)
        middle = current + dot(merged, out_weight)
        normed_two = scaled(middle, gains_two[layer]).astype(low)
        tokens = plane_gather(normed_two)
        hot, chosen = routing(layer)
        router_logits = dot(tokens, routers[layer])
        router_logits = jnp.where(chosen, router_logits, negative)
        raised = jnp.exp(router_logits - jnp.max(router_logits, axis=1, keepdims=True))
        shares = raised / jnp.sum(raised, axis=1, keepdims=True)
        own_share = lax.dynamic_slice_in_dim(shares, seq_index, 1, 1)
        slots = to_slots(hot, tokens)
        pre = dot(slots, up)
        hidden = gelu_parts(pre)[0].astype(low)
        pre = pre.astype(low)
        result = dot_nt(hidden, down).astype(low)
        part = (own_share * from_slots(hot, result)).astype(low)
        following = middle + plane_sum(part).astype(jnp.float32)
        saved.append(
            (current, normed_all, qkv, line, log_total, merged, middle, tokens, hot, shares, own_share, slots, pre, hidden,
             qkv_weight, out_weight, up, down)
        )
        current = following

    results = [None] * LAYERS
    for layer in range(LAYERS - 1, -1, -1):
        (layer_in, normed_all, qkv, line, log_total, merged, middle, tokens, hot, shares, own_share, slots, pre, hidden,
         qkv_weight, out_weight, up, down) = saved[layer]
        grad_rows = plane_gather(grad.astype(low)).astype(jnp.float32)
        result_grad = to_slots(hot, (own_share * grad_rows).astype(low))
        hidden_grad = dot(result_grad, down)
        down_grad = dot_tn(result_grad, hidden)
        pair_sum = jnp.sum(hidden.astype(jnp.float32) * hidden_grad, axis=1)
        pre_grad = (gelu_parts(pre.astype(jnp.float32))[1] * hidden_grad).astype(low)
        up_grad = dot_tn(slots, pre_grad)
        slot_grad = dot_nt(pre_grad, up).astype(low)
        token_pair = jnp.einsum(
            "gct,gc->gt", hot.astype(jnp.float32), pair_sum.reshape(n_seq, capacity), precision=highest_precision
        ).reshape(-1, 1)
        own_hot = (lax.iota(jnp.int32, experts) == seq_index).astype(jnp.float32)
        logit_grad = (token_pair * (own_hot[None, :] - shares)).astype(low)
        part = from_slots(hot, slot_grad) + dot_nt(logit_grad, routers[layer])
        router_grad = dot_tn(tokens, logit_grad)
        normed_two_grad = plane_sum(part.astype(low)).astype(jnp.float32)
        middle_part, gain_two_grad = norm_back(middle, gains_two[layer], normed_two_grad)
        middle_grad = grad + middle_part
        out_grad = middle_grad.astype(low)
        out_weight_grad = dot_tn(merged, out_grad)
        merged_grad = dot_nt(out_grad, out_weight).astype(low)
        mixed_grad = tokens_to_heads(merged_grad)
        qkv_grad, band = attend_back(qkv, seg_row, seg_col, line, log_total, mixed_grad)
        qkv_weight_grad = dot_tn(normed_all, qkv_grad)
        normed_grad = seq_sum(dot_nt(qkv_grad, qkv_weight).astype(low)).astype(jnp.float32)
        input_part, gain_one_grad = norm_back(layer_in, gains_one[layer], normed_grad)
        grad = middle_grad + input_part
        table_grad = jnp.dot(line_hot, band.T, precision=highest_precision)
        table_grad = lax.dynamic_update_slice_in_dim(
            jnp.zeros((bucket_count, HEADS), jnp.float32), table_grad, seq_index * local_heads, 1
        )

        expert_grads = []
        for piece_grad in (up_grad, down_grad):
            piece_grad = lax.psum_scatter(piece_grad.astype(low), "dp", scatter_dimension=0, tiled=True)
            expert_grads.append(lax.all_gather(piece_grad, "seq", axis=0).astype(jnp.float32))
        up_total, down_total = expert_grads[0], expert_grads[1].swapaxes(1, 2)

        packed = jnp.concatenate(
            [
                gain_one_grad.reshape(n_dp, -1),
                gain_two_grad.reshape(n_dp, -1),
                table_grad.reshape(n_dp, -1),
                router_grad.reshape(n_dp, -1),
            ],
            axis=1,
        )
        packed_width = packed.shape[1]
        lanes = width
        per_row = n_plane * lanes
        extra = -(-packed_width // per_row) * per_row - packed_width
        packed = jnp.pad(packed, ((0, 0), (0, extra))).reshape(n_dp, n_plane, -1, lanes)
        both = jnp.concatenate([out_weight_grad.reshape(n_dp, n_plane, -1, width), packed], axis=2).astype(low)
        both = lax.psum_scatter(both.reshape((n_dp * n_plane,) + both.shape[2:]), ("dp", "seq", "tensor"), scatter_dimension=0, tiled=True)
        both = lax.all_gather(both, ("seq", "tensor"), axis=0, tiled=True).astype(jnp.float32)
        out_rows = shard // n_plane
        out_total = both[:, :out_rows].reshape(shard, width)
        packed_total = both[:, out_rows:].reshape(-1)[:packed_width]
        gain_one_total = packed_total[: cuts[0]]
        gain_two_total = packed_total[cuts[0] : cuts[1]]
        table_total = packed_total[cuts[1] : cuts[2]].reshape(bucket_shard, HEADS)
        router_total = packed_total[cuts[2] :].reshape(shard, experts)

        qkv_total = lax.psum_scatter(qkv_weight_grad.astype(low), ("dp", "tensor"), scatter_dimension=0, tiled=True)
        qkv_total = lax.all_gather(qkv_total, ("seq", "tensor"), axis=0).astype(jnp.float32)
        qkv_total = qkv_total.reshape(n_seq, shard, 3, head_width)
        qkv_total = jnp.moveaxis(qkv_total, 0, 2).reshape(shard, 3 * width)
        results[layer] = (gain_one_total, qkv_total, out_total, table_total, gain_two_total, router_total, up_total, down_total)

    stacked = [jnp.stack([results[layer][member] for layer in range(LAYERS)]) for member in range(8)]
    return (current[None], grad[None]) + tuple(stacked)


def solution(mesh):
    in_specs = (
        P(("dp", "tensor"), "seq", None),
        P(("dp", "tensor"), None),
        P(None, "dp", "seq", None),
        P(),
        P(None, "dp"),
        P(None, "dp", None),
        P(None, "dp", None),
        P(None, "dp", None),
        P(None, "dp"),
        P(None, "dp", None),
        P(None, None, "dp", "tensor"),
        P(None, None, "tensor", "dp"),
        P(("dp", "tensor"), "seq", None),
    )
    out_specs = (
        P(("dp", "tensor"), "seq", None),
        P(("dp", "tensor"), "seq", None),
        P(None, "dp"),
        P(None, "dp", None),
        P(None, "dp", None),
        P(None, "dp", None),
        P(None, "dp"),
        P(None, "dp", None),
        P(None, None, "dp", "tensor"),
        P(None, None, "tensor", "dp"),
    )
    return jax.shard_map(body, mesh=mesh, in_specs=in_specs, out_specs=out_specs, check_vma=False)
```

```python
import functools

import jax
import jax.numpy as jnp
from jax import lax
from jax.experimental import pallas as pl
from jax.experimental.pallas import tpu as pltpu
from jax.sharding import PartitionSpec as P

HEADS = 12
LAYERS = 2
epsilon = 1e-06
negative = -1e30
highest_precision = lax.Precision.HIGHEST


def scaled(values, gain_vec):
    return values * lax.rsqrt(jnp.mean(values * values, axis=-1, keepdims=True) + epsilon) * gain_vec


HD = 64
ROWS = 128
NT = (((1,), (1,)), ((), ()))
TN = (((0,), (0,)), ((), ()))


def visit_blocks(length, span, one_block, midway=None):
    full = span // ROWS
    for i in range(min(full - 1, length // ROWS)):
        one_block(i * ROWS, 0, (i + 1) * ROWS)

    def step(i, carry):
        start = pl.multiple_of(i * ROWS, ROWS)
        one_block(start, pl.multiple_of(start + ROWS - span, ROWS), span)
        return carry

    middle = (full + length // ROWS) // 2
    if midway is None:
        lax.fori_loop(full - 1, length // ROWS, step, 0)
    else:
        lax.fori_loop(full - 1, middle, step, 0)
        midway()
        lax.fori_loop(middle, length // ROWS, step, 0)


def fill_mask(mask_ref, segr_ref, segc_ref, start, low, width):
    same = segc_ref[pl.ds(start, ROWS), :] == segr_ref[:, pl.ds(low, width)]
    back = lax.broadcasted_iota(jnp.int32, (ROWS, width), 0) + (width - ROWS)
    allowed = same & (back >= lax.broadcasted_iota(jnp.int32, (ROWS, width), 1))
    mask_ref[:, :width] = jnp.where(allowed, 0.0, -1e30)


def fill_slab(slab_ref, line_ref, heads, span):
    for h in range(heads):
        spread = jnp.broadcast_to(line_ref[h : h + 1, :], (ROWS, span))
        slab_ref[h] = pltpu.roll(spread, 0, 1, stride=1, stride_axis=0)


def split_heads(qkv_ref, parts_ref, heads):
    for h in range(3 * heads):
        part = qkv_ref[:, h * HD : (h + 1) * HD]
        parts_ref[h] = part * jnp.bfloat16(0.125) if h < heads else part


def attn_fwd_kernel(heads, span, spread, *refs):
    qkv_ref, segr_ref, segc_ref, line_ref = refs[:4]
    midway = None
    if spread:
        rows_ref, out_ref, lse_ref, gathered_ref = refs[4:8]
        wires = Wires(*refs[12:])
        place = plane_place()
        greet(*plane_peers(place))
        gathered_ref[place[0], place[1]] = rows_ref[...].astype(jnp.bfloat16)
        first = plane_gather_start(wires, gathered_ref, place)
        second = []
        midway = lambda: second.extend(plane_gather_forward(wires, gathered_ref, place, first))
        refs = refs[8:12]
    else:
        out_ref, lse_ref = refs[4:6]
        refs = refs[6:10]
    parts_ref, mixed_ref, slab_ref, mask_ref = refs
    length = qkv_ref.shape[0]
    fill_slab(slab_ref, line_ref, heads, span)
    split_heads(qkv_ref, parts_ref, heads)

    def one_block(start, low, width):
        fill_mask(mask_ref, segr_ref, segc_ref, start, low, width)

        def one_head(h, carry):
            q = parts_ref[h, pl.ds(start, ROWS), :]
            k = parts_ref[heads + h, pl.ds(low, width), :]
            v = parts_ref[2 * heads + h, pl.ds(low, width), :]
            s = lax.dot_general(q, k, NT, preferred_element_type=jnp.float32)
            s = s + slab_ref[h, :, span - width :] + mask_ref[:, :width]
            top = jnp.max(s, axis=1, keepdims=True)
            e = jnp.exp(s - top)
            total = jnp.sum(e, axis=1, keepdims=True)
            mixed = jnp.dot(e.astype(jnp.bfloat16), v, preferred_element_type=jnp.float32)
            mixed_ref[h, pl.ds(start, ROWS), :] = (mixed / total).astype(jnp.bfloat16)
            lse_ref[h, pl.ds(start, ROWS), :] = top + jnp.log(total)
            return carry

        lax.fori_loop(0, heads, one_head, 0)

    visit_blocks(length, span, one_block, midway)
    out_ref[...] = jnp.concatenate([mixed_ref[h] for h in range(heads)], axis=1)
    if spread:
        plane_gather_finish(wires, gathered_ref, place, first, second)
        wires.finish()


def attn_bwd_kernel(heads, span, qkv_ref, segr_ref, segc_ref, line_ref, lse_ref, grad_ref, out_ref, band_ref,
                    parts_ref, gparts_ref, qgrad_ref, kgrad_ref, vgrad_ref, slab_ref, mask_ref, band_acc):
    length = qkv_ref.shape[0]
    fill_slab(slab_ref, line_ref, heads, span)
    split_heads(qkv_ref, parts_ref, heads)
    for h in range(heads):
        gparts_ref[h] = grad_ref[:, h * HD : (h + 1) * HD]
    kgrad_ref[...] = jnp.zeros_like(kgrad_ref)
    vgrad_ref[...] = jnp.zeros_like(vgrad_ref)
    band_acc[...] = jnp.zeros_like(band_acc)

    def one_block(start, low, width):
        fill_mask(mask_ref, segr_ref, segc_ref, start, low, width)

        def one_head(h, carry):
            rows = pl.ds(start, ROWS)
            window = pl.ds(low, width)
            q = parts_ref[h, rows, :]
            k = parts_ref[heads + h, window, :]
            v = parts_ref[2 * heads + h, window, :]
            grad = gparts_ref[h, rows, :]
            s = lax.dot_general(q, k, NT, preferred_element_type=jnp.float32)
            s = s + slab_ref[h, :, span - width :] + mask_ref[:, :width]
            p = jnp.exp(s - lse_ref[h, rows, :])
            dp = lax.dot_general(grad, v, NT, preferred_element_type=jnp.float32)
            inner = jnp.sum(p * dp, axis=1, keepdims=True)
            ds = p * (dp - inner)
            band_acc[h, :, span - width :] += ds
            ds = ds.astype(jnp.bfloat16)
            qgrad = jnp.dot(ds, k, preferred_element_type=jnp.float32)
            qgrad_ref[h, rows, :] = (qgrad * 0.125).astype(jnp.bfloat16)
            kgrad_ref[h, window, :] += lax.dot_general(ds, q, TN, preferred_element_type=jnp.float32)
            vgrad_ref[h, window, :] += lax.dot_general(p.astype(jnp.bfloat16), grad, TN, preferred_element_type=jnp.float32)
            return carry

        lax.fori_loop(0, heads, one_head, 0)

    visit_blocks(length, span, one_block)
    parts = [qgrad_ref[h] for h in range(heads)]
    parts += [kgrad_ref[h].astype(jnp.bfloat16) for h in range(heads)]
    parts += [vgrad_ref[h].astype(jnp.bfloat16) for h in range(heads)]
    out_ref[...] = jnp.concatenate(parts, axis=1)
    row = lax.broadcasted_iota(jnp.int32, (ROWS, span), 0)
    for h in range(heads):
        acc = band_acc[h]
        bit = 1
        while bit < ROWS:
            acc = jnp.where((row & bit) != 0, pltpu.roll(acc, span - bit, 1), acc)
            bit *= 2
        band_ref[h : h + 1, :] = jnp.sum(acc, axis=0, keepdims=True)


def vmem(count):
    return [pl.BlockSpec(memory_space=pltpu.VMEM)] * count


def attend_scratch(heads, length, span):
    return [
        pltpu.VMEM((3 * heads, length, HD), jnp.bfloat16),
        pltpu.VMEM((heads, length, HD), jnp.bfloat16),
        pltpu.VMEM((heads, ROWS, span), jnp.float32),
        pltpu.VMEM((ROWS, span), jnp.float32),
    ]


def attend(qkv, seg_row, seg_col, line):
    length, width = qkv.shape
    heads, span = line.shape
    return pl.pallas_call(
        functools.partial(attn_fwd_kernel, heads, span, False),
        out_shape=(
            jax.ShapeDtypeStruct((length, heads * HD), jnp.bfloat16),
            jax.ShapeDtypeStruct((heads, length, 1), jnp.float32),
        ),
        in_specs=vmem(4),
        out_specs=tuple(vmem(2)),
        scratch_shapes=attend_scratch(heads, length, span),
        cost_estimate=cost(15.0),
        name="attend",
    )(qkv, seg_row, seg_col, line)


def attend_back(qkv, seg_row, seg_col, line, lse, grad):
    length, width = qkv.shape
    heads, span = line.shape
    return pl.pallas_call(
        functools.partial(attn_bwd_kernel, heads, span),
        out_shape=(
            jax.ShapeDtypeStruct((length, width), jnp.bfloat16),
            jax.ShapeDtypeStruct((heads, span), jnp.float32),
        ),
        in_specs=vmem(6),
        out_specs=tuple(vmem(2)),
        scratch_shapes=[
            pltpu.VMEM((3 * heads, length, HD), jnp.bfloat16),
            pltpu.VMEM((heads, length, HD), jnp.bfloat16),
            pltpu.VMEM((heads, length, HD), jnp.bfloat16),
            pltpu.VMEM((heads, length, HD), jnp.float32),
            pltpu.VMEM((heads, length, HD), jnp.float32),
            pltpu.VMEM((heads, ROWS, span), jnp.float32),
            pltpu.VMEM((ROWS, span), jnp.float32),
            pltpu.VMEM((heads, ROWS, span), jnp.float32),
        ],
        cost_estimate=cost(21.0),
        name="attend_back",
    )(qkv, seg_row, seg_col, line, lse, grad)


MESH_ID = pl.DeviceIdType.MESH


class Wires:
    def __init__(self, send, recv):
        self.send, self.recv, self.next, self.started = send, recv, 0, []

    def copy(self, src, dst, where):
        one = pltpu.make_async_remote_copy(
            src_ref=src, dst_ref=dst, send_sem=self.send.at[self.next], recv_sem=self.recv.at[self.next],
            device_id=where, device_id_type=MESH_ID,
        )
        self.next += 1
        one.start()
        self.started.append(one)
        return one

    def finish(self):
        for one in self.started:
            one.wait_send()


def plane_place():
    me = lax.axis_index("seq")
    core = lax.axis_index("tensor")
    near, far = me + 1 - 2 * lax.rem(me, 2), lax.rem(me + 2, 4)
    cross = lax.rem(near + 2, 4)
    return me, core, near, far, cross


def greet(*places):
    barrier = pltpu.get_barrier_semaphore()
    for where in places:
        pl.semaphore_signal(barrier, inc=1, device_id=where, device_id_type=MESH_ID)
    pl.semaphore_wait(barrier, len(places))


def seq_gather_start(wires, ref, place):
    me, core, near, far, cross = place
    mine = ref.at[me]
    return wires.copy(mine, mine, {"seq": near}), wires.copy(mine, mine, {"seq": far})


def seq_gather_forward(wires, ref, place, first):
    me, core, near, far, cross = place
    half = ref.shape[1] // 2
    first[0].wait_recv()
    upper = ref.at[near, pl.ds(0, half)]
    one = wires.copy(upper, upper, {"seq": far})
    first[1].wait_recv()
    lower = ref.at[far, pl.ds(half, half)]
    return one, wires.copy(lower, lower, {"seq": near})


def plane_gather_start(wires, ref, place):
    me, core, near, far, cross = place
    mine = ref.at[me, core]
    return (
        wires.copy(mine, mine, {"seq": near}),
        wires.copy(mine, mine, {"seq": far}),
        wires.copy(mine, mine, {"tensor": 1 - core}),
    )


def plane_gather_forward(wires, ref, place, first):
    me, core, near, far, cross = place
    half = ref.shape[2] // 2
    partner = {"tensor": 1 - core}
    first[0].wait_recv()
    upper = ref.at[near, core, pl.ds(0, half)]
    one = wires.copy(upper, upper, {"seq": far})
    first[1].wait_recv()
    lower = ref.at[far, core, pl.ds(half, half)]
    two = wires.copy(lower, lower, {"seq": near})
    block = ref.at[near, core]
    three = wires.copy(block, block, partner)
    block = ref.at[far, core]
    four = wires.copy(block, block, partner)
    return one, two, three, four


def plane_gather_finish(wires, ref, place, first, second):
    me, core, near, far, cross = place
    half = ref.shape[2] // 2
    partner = {"tensor": 1 - core}
    second[0].wait_recv()
    upper = ref.at[cross, core, pl.ds(0, half)]
    one = wires.copy(upper, upper, partner)
    second[1].wait_recv()
    lower = ref.at[cross, core, pl.ds(half, half)]
    two = wires.copy(lower, lower, partner)
    for other in (first[2], second[2], second[3], one, two):
        other.wait_recv()


def wide(values):
    return values.astype(jnp.float32)


def cross_sum(wires, place, total_of, out_refs):
    me, core, near, far, cross = place
    cross_ref, near_ref, far_ref, cross_in, near_in, far_in = out_refs
    half = near_ref.shape[0] // 2
    top, bottom = pl.ds(0, half), pl.ds(half, half)
    cross_ref[...] = total_of(cross).astype(cross_ref.dtype)
    to_near = wires.copy(cross_ref.at[top], cross_in.at[top], {"seq": near})
    to_far = wires.copy(cross_ref.at[bottom], cross_in.at[bottom], {"seq": far})
    near_ref[...] = total_of(near).astype(near_ref.dtype)
    near_one = wires.copy(near_ref.at[top], near_in.at[top], {"seq": near})
    far_ref[...] = total_of(far).astype(far_ref.dtype)
    far_one = wires.copy(far_ref.at[bottom], far_in.at[bottom], {"seq": far})
    own = total_of(me)
    to_near.wait_recv()
    far_ref[top, :] = (wide(far_ref[top, :]) + wide(cross_in[top, :])).astype(far_ref.dtype)
    far_two = wires.copy(far_ref.at[top], far_in.at[top], {"seq": far})
    to_far.wait_recv()
    near_ref[bottom, :] = (wide(near_ref[bottom, :]) + wide(cross_in[bottom, :])).astype(near_ref.dtype)
    near_two = wires.copy(near_ref.at[bottom], near_in.at[bottom], {"seq": near})
    for one in (near_one, far_one, far_two, near_two):
        one.wait_recv()
    return own + wide(near_in[...]) + wide(far_in[...])


def plane_sum(wires, place, part_ref, partner_in, out_refs):
    me, core, near, far, cross = place
    arrivals = {}
    for name, spot in (("cross", cross), ("near", near), ("far", far), ("me", me)):
        arrivals[name] = wires.copy(part_ref.at[spot, 1 - core], partner_in.at[spot], {"tensor": 1 - core})
    order = iter(("cross", "near", "far", "me"))

    def total_of(spot):
        arrivals[next(order)].wait_recv()
        return wide(part_ref[spot, core]) + wide(partner_in[spot])

    return cross_sum(wires, place, total_of, out_refs)


def sum_scratch(piece, width):
    return [pltpu.VMEM((piece, width), jnp.bfloat16)] * 6


def sems(count):
    return [pltpu.SemaphoreType.DMA((count,)), pltpu.SemaphoreType.DMA((count,))]


def plane_peers(place):
    me, core, near, far, cross = place
    return {"seq": near}, {"seq": far}, {"tensor": 1 - core}


def norm_of(values, gain_vec):
    return values * lax.rsqrt(jnp.mean(values * values, axis=-1, keepdims=True) + epsilon) * gain_vec


def norm_back(values, gain_vec, grad):
    inverse = lax.rsqrt(jnp.mean(values * values, axis=-1, keepdims=True) + epsilon)
    unit = values * inverse
    scaled_grad = grad * gain_vec
    gain_grad = jnp.sum(grad * unit, axis=0, keepdims=True)
    return inverse * (scaled_grad - unit * jnp.mean(scaled_grad * unit, axis=-1, keepdims=True)), gain_grad


def dot(left, right):
    return jnp.dot(left, right, preferred_element_type=jnp.float32)


def dot_nt(left, right):
    return lax.dot_general(left, right, NT, preferred_element_type=jnp.float32)


def dot_tn(left, right):
    return lax.dot_general(left, right, TN, preferred_element_type=jnp.float32)


def project_steps(place, x_ref, gain_ref, w_ref, normed_ref, qkv_ref, wires):
    me, core, near, far, cross = place
    normed_ref[me] = norm_of(x_ref[...], gain_ref[...]).astype(jnp.bfloat16)
    first = seq_gather_start(wires, normed_ref, place)
    qkv_ref[me] = dot(normed_ref[me], w_ref[...]).astype(jnp.bfloat16)
    second = seq_gather_forward(wires, normed_ref, place, first)
    qkv_ref[near] = dot(normed_ref[near], w_ref[...]).astype(jnp.bfloat16)
    qkv_ref[far] = dot(normed_ref[far], w_ref[...]).astype(jnp.bfloat16)
    second[0].wait_recv()
    second[1].wait_recv()
    qkv_ref[cross] = dot(normed_ref[cross], w_ref[...]).astype(jnp.bfloat16)


def project_kernel(x_ref, gain_ref, w_ref, routes_ref, normed_ref, qkv_ref, routes_all_ref, send, recv):
    place = plane_place()
    me, core, near, far, cross = place
    wires = Wires(send, recv)
    greet({"seq": near}, {"seq": far}, {"seq": cross})
    routes_all_ref[me] = routes_ref[...]
    picks = [wires.copy(routes_ref, routes_all_ref.at[me], {"seq": spot}) for spot in (near, far, cross)]
    project_steps(place, x_ref, gain_ref, w_ref, normed_ref, qkv_ref, wires)
    for one in picks:
        one.wait_recv()
    wires.finish()


def sum_project_kernel(part_ref, base_ref, gain_ref, w_ref, x_ref, normed_ref, qkv_ref, partner_in, *rest):
    out_refs, (send, recv) = rest[:6], rest[6:]
    place = plane_place()
    wires = Wires(send, recv)
    greet(*plane_peers(place))
    x_ref[...] = base_ref[...] + plane_sum(wires, place, part_ref, partner_in, out_refs)
    project_steps(place, x_ref, gain_ref, w_ref, normed_ref, qkv_ref, wires)
    wires.finish()


def sum_kernel(part_ref, base_ref, x_ref, partner_in, *rest):
    out_refs, (send, recv) = rest[:6], rest[6:]
    place = plane_place()
    wires = Wires(send, recv)
    greet(*plane_peers(place))
    x_ref[...] = base_ref[...] + plane_sum(wires, place, part_ref, partner_in, out_refs)
    wires.finish()


def merge_kernel(mixed_ref, base_ref, w_ref, gain_ref, merged_ref, middle_ref, tokens_ref, send, recv):
    place = plane_place()
    me, core, near, far, cross = place
    wires = Wires(send, recv)
    greet({"seq": near}, {"seq": far}, {"seq": cross}, {"tensor": 1 - core})
    copies = [wires.copy(mixed_ref.at[spot], merged_ref.at[me], {"seq": spot}) for spot in (cross, near, far)]
    merged_ref[me] = mixed_ref[me]
    total = base_ref[...] + dot(mixed_ref[me], w_ref[me])
    for spot, one in ((near, copies[1]), (far, copies[2]), (cross, copies[0])):
        one.wait_recv()
        total = total + dot(merged_ref[spot], w_ref[spot])
    middle_ref[...] = total
    tokens_ref[me, core] = norm_of(total, gain_ref[...]).astype(jnp.bfloat16)
    first = plane_gather_start(wires, tokens_ref, place)
    second = plane_gather_forward(wires, tokens_ref, place, first)
    plane_gather_finish(wires, tokens_ref, place, first, second)
    wires.finish()


def split_kernel(part_ref, middle_ref, gain_ref, grad_ref, w_ref, middle_grad_ref, out_grad_ref, gain_grad_ref, mixed_grad_ref,
                 outgoing, partner_in, *rest):
    out_refs, (send, recv) = rest[:6], rest[6:]
    place = plane_place()
    me, core, near, far, cross = place
    wires = Wires(send, recv)
    greet({"seq": near}, {"seq": far}, {"seq": cross}, {"tensor": 1 - core})
    normed_grad = plane_sum(wires, place, part_ref, partner_in, out_refs)
    part, gain_grad_ref[...] = norm_back(middle_ref[...], gain_ref[...], normed_grad)
    middle_grad = grad_ref[...] + part
    middle_grad_ref[...] = middle_grad
    out_grad_ref[...] = middle_grad.astype(jnp.bfloat16)
    copies = []
    for spot in (cross, near, far):
        outgoing[spot] = dot_nt(out_grad_ref[...], w_ref[spot]).astype(jnp.bfloat16)
        copies.append(wires.copy(outgoing.at[spot], mixed_grad_ref.at[me], {"seq": spot}))
    mixed_grad_ref[me] = dot_nt(out_grad_ref[...], w_ref[me]).astype(jnp.bfloat16)
    for one in copies:
        one.wait_recv()
    wires.finish()


def input_grad_kernel(spread, qkv_grad_ref, w_ref, x_ref, gain_ref, middle_grad_ref, *rest):
    grad_ref, gain_grad_ref = rest[:2]
    rows_ref = rest[2] if spread else None
    rest = rest[3:] if spread else rest[2:]
    out_refs, (send, recv) = rest[:6], rest[6:]
    place = plane_place()
    me, core, near, far, cross = place
    wires = Wires(send, recv)
    greet(*plane_peers(place)[: 3 if spread else 2])
    normed_grad = cross_sum(wires, place, lambda spot: dot_nt(qkv_grad_ref[spot], w_ref[...]), out_refs)
    part, gain_grad_ref[...] = norm_back(x_ref[...], gain_ref[...], normed_grad)
    grad = middle_grad_ref[...] + part
    grad_ref[...] = grad
    if spread:
        rows_ref[me, core] = grad.astype(jnp.bfloat16)
        first = plane_gather_start(wires, rows_ref, place)
        second = plane_gather_forward(wires, rows_ref, place, first)
        plane_gather_finish(wires, rows_ref, place, first, second)
    wires.finish()


def comm_call(kernel, name, number, time, outs, scratch, wire_count, *operands):
    return pl.pallas_call(
        kernel,
        out_shape=tuple(outs),
        in_specs=vmem(len(operands)),
        out_specs=tuple(vmem(len(outs))),
        scratch_shapes=scratch + sems(wire_count),
        compiler_params=pltpu.CompilerParams(collective_id=number, has_side_effects=True),
        cost_estimate=cost(time),
        name=name,
    )(*operands)


def cost(time):
    return pl.CostEstimate(flops=0, bytes_accessed=int(time * 3e6), transcendentals=0)


def low_array(*shape):
    return jax.ShapeDtypeStruct(shape, jnp.bfloat16)


def wide_array(*shape):
    return jax.ShapeDtypeStruct(shape, jnp.float32)


def attend_gather(qkv, seg_row, seg_col, line, rows, n_tensor):
    length, width = qkv.shape
    heads, span = line.shape
    piece, depth = rows.shape
    outs = [low_array(length, heads * HD), wide_array(heads, length, 1), low_array(length // piece, n_tensor, piece, depth)]
    return comm_call(functools.partial(attn_fwd_kernel, heads, span, True), "attend_gather", 6, 16.0, outs,
                     attend_scratch(heads, length, span), 9, qkv, seg_row, seg_col, line, rows)


def gelu_parts(values):
    cubic = values * values * 0.044715
    inner = jnp.tanh(0.7978845608028654 * values * (1.0 + cubic))
    slope = 0.5 * (1.0 + inner) + 0.5 * values * (1.0 - inner * inner) * 0.7978845608028654 * (1.0 + 3.0 * cubic)
    return 0.5 * values * (1.0 + inner), slope


def body(
    block_input,
    segments,
    routes,
    distance_bucket,
    first_gain,
    query_key_value,
    attention_out,
    bias_table,
    second_gain,
    router_weights,
    expert_up,
    expert_down,
    cotangent,
):
    low = jnp.bfloat16
    seq_count, piece, width = block_input.shape
    n_dp, n_seq, n_tensor = (lax.axis_size(name) for name in ("dp", "seq", "tensor"))
    n_plane = n_seq * n_tensor
    length = piece * n_seq
    local_heads = HEADS // n_seq
    head_width = local_heads * HD
    experts = expert_up.shape[1]
    assert seq_count == 1 and experts == n_seq
    shard = width // n_dp
    bucket_count = bias_table.shape[1] * n_dp
    bucket_shard = bias_table.shape[1]
    group_rows = n_tensor * piece
    capacity = group_rows * routes.shape[-1] // experts
    seq_index = lax.axis_index("seq")
    plane_index = seq_index * n_tensor + lax.axis_index("tensor")
    span = ROWS + length // 2

    small = jnp.concatenate(
        [
            first_gain.reshape(LAYERS, -1),
            second_gain.reshape(LAYERS, -1),
            bias_table.reshape(LAYERS, -1),
            router_weights.reshape(LAYERS, -1),
        ],
        axis=1,
    )
    small = lax.all_gather(small, "dp", axis=0)
    cuts = [shard, 2 * shard, 2 * shard + bucket_shard * HEADS]
    gains_one, gains_two, tables, routers = jnp.split(small, cuts, axis=2)

    def whole(values, trailing):
        return jnp.moveaxis(values, 1, 0).reshape((LAYERS, -1) + trailing)

    gains_one = whole(gains_one, ()).astype(jnp.float32)
    gains_two = whole(gains_two, ()).astype(jnp.float32)
    tables = whole(tables, (HEADS,)).astype(jnp.float32)
    routers = whole(routers, (experts,))

    own_qkv = lax.dynamic_index_in_dim(
        query_key_value.reshape(LAYERS, shard, 3, n_seq, head_width), seq_index, 3, keepdims=False
    ).reshape(LAYERS, shard, 3 * head_width)
    out_columns = width // n_plane
    own_out = lax.dynamic_index_in_dim(
        attention_out.reshape(LAYERS, shard, n_plane, out_columns), plane_index, 2, keepdims=False
    )
    own_up = lax.dynamic_index_in_dim(expert_up, seq_index, 1, keepdims=False)
    own_down = lax.dynamic_index_in_dim(expert_down, seq_index, 1, keepdims=False).swapaxes(1, 2)

    def attention_weights(layer):
        qkv = lax.all_gather(own_qkv[layer], "dp", axis=0, tiled=True)
        out = lax.all_gather(own_out[layer], ("dp", "seq", "tensor"), axis=0)
        out = out.reshape(n_dp, n_plane, shard, out_columns)
        return qkv, jnp.moveaxis(out, 1, 2).reshape(n_seq, head_width, width)

    def expert_weights(layer):
        up = lax.all_gather(own_up[layer], "dp", axis=0, tiled=True)
        down = lax.all_gather(own_down[layer], "dp", axis=0, tiled=True)
        return up, down

    assert n_seq == 4 and n_tensor == 2
    routes_own = routes.reshape(-1, 128)
    seg_row = segments
    seg_col = segments.reshape(length, 1)
    bucket_line = distance_bucket[length // 2 - 1 :: -1][: length // 2]
    bucket_line = jnp.concatenate(
        [jnp.full((1,), -1, jnp.int32), bucket_line, jnp.full((span - 1 - length // 2,), -1, jnp.int32)]
    )
    line_hot = (bucket_line[None, :] == lax.iota(jnp.int32, bucket_count)[:, None]).astype(jnp.float32)
    strict_upper = (
        lax.iota(jnp.int32, group_rows)[:, None] < lax.iota(jnp.int32, group_rows)[None, :]
    ).astype(low)

    def routing(layer, routes_all):
        layer_routes = routes_all[layer]
        mine = jnp.any(layer_routes == seq_index, axis=-1)
        slot = dot(mine.astype(low), strict_upper).astype(jnp.int32)
        slot = jnp.where(mine & (slot < capacity), slot, -1)
        hot = (slot[:, None, :] == lax.iota(jnp.int32, capacity)[None, :, None]).astype(low)
        chosen = jnp.any(layer_routes[..., None] == lax.iota(jnp.int32, experts), axis=2)
        return hot, chosen.reshape(n_seq * group_rows, experts)

    def to_slots(hot, rows):
        rows = rows.reshape(n_seq, group_rows, width)
        out = jnp.einsum("gct,gtd->gcd", hot, rows, preferred_element_type=jnp.float32)
        return out.astype(low).reshape(n_seq * capacity, width)

    def from_slots(hot, rows):
        rows = rows.reshape(n_seq, capacity, -1)
        out = jnp.einsum("gct,gcd->gtd", hot, rows, preferred_element_type=jnp.float32)
        return out.reshape(n_seq * group_rows, -1)

    current = block_input[0]
    grad = cotangent[0]
    saved = []
    for layer in range(LAYERS):
        qkv_weight, out_weight = attention_weights(layer)
        up, down = expert_weights(layer)
        gain_one, gain_two = gains_one[layer][None], gains_two[layer][None]
        outs = [low_array(n_seq, piece, width), low_array(n_seq, piece, 3 * head_width)]
        if layer == 0:
            outs.append(jax.ShapeDtypeStruct((n_seq,) + routes_own.shape, jnp.int32))
            normed_all, qkv, routes_all = comm_call(
                project_kernel, "project", 1, 16.0, outs, [], 7, current, gain_one, qkv_weight, routes_own
            )
            routes_all = routes_all.reshape((n_seq,) + routes.shape)
            routes_all = jnp.moveaxis(routes_all, 0, 1).reshape(LAYERS, n_seq, group_rows, -1)
        else:
            current, normed_all, qkv = comm_call(
                sum_project_kernel, "sum_project", 2, 32.0, [wide_array(piece, width)] + outs,
                [pltpu.VMEM((n_seq, piece, width), low)] + sum_scratch(piece, width), 14, part, middle, gain_one, qkv_weight
            )
        qkv = qkv.reshape(length, 3 * head_width)
        own_table = lax.dynamic_slice_in_dim(tables[layer], seq_index * local_heads, local_heads, 1)
        line = jnp.dot(own_table.T, line_hot, precision=highest_precision)
        if layer == 0:
            mixed, log_total, grad_rows = attend_gather(qkv, seg_row, seg_col, line, grad, n_tensor)
        else:
            mixed, log_total = attend(qkv, seg_row, seg_col, line)
        merged, middle, tokens = comm_call(
            merge_kernel, "merge", 3, 21.0,
            [low_array(n_seq, piece, head_width), wide_array(piece, width), low_array(n_seq, n_tensor, piece, width)], [], 12,
            mixed.reshape(n_seq, piece, head_width), current, out_weight, gain_two
        )
        tokens = tokens.reshape(n_plane * piece, width)
        hot, chosen = routing(layer, routes_all)
        router_logits = dot(tokens, routers[layer])
        router_logits = jnp.where(chosen, router_logits, negative)
        raised = jnp.exp(router_logits - jnp.max(router_logits, axis=1, keepdims=True))
        shares = raised / jnp.sum(raised, axis=1, keepdims=True)
        own_share = lax.dynamic_slice_in_dim(shares, seq_index, 1, 1)
        slots = to_slots(hot, tokens)
        pre = dot(slots, up)
        hidden = gelu_parts(pre)[0].astype(low)
        pre = pre.astype(low)
        result = dot_nt(hidden, down).astype(low)
        part = (own_share * from_slots(hot, result)).astype(low)
        part = part.reshape(n_seq, n_tensor, piece, width)
        saved.append(
            (current, normed_all, qkv, line, log_total, merged, middle, tokens, hot, shares, own_share, slots, pre, hidden,
             qkv_weight, out_weight, up, down)
        )

    (block_output,) = comm_call(
        sum_kernel, "sum_last", 4, 16.0, [wide_array(piece, width)], [pltpu.VMEM((n_seq, piece, width), low)] + sum_scratch(piece, width),
        10, part, middle
    )
    results = [None] * LAYERS
    for layer in range(LAYERS - 1, -1, -1):
        (layer_in, normed_all, qkv, line, log_total, merged, middle, tokens, hot, shares, own_share, slots, pre, hidden,
         qkv_weight, out_weight, up, down) = saved[layer]
        gain_one, gain_two = gains_one[layer][None], gains_two[layer][None]
        grad_rows = grad_rows.reshape(n_plane * piece, width).astype(jnp.float32)
        result_grad = to_slots(hot, (own_share * grad_rows).astype(low))
        hidden_grad = dot(result_grad, down)
        down_grad = dot_tn(result_grad, hidden)
        pair_sum = jnp.sum(hidden.astype(jnp.float32) * hidden_grad, axis=1)
        pre_grad = (gelu_parts(pre.astype(jnp.float32))[1] * hidden_grad).astype(low)
        up_grad = dot_tn(slots, pre_grad)
        slot_grad = dot_nt(pre_grad, up).astype(low)
        token_pair = jnp.einsum(
            "gct,gc->gt", hot.astype(jnp.float32), pair_sum.reshape(n_seq, capacity), precision=highest_precision
        ).reshape(-1, 1)
        own_hot = (lax.iota(jnp.int32, experts) == seq_index).astype(jnp.float32)
        logit_grad = (token_pair * (own_hot[None, :] - shares)).astype(low)
        part = from_slots(hot, slot_grad) + dot_nt(logit_grad, routers[layer])
        router_grad = dot_tn(tokens, logit_grad)
        part = part.astype(low).reshape(n_seq, n_tensor, piece, width)
        middle_grad, out_grad, gain_two_grad, mixed_grad = comm_call(
            split_kernel, "split", 5, 22.0,
            [wide_array(piece, width), low_array(piece, width), wide_array(1, width), low_array(n_seq, piece, head_width)],
            [pltpu.VMEM((n_seq, piece, head_width), low), pltpu.VMEM((n_seq, piece, width), low)] + sum_scratch(piece, width), 13,
            part, middle, gain_two, grad, out_weight
        )
        out_weight_grad = jnp.einsum("gtd,te->gde", merged, out_grad, preferred_element_type=jnp.float32).reshape(width, width)
        qkv_grad, band = attend_back(qkv, seg_row, seg_col, line, log_total, mixed_grad.reshape(length, head_width))
        qkv_weight_grad = dot_tn(normed_all.reshape(length, width), qkv_grad)
        spread = layer > 0
        outs = [wide_array(piece, width), wide_array(1, width)]
        outs += [low_array(n_seq, n_tensor, piece, width)] if spread else []
        outs = comm_call(
            functools.partial(input_grad_kernel, spread), "input_grad_spread" if spread else "input_grad", 7 + spread, 32.0 if spread else 16.0,
            outs, sum_scratch(piece, width), 15, qkv_grad.reshape(n_seq, piece, -1), qkv_weight, layer_in, gain_one, middle_grad
        )
        grad, gain_one_grad = outs[:2]
        grad_rows = outs[2] if spread else None
        table_grad = jnp.dot(line_hot, band.T, precision=highest_precision)
        table_grad = lax.dynamic_update_slice_in_dim(
            jnp.zeros((bucket_count, HEADS), jnp.float32), table_grad, seq_index * local_heads, 1
        )

        expert_grads = []
        for piece_grad in (up_grad, down_grad):
            piece_grad = lax.psum_scatter(piece_grad.astype(low), "dp", scatter_dimension=0, tiled=True)
            expert_grads.append(lax.all_gather(piece_grad, "seq", axis=0).astype(jnp.float32))
        up_total, down_total = expert_grads[0], expert_grads[1].swapaxes(1, 2)

        packed = jnp.concatenate(
            [
                gain_one_grad.reshape(n_dp, -1),
                gain_two_grad.reshape(n_dp, -1),
                table_grad.reshape(n_dp, -1),
                router_grad.reshape(n_dp, -1),
            ],
            axis=1,
        )
        packed_width = packed.shape[1]
        lanes = width
        per_row = n_plane * lanes
        extra = -(-packed_width // per_row) * per_row - packed_width
        packed = jnp.pad(packed, ((0, 0), (0, extra))).reshape(n_dp, n_plane, -1, lanes)
        both = jnp.concatenate([out_weight_grad.reshape(n_dp, n_plane, -1, width), packed], axis=2).astype(low)
        both = lax.psum_scatter(both.reshape((n_dp * n_plane,) + both.shape[2:]), ("dp", "seq", "tensor"), scatter_dimension=0, tiled=True)
        both = lax.all_gather(both, ("seq", "tensor"), axis=0, tiled=True).astype(jnp.float32)
        out_rows = shard // n_plane
        out_total = both[:, :out_rows].reshape(shard, width)
        packed_total = both[:, out_rows:].reshape(-1)[:packed_width]
        gain_one_total = packed_total[: cuts[0]]
        gain_two_total = packed_total[cuts[0] : cuts[1]]
        table_total = packed_total[cuts[1] : cuts[2]].reshape(bucket_shard, HEADS)
        router_total = packed_total[cuts[2] :].reshape(shard, experts)

        qkv_total = lax.psum_scatter(qkv_weight_grad.astype(low), ("dp", "tensor"), scatter_dimension=0, tiled=True)
        qkv_total = lax.all_gather(qkv_total, ("seq", "tensor"), axis=0).astype(jnp.float32)
        qkv_total = qkv_total.reshape(n_seq, shard, 3, head_width)
        qkv_total = jnp.moveaxis(qkv_total, 0, 2).reshape(shard, 3 * width)
        results[layer] = (gain_one_total, qkv_total, out_total, table_total, gain_two_total, router_total, up_total, down_total)

    stacked = [jnp.stack([results[layer][member] for layer in range(LAYERS)]) for member in range(8)]
    return (block_output[None], grad[None]) + tuple(stacked)


def solution(mesh):
    in_specs = (
        P(("dp", "tensor"), "seq", None),
        P(("dp", "tensor"), None),
        P(None, "dp", "seq", None),
        P(),
        P(None, "dp"),
        P(None, "dp", None),
        P(None, "dp", None),
        P(None, "dp", None),
        P(None, "dp"),
        P(None, "dp", None),
        P(None, None, "dp", "tensor"),
        P(None, None, "tensor", "dp"),
        P(("dp", "tensor"), "seq", None),
    )
    out_specs = (
        P(("dp", "tensor"), "seq", None),
        P(("dp", "tensor"), "seq", None),
        P(None, "dp"),
        P(None, "dp", None),
        P(None, "dp", None),
        P(None, "dp", None),
        P(None, "dp"),
        P(None, "dp", None),
        P(None, None, "dp", "tensor"),
        P(None, None, "tensor", "dp"),
    )
    return jax.shard_map(body, mesh=mesh, in_specs=in_specs, out_specs=out_specs, check_vma=False)
```

```python
import functools

import jax
import jax.numpy as jnp
from jax import lax
from jax.experimental import pallas as pl
from jax.experimental.pallas import tpu as pltpu
from jax.sharding import PartitionSpec as P

HEADS = 12
LAYERS = 2
epsilon = 1e-06
negative = -1e30
highest_precision = lax.Precision.HIGHEST


def scaled(values, gain_vec):
    return values * lax.rsqrt(jnp.mean(values * values, axis=-1, keepdims=True) + epsilon) * gain_vec


HD = 64
ROWS = 128
NT = (((1,), (1,)), ((), ()))
TN = (((0,), (0,)), ((), ()))


def visit_blocks(length, span, one_block, midway=None):
    full = span // ROWS
    for i in range(min(full - 1, length // ROWS)):
        one_block(i * ROWS, 0, (i + 1) * ROWS)

    def step(i, carry):
        start = pl.multiple_of(i * ROWS, ROWS)
        one_block(start, pl.multiple_of(start + ROWS - span, ROWS), span)
        return carry

    middle = (full + length // ROWS) // 2
    if midway is None:
        lax.fori_loop(full - 1, length // ROWS, step, 0)
    else:
        lax.fori_loop(full - 1, middle, step, 0)
        midway()
        lax.fori_loop(middle, length // ROWS, step, 0)


def fill_mask(mask_ref, segr_ref, segc_ref, start, low, width):
    same = segc_ref[pl.ds(start, ROWS), :] == segr_ref[:, pl.ds(low, width)]
    back = lax.broadcasted_iota(jnp.int32, (ROWS, width), 0) + (width - ROWS)
    allowed = same & (back >= lax.broadcasted_iota(jnp.int32, (ROWS, width), 1))
    mask_ref[:, :width] = jnp.where(allowed, 0.0, -1e30)


def fill_slab(slab_ref, line_ref, heads, span):
    for h in range(heads):
        spread = jnp.broadcast_to(line_ref[h : h + 1, :], (ROWS, span))
        slab_ref[h] = pltpu.roll(spread, 0, 1, stride=1, stride_axis=0)


def split_heads(qkv_ref, parts_ref, heads):
    for h in range(3 * heads):
        part = qkv_ref[:, h * HD : (h + 1) * HD]
        parts_ref[h] = part * jnp.bfloat16(0.125) if h < heads else part


def attn_fwd_kernel(heads, span, spread, *refs):
    qkv_ref, segr_ref, segc_ref, line_ref = refs[:4]
    midway = None
    if spread:
        rows_ref, qkv_next, out_next, out_ref, lse_ref, gathered_ref, qkv_all, out_all = refs[4:12]
        wires = Wires(*refs[16:])
        place = plane_place()
        core = place[1]
        line_me, targets, sources = dp_peers()
        greet(*plane_peers(place), *[{"dp": spot} for spot in targets])
        gathered_ref[place[0], core] = rows_ref[...].astype(jnp.bfloat16)
        first = plane_gather_start(wires, gathered_ref, place)
        qkvs = line_start(wires, qkv_next, qkv_all, core, line_me, targets)
        outs = line_start(wires, out_next, out_all, core, line_me, targets)
        second = []
        midway = lambda: second.extend(plane_gather_forward(wires, gathered_ref, place, first))
        refs = refs[12:16]
    else:
        out_ref, lse_ref = refs[4:6]
        refs = refs[6:10]
    parts_ref, mixed_ref, slab_ref, mask_ref = refs
    length = qkv_ref.shape[0]
    fill_slab(slab_ref, line_ref, heads, span)
    split_heads(qkv_ref, parts_ref, heads)

    def one_block(start, low, width):
        fill_mask(mask_ref, segr_ref, segc_ref, start, low, width)

        def one_head(h, carry):
            q = parts_ref[h, pl.ds(start, ROWS), :]
            k = parts_ref[heads + h, pl.ds(low, width), :]
            v = parts_ref[2 * heads + h, pl.ds(low, width), :]
            s = lax.dot_general(q, k, NT, preferred_element_type=jnp.float32)
            s = s + slab_ref[h, :, span - width :] + mask_ref[:, :width]
            top = jnp.max(s, axis=1, keepdims=True)
            e = jnp.exp(s - top)
            total = jnp.sum(e, axis=1, keepdims=True)
            mixed = jnp.dot(e.astype(jnp.bfloat16), v, preferred_element_type=jnp.float32)
            mixed_ref[h, pl.ds(start, ROWS), :] = (mixed / total).astype(jnp.bfloat16)
            lse_ref[h, pl.ds(start, ROWS), :] = top + jnp.log(total)
            return carry

        lax.fori_loop(0, heads, one_head, 0)

    visit_blocks(length, span, one_block, midway)
    out_ref[...] = jnp.concatenate([mixed_ref[h] for h in range(heads)], axis=1)
    if spread:
        plane_gather_finish(wires, gathered_ref, place, first, second)
        onward = line_forward(wires, qkv_all, core, qkvs, sources)
        onward += line_forward(wires, out_all, core, outs, sources)
        for one in onward:
            one.wait_recv()
        wires.finish()


def attn_bwd_kernel(heads, span, spread, *refs):
    qkv_ref, segr_ref, segc_ref, line_ref, lse_ref, grad_ref = refs[:6]
    midway = None
    if spread:
        shard_ref, out_ref, band_ref, shared_ref = refs[6:10]
        wires = Wires(*refs[18:])
        place = plane_place()
        greet({"seq": place[2]}, {"seq": place[3]})
        shared_ref[place[0]] = shard_ref[...]
        first = seq_gather_start(wires, shared_ref, place)
        second = []
        midway = lambda: second.extend(seq_gather_forward(wires, shared_ref, place, first))
        refs = refs[10:18]
    else:
        out_ref, band_ref = refs[6:8]
        refs = refs[8:16]
    parts_ref, gparts_ref, qgrad_ref, kgrad_ref, vgrad_ref, slab_ref, mask_ref, band_acc = refs
    length = qkv_ref.shape[0]
    fill_slab(slab_ref, line_ref, heads, span)
    split_heads(qkv_ref, parts_ref, heads)
    for h in range(heads):
        gparts_ref[h] = grad_ref[:, h * HD : (h + 1) * HD]
    kgrad_ref[...] = jnp.zeros_like(kgrad_ref)
    vgrad_ref[...] = jnp.zeros_like(vgrad_ref)
    band_acc[...] = jnp.zeros_like(band_acc)

    def one_block(start, low, width):
        fill_mask(mask_ref, segr_ref, segc_ref, start, low, width)

        def one_head(h, carry):
            rows = pl.ds(start, ROWS)
            window = pl.ds(low, width)
            q = parts_ref[h, rows, :]
            k = parts_ref[heads + h, window, :]
            v = parts_ref[2 * heads + h, window, :]
            grad = gparts_ref[h, rows, :]
            s = lax.dot_general(q, k, NT, preferred_element_type=jnp.float32)
            s = s + slab_ref[h, :, span - width :] + mask_ref[:, :width]
            p = jnp.exp(s - lse_ref[h, rows, :])
            dp = lax.dot_general(grad, v, NT, preferred_element_type=jnp.float32)
            inner = jnp.sum(p * dp, axis=1, keepdims=True)
            ds = p * (dp - inner)
            band_acc[h, :, span - width :] += ds
            ds = ds.astype(jnp.bfloat16)
            qgrad = jnp.dot(ds, k, preferred_element_type=jnp.float32)
            qgrad_ref[h, rows, :] = (qgrad * 0.125).astype(jnp.bfloat16)
            kgrad_ref[h, window, :] += lax.dot_general(ds, q, TN, preferred_element_type=jnp.float32)
            vgrad_ref[h, window, :] += lax.dot_general(p.astype(jnp.bfloat16), grad, TN, preferred_element_type=jnp.float32)
            return carry

        lax.fori_loop(0, heads, one_head, 0)

    visit_blocks(length, span, one_block, midway)
    parts = [qgrad_ref[h] for h in range(heads)]
    parts += [kgrad_ref[h].astype(jnp.bfloat16) for h in range(heads)]
    parts += [vgrad_ref[h].astype(jnp.bfloat16) for h in range(heads)]
    out_ref[...] = jnp.concatenate(parts, axis=1)
    row = lax.broadcasted_iota(jnp.int32, (ROWS, span), 0)
    for h in range(heads):
        acc = band_acc[h]
        bit = 1
        while bit < ROWS:
            acc = jnp.where((row & bit) != 0, pltpu.roll(acc, span - bit, 1), acc)
            bit *= 2
        band_ref[h : h + 1, :] = jnp.sum(acc, axis=0, keepdims=True)
    if spread:
        for one in second:
            one.wait_recv()
        wires.finish()


def vmem(count):
    return [pl.BlockSpec(memory_space=pltpu.VMEM)] * count


def attend_scratch(heads, length, span):
    return [
        pltpu.VMEM((3 * heads, length, HD), jnp.bfloat16),
        pltpu.VMEM((heads, length, HD), jnp.bfloat16),
        pltpu.VMEM((heads, ROWS, span), jnp.float32),
        pltpu.VMEM((ROWS, span), jnp.float32),
    ]


def attend(qkv, seg_row, seg_col, line):
    length, width = qkv.shape
    heads, span = line.shape
    return pl.pallas_call(
        functools.partial(attn_fwd_kernel, heads, span, False),
        out_shape=(
            jax.ShapeDtypeStruct((length, heads * HD), jnp.bfloat16),
            jax.ShapeDtypeStruct((heads, length, 1), jnp.float32),
        ),
        in_specs=vmem(4),
        out_specs=tuple(vmem(2)),
        scratch_shapes=attend_scratch(heads, length, span),
        cost_estimate=cost(15.0),
        name="attend",
    )(qkv, seg_row, seg_col, line)


def attend_back(qkv, seg_row, seg_col, line, lse, grad, shard=None):
    length, width = qkv.shape
    heads, span = line.shape
    outs = [low_array(length, width), wide_array(heads, span)]
    scratch = [
        pltpu.VMEM((3 * heads, length, HD), jnp.bfloat16),
        pltpu.VMEM((heads, length, HD), jnp.bfloat16),
        pltpu.VMEM((heads, length, HD), jnp.bfloat16),
        pltpu.VMEM((heads, length, HD), jnp.float32),
        pltpu.VMEM((heads, length, HD), jnp.float32),
        pltpu.VMEM((heads, ROWS, span), jnp.float32),
        pltpu.VMEM((ROWS, span), jnp.float32),
        pltpu.VMEM((heads, ROWS, span), jnp.float32),
    ]
    operands = [qkv, seg_row, seg_col, line, lse, grad]
    if shard is not None:
        outs.append(low_array(4, *shard.shape))
        kernel = functools.partial(attn_bwd_kernel, heads, span, True)
        return comm_call(kernel, "attend_back_share", 9, 25.0, outs, scratch, 4, *operands, shard)
    return pl.pallas_call(
        functools.partial(attn_bwd_kernel, heads, span, False),
        out_shape=tuple(outs),
        in_specs=vmem(6),
        out_specs=tuple(vmem(2)),
        scratch_shapes=scratch,
        cost_estimate=cost(21.0),
        name="attend_back",
    )(*operands)


MESH_ID = pl.DeviceIdType.MESH


class Wires:
    def __init__(self, send, recv):
        self.send, self.recv, self.next, self.started = send, recv, 0, []

    def copy(self, src, dst, where):
        one = pltpu.make_async_remote_copy(
            src_ref=src, dst_ref=dst, send_sem=self.send.at[self.next], recv_sem=self.recv.at[self.next],
            device_id=where, device_id_type=MESH_ID,
        )
        self.next += 1
        one.start()
        self.started.append(one)
        return one

    def finish(self):
        for one in self.started:
            one.wait_send()


def plane_place():
    me = lax.axis_index("seq")
    core = lax.axis_index("tensor")
    near, far = me + 1 - 2 * lax.rem(me, 2), lax.rem(me + 2, 4)
    cross = lax.rem(near + 2, 4)
    return me, core, near, far, cross


def greet(*places):
    barrier = pltpu.get_barrier_semaphore()
    for where in places:
        pl.semaphore_signal(barrier, inc=1, device_id=where, device_id_type=MESH_ID)
    pl.semaphore_wait(barrier, len(places))


def seq_gather_start(wires, ref, place):
    me, core, near, far, cross = place
    mine = ref.at[me]
    return wires.copy(mine, mine, {"seq": near}), wires.copy(mine, mine, {"seq": far})


def seq_gather_forward(wires, ref, place, first):
    me, core, near, far, cross = place
    half = ref.shape[1] // 2
    first[0].wait_recv()
    upper = ref.at[near, pl.ds(0, half)]
    one = wires.copy(upper, upper, {"seq": far})
    first[1].wait_recv()
    lower = ref.at[far, pl.ds(half, half)]
    return one, wires.copy(lower, lower, {"seq": near})


def plane_gather_start(wires, ref, place):
    me, core, near, far, cross = place
    mine = ref.at[me, core]
    return (
        wires.copy(mine, mine, {"seq": near}),
        wires.copy(mine, mine, {"seq": far}),
        wires.copy(mine, mine, {"tensor": 1 - core}),
    )


def plane_gather_forward(wires, ref, place, first):
    me, core, near, far, cross = place
    half = ref.shape[2] // 2
    partner = {"tensor": 1 - core}
    first[0].wait_recv()
    upper = ref.at[near, core, pl.ds(0, half)]
    one = wires.copy(upper, upper, {"seq": far})
    first[1].wait_recv()
    lower = ref.at[far, core, pl.ds(half, half)]
    two = wires.copy(lower, lower, {"seq": near})
    block = ref.at[near, core]
    three = wires.copy(block, block, partner)
    block = ref.at[far, core]
    four = wires.copy(block, block, partner)
    return one, two, three, four


def plane_gather_finish(wires, ref, place, first, second):
    me, core, near, far, cross = place
    half = ref.shape[2] // 2
    partner = {"tensor": 1 - core}
    second[0].wait_recv()
    upper = ref.at[cross, core, pl.ds(0, half)]
    one = wires.copy(upper, upper, partner)
    second[1].wait_recv()
    lower = ref.at[cross, core, pl.ds(half, half)]
    two = wires.copy(lower, lower, partner)
    for other in (first[2], second[2], second[3], one, two):
        other.wait_recv()


def wide(values):
    return values.astype(jnp.float32)


def cross_sum(wires, place, total_of, out_refs):
    me, core, near, far, cross = place
    cross_ref, near_ref, far_ref, cross_in, near_in, far_in = out_refs
    half = near_ref.shape[0] // 2
    top, bottom = pl.ds(0, half), pl.ds(half, half)
    cross_ref[...] = total_of(cross).astype(cross_ref.dtype)
    to_near = wires.copy(cross_ref.at[top], cross_in.at[top], {"seq": near})
    to_far = wires.copy(cross_ref.at[bottom], cross_in.at[bottom], {"seq": far})
    near_ref[...] = total_of(near).astype(near_ref.dtype)
    near_one = wires.copy(near_ref.at[top], near_in.at[top], {"seq": near})
    far_ref[...] = total_of(far).astype(far_ref.dtype)
    far_one = wires.copy(far_ref.at[bottom], far_in.at[bottom], {"seq": far})
    own = total_of(me)
    to_near.wait_recv()
    far_ref[top, :] = (wide(far_ref[top, :]) + wide(cross_in[top, :])).astype(far_ref.dtype)
    far_two = wires.copy(far_ref.at[top], far_in.at[top], {"seq": far})
    to_far.wait_recv()
    near_ref[bottom, :] = (wide(near_ref[bottom, :]) + wide(cross_in[bottom, :])).astype(near_ref.dtype)
    near_two = wires.copy(near_ref.at[bottom], near_in.at[bottom], {"seq": near})
    for one in (near_one, far_one, far_two, near_two):
        one.wait_recv()
    return own + wide(near_in[...]) + wide(far_in[...])


def plane_sum(wires, place, part_ref, partner_in, out_refs):
    me, core, near, far, cross = place
    arrivals = {}
    for name, spot in (("cross", cross), ("near", near), ("far", far), ("me", me)):
        arrivals[name] = wires.copy(part_ref.at[spot, 1 - core], partner_in.at[spot], {"tensor": 1 - core})
    order = iter(("cross", "near", "far", "me"))

    def total_of(spot):
        arrivals[next(order)].wait_recv()
        return wide(part_ref[spot, core]) + wide(partner_in[spot])

    return cross_sum(wires, place, total_of, out_refs)


def sum_scratch(piece, width):
    return [pltpu.VMEM((piece, width), jnp.bfloat16)] * 6


def sems(count):
    return [pltpu.SemaphoreType.DMA((count,)), pltpu.SemaphoreType.DMA((count,))]


def plane_peers(place):
    me, core, near, far, cross = place
    return {"seq": near}, {"seq": far}, {"tensor": 1 - core}


def norm_of(values, gain_vec):
    return values * lax.rsqrt(jnp.mean(values * values, axis=-1, keepdims=True) + epsilon) * gain_vec


def norm_back(values, gain_vec, grad):
    inverse = lax.rsqrt(jnp.mean(values * values, axis=-1, keepdims=True) + epsilon)
    unit = values * inverse
    scaled_grad = grad * gain_vec
    gain_grad = jnp.sum(grad * unit, axis=0, keepdims=True)
    return inverse * (scaled_grad - unit * jnp.mean(scaled_grad * unit, axis=-1, keepdims=True)), gain_grad


def dot(left, right):
    return jnp.dot(left, right, preferred_element_type=jnp.float32)


def dot_nt(left, right):
    return lax.dot_general(left, right, NT, preferred_element_type=jnp.float32)


def dot_tn(left, right):
    return lax.dot_general(left, right, TN, preferred_element_type=jnp.float32)


def project_steps(place, x_ref, gain_ref, w_ref, normed_ref, qkv_ref, wires):
    me, core, near, far, cross = place
    normed_ref[me] = norm_of(x_ref[...], gain_ref[...]).astype(jnp.bfloat16)
    first = seq_gather_start(wires, normed_ref, place)
    qkv_ref[me] = dot(normed_ref[me], w_ref[...]).astype(jnp.bfloat16)
    second = seq_gather_forward(wires, normed_ref, place, first)
    qkv_ref[near] = dot(normed_ref[near], w_ref[...]).astype(jnp.bfloat16)
    qkv_ref[far] = dot(normed_ref[far], w_ref[...]).astype(jnp.bfloat16)
    second[0].wait_recv()
    second[1].wait_recv()
    qkv_ref[cross] = dot(normed_ref[cross], w_ref[...]).astype(jnp.bfloat16)


def project_kernel(x_ref, gain_ref, w_ref, routes_ref, normed_ref, qkv_ref, routes_all_ref, send, recv):
    place = plane_place()
    me, core, near, far, cross = place
    wires = Wires(send, recv)
    greet({"seq": near}, {"seq": far}, {"seq": cross})
    routes_all_ref[me] = routes_ref[...]
    picks = [wires.copy(routes_ref, routes_all_ref.at[me], {"seq": spot}) for spot in (near, far, cross)]
    project_steps(place, x_ref, gain_ref, w_ref, normed_ref, qkv_ref, wires)
    for one in picks:
        one.wait_recv()
    wires.finish()


def sum_project_kernel(part_ref, base_ref, gain_ref, w_ref, x_ref, normed_ref, qkv_ref, partner_in, *rest):
    out_refs, (send, recv) = rest[:6], rest[6:]
    place = plane_place()
    wires = Wires(send, recv)
    greet(*plane_peers(place))
    x_ref[...] = base_ref[...] + plane_sum(wires, place, part_ref, partner_in, out_refs)
    project_steps(place, x_ref, gain_ref, w_ref, normed_ref, qkv_ref, wires)
    wires.finish()


def sum_kernel(part_ref, base_ref, x_ref, partner_in, *rest):
    out_refs, (send, recv) = rest[:6], rest[6:]
    place = plane_place()
    wires = Wires(send, recv)
    greet(*plane_peers(place))
    x_ref[...] = base_ref[...] + plane_sum(wires, place, part_ref, partner_in, out_refs)
    wires.finish()


def merge_kernel(mixed_ref, base_ref, w_ref, gain_ref, merged_ref, middle_ref, tokens_ref, send, recv):
    place = plane_place()
    me, core, near, far, cross = place
    wires = Wires(send, recv)
    greet({"seq": near}, {"seq": far}, {"seq": cross}, {"tensor": 1 - core})
    copies = [wires.copy(mixed_ref.at[spot], merged_ref.at[me], {"seq": spot}) for spot in (cross, near, far)]
    merged_ref[me] = mixed_ref[me]
    total = base_ref[...] + dot(mixed_ref[me], w_ref[me])
    for spot, one in ((near, copies[1]), (far, copies[2]), (cross, copies[0])):
        one.wait_recv()
        total = total + dot(merged_ref[spot], w_ref[spot])
    middle_ref[...] = total
    tokens_ref[me, core] = norm_of(total, gain_ref[...]).astype(jnp.bfloat16)
    first = plane_gather_start(wires, tokens_ref, place)
    second = plane_gather_forward(wires, tokens_ref, place, first)
    plane_gather_finish(wires, tokens_ref, place, first, second)
    wires.finish()


def split_kernel(part_ref, middle_ref, gain_ref, grad_ref, w_ref, middle_grad_ref, out_grad_ref, gain_grad_ref, mixed_grad_ref,
                 outgoing, partner_in, *rest):
    out_refs, (send, recv) = rest[:6], rest[6:]
    place = plane_place()
    me, core, near, far, cross = place
    wires = Wires(send, recv)
    greet({"seq": near}, {"seq": far}, {"seq": cross}, {"tensor": 1 - core})
    normed_grad = plane_sum(wires, place, part_ref, partner_in, out_refs)
    part, gain_grad_ref[...] = norm_back(middle_ref[...], gain_ref[...], normed_grad)
    middle_grad = grad_ref[...] + part
    middle_grad_ref[...] = middle_grad
    out_grad_ref[...] = middle_grad.astype(jnp.bfloat16)
    copies = []
    for spot in (cross, near, far):
        outgoing[spot] = dot_nt(out_grad_ref[...], w_ref[spot]).astype(jnp.bfloat16)
        copies.append(wires.copy(outgoing.at[spot], mixed_grad_ref.at[me], {"seq": spot}))
    mixed_grad_ref[me] = dot_nt(out_grad_ref[...], w_ref[me]).astype(jnp.bfloat16)
    for one in copies:
        one.wait_recv()
    wires.finish()


def input_grad_kernel(spread, qkv_grad_ref, w_ref, x_ref, gain_ref, middle_grad_ref, *rest):
    grad_ref, gain_grad_ref = rest[:2]
    rows_ref = rest[2] if spread else None
    rest = rest[3:] if spread else rest[2:]
    out_refs, (send, recv) = rest[:6], rest[6:]
    place = plane_place()
    me, core, near, far, cross = place
    wires = Wires(send, recv)
    greet(*plane_peers(place)[: 3 if spread else 2])
    normed_grad = cross_sum(wires, place, lambda spot: dot_nt(qkv_grad_ref[spot], w_ref[...]), out_refs)
    part, gain_grad_ref[...] = norm_back(x_ref[...], gain_ref[...], normed_grad)
    grad = middle_grad_ref[...] + part
    grad_ref[...] = grad
    if spread:
        rows_ref[me, core] = grad.astype(jnp.bfloat16)
        first = plane_gather_start(wires, rows_ref, place)
        second = plane_gather_forward(wires, rows_ref, place, first)
        plane_gather_finish(wires, rows_ref, place, first, second)
    wires.finish()


def comm_call(kernel, name, number, time, outs, scratch, wire_count, *operands):
    return pl.pallas_call(
        kernel,
        out_shape=tuple(outs),
        in_specs=vmem(len(operands)),
        out_specs=tuple(vmem(len(outs))),
        scratch_shapes=scratch + sems(wire_count),
        compiler_params=pltpu.CompilerParams(collective_id=number, has_side_effects=True),
        cost_estimate=cost(time),
        name=name,
    )(*operands)


def cost(time):
    return pl.CostEstimate(flops=0, bytes_accessed=int(time * 3e6), transcendentals=0)


def low_array(*shape):
    return jax.ShapeDtypeStruct(shape, jnp.bfloat16)


def wide_array(*shape):
    return jax.ShapeDtypeStruct(shape, jnp.float32)


def attend_gather(qkv, seg_row, seg_col, line, rows, qkv_next, out_next, n_tensor, n_dp):
    length, width = qkv.shape
    heads, span = line.shape
    piece, depth = rows.shape
    outs = [low_array(length, heads * HD), wide_array(heads, length, 1), low_array(length // piece, n_tensor, piece, depth),
            low_array(n_dp, *qkv_next.shape), low_array(n_dp, *out_next.shape)]
    return comm_call(functools.partial(attn_fwd_kernel, heads, span, True), "attend_gather", 6, 20.0, outs,
                     attend_scratch(heads, length, span), 9 + 4 * (n_dp - 1), qkv, seg_row, seg_col, line, rows, qkv_next, out_next)


def gelu_parts(values):
    square = values * values
    inner = jnp.tanh(values * (0.7978845608028654 + (0.7978845608028654 * 0.044715) * square))
    lift = 0.5 + 0.5 * inner
    slope = lift + (0.5 * values) * (1.0 - inner * inner) * (0.7978845608028654 + (3.0 * 0.7978845608028654 * 0.044715) * square)
    return values * lift, slope


def slot_hot(slot_row, capacity):
    rows = lax.broadcasted_iota(jnp.int32, (capacity, slot_row.shape[1]), 0)
    return (rows == slot_row).astype(jnp.bfloat16)


def experts_kernel(tokens_ref, slot_ref, chosen_ref, own_ref, router_ref, up_ref, down_ref, part_ref, slots_ref, pre_ref, shares_ref):
    capacity = slots_ref.shape[0]
    tokens = tokens_ref[...]
    logits = jnp.where(chosen_ref[...] > 0, dot_nt(tokens, router_ref[...]), negative)
    raised = jnp.exp(logits - jnp.max(logits, axis=1, keepdims=True))
    shares = raised / jnp.sum(raised, axis=1, keepdims=True)
    shares_ref[...] = shares
    own_share = jnp.sum(shares * own_ref[...], axis=1, keepdims=True)
    hot = slot_hot(slot_ref[...], capacity)
    slots = dot(hot, tokens).astype(jnp.bfloat16)
    slots_ref[...] = slots
    pre = dot(slots, up_ref[...])
    pre_ref[...] = pre.astype(jnp.bfloat16)
    hidden = gelu_parts(pre)[0].astype(jnp.bfloat16)
    result = dot_nt(hidden, down_ref[...]).astype(jnp.bfloat16)
    part_ref[...] = (own_share * dot_tn(hot, result)).astype(jnp.bfloat16)


def experts_back_kernel(rows_ref, tokens_ref, slot_ref, shares_ref, own_ref, router_ref, up_ref, down_ref, slots_ref, pre_ref,
                        part_ref, up_grad_ref, down_grad_ref, router_grad_ref, up_acc, down_acc):
    group = pl.program_id(0)

    @pl.when(group == 0)
    def _():
        up_acc[...] = jnp.zeros_like(up_acc)
        down_acc[...] = jnp.zeros_like(down_acc)
        router_grad_ref[...] = jnp.zeros_like(router_grad_ref)

    capacity = slots_ref.shape[0]
    shares = shares_ref[...]
    own = own_ref[...]
    own_share = jnp.sum(shares * own, axis=1, keepdims=True)
    hot = slot_hot(slot_ref[...], capacity)
    scaled_rows = (own_share * rows_ref[...].astype(jnp.float32)).astype(jnp.bfloat16)
    result_grad = dot(hot, scaled_rows).astype(jnp.bfloat16)
    hidden_grad = dot(result_grad, down_ref[...])
    hidden, slope = gelu_parts(pre_ref[...].astype(jnp.float32))
    pre_grad = (slope * hidden_grad).astype(jnp.bfloat16)
    pair_sum = jnp.sum(hidden * hidden_grad, axis=1, keepdims=True)
    down_acc[...] += dot_tn(result_grad, hidden.astype(jnp.bfloat16))
    up_acc[...] += dot_tn(slots_ref[...], pre_grad)
    slot_grad = dot_nt(pre_grad, up_ref[...]).astype(jnp.bfloat16)
    high = pair_sum.astype(jnp.bfloat16)
    rest = (pair_sum - high.astype(jnp.float32)).astype(jnp.bfloat16)
    token_pair = dot_tn(hot, jnp.concatenate([jnp.broadcast_to(high, (capacity, 128)), jnp.broadcast_to(rest, (capacity, 128))], axis=1))
    token_pair = token_pair[:, :1] + token_pair[:, 128:129]
    logit_grad = (token_pair * (own - shares)).astype(jnp.bfloat16)
    router_grad_ref[...] += dot_tn(logit_grad, tokens_ref[...])
    part_ref[...] = (dot_tn(hot, slot_grad) + dot(logit_grad, router_ref[...])).astype(jnp.bfloat16)

    @pl.when(group == pl.num_programs(0) - 1)
    def _():
        up_grad_ref[...] = up_acc[...].astype(jnp.bfloat16)
        down_grad_ref[...] = down_acc[...].astype(jnp.bfloat16)


def by_group(*shape):
    return pl.BlockSpec((None,) + shape, lambda g: (g,) + (0,) * len(shape))


def held(*shape):
    return pl.BlockSpec(shape, lambda g: (0,) * len(shape), pipeline_mode=pl.Buffered(1))


def run_experts(tokens, slot, chosen, own, router, up, down, capacity):
    groups, rows, width = tokens.shape
    experts, wide_ff = router.shape[0], up.shape[1]
    return pl.pallas_call(
        experts_kernel,
        grid=(groups,),
        out_shape=(low_array(groups, rows, width), low_array(groups, capacity, width), low_array(groups, capacity, wide_ff),
                   wide_array(groups, rows, experts)),
        in_specs=[by_group(rows, width), by_group(1, rows), by_group(rows, experts), held(1, experts), held(experts, width),
                  held(width, wide_ff), held(width, wide_ff)],
        out_specs=(by_group(rows, width), by_group(capacity, width), by_group(capacity, wide_ff), by_group(rows, experts)),
        compiler_params=pltpu.CompilerParams(dimension_semantics=("arbitrary",)),
        cost_estimate=cost(14.0),
        name="experts",
    )(tokens, slot, chosen, own, router, up, down)


def run_experts_back(rows_grad, tokens, slot, shares, own, router, up, down, slots, pre):
    groups, rows, width = tokens.shape
    experts, wide_ff = router.shape[0], up.shape[1]
    capacity = slots.shape[1]
    return pl.pallas_call(
        experts_back_kernel,
        grid=(groups,),
        out_shape=(low_array(groups, rows, width), low_array(width, wide_ff), low_array(width, wide_ff), wide_array(experts, width)),
        in_specs=[by_group(rows, width), by_group(rows, width), by_group(1, rows), by_group(rows, experts), held(1, experts),
                  held(experts, width), held(width, wide_ff), held(width, wide_ff), by_group(capacity, width), by_group(capacity, wide_ff)],
        out_specs=(by_group(rows, width), held(width, wide_ff), held(width, wide_ff), held(experts, width)),
        scratch_shapes=[pltpu.VMEM((width, wide_ff), jnp.float32), pltpu.VMEM((width, wide_ff), jnp.float32)],
        compiler_params=pltpu.CompilerParams(dimension_semantics=("arbitrary",)),
        cost_estimate=cost(26.0),
        name="experts_back",
    )(rows_grad, tokens, slot, shares, own, router, up, down, slots, pre)


def dp_peers():
    me, count = lax.axis_index("dp"), lax.axis_size("dp")
    return me, [lax.rem(me + step, count) for step in range(1, count)], [lax.rem(me + count - step, count) for step in range(1, count)]


def line_start(wires, own_ref, all_ref, core, me, targets):
    half = own_ref.at[core]
    copies = [wires.copy(half, all_ref.at[me, core], {"dp": spot}) for spot in targets]
    all_ref[me] = own_ref[...]
    return copies


def line_forward(wires, all_ref, core, copies, sources):
    onward = []
    for one, spot in zip(copies, sources):
        one.wait_recv()
        block = all_ref.at[spot, core]
        onward.append(wires.copy(block, block, {"tensor": 1 - core}))
    return onward


def weights_kernel(small_ref, qkv_ref, out_ref, small_all, qkv_all, out_all, send, recv):
    core = lax.axis_index("tensor")
    me, targets, sources = dp_peers()
    wires = Wires(send, recv)
    greet(*[{"dp": spot} for spot in targets], {"tensor": 1 - core})
    smalls = [wires.copy(small_ref, small_all.at[me], {"dp": spot}) for spot in targets]
    small_all[me] = small_ref[...]
    qkvs = line_start(wires, qkv_ref, qkv_all, core, me, targets)
    outs = line_start(wires, out_ref, out_all, core, me, targets)
    onward = line_forward(wires, qkv_all, core, qkvs, sources)
    onward += line_forward(wires, out_all, core, outs, sources)
    for one in smalls + onward:
        one.wait_recv()
    wires.finish()


def reduce_kernel(layers, *refs):
    q_refs, o_refs = refs[:layers], refs[layers : 2 * layers]
    refs = refs[2 * layers :]
    q_outs, o_outs = refs[:layers], refs[layers : 2 * layers]
    refs = refs[2 * layers :]
    scratch = [refs[6 * layer : 6 * layer + 6] for layer in range(layers)]
    send, recv = refs[6 * layers :]
    place = plane_place()
    me, core, near, far, cross = place
    others = (cross, near, far)
    line_me, targets, sources = dp_peers()
    wires = Wires(send, recv)
    partner = {"tensor": 1 - core}
    greet({"seq": near}, {"seq": far}, {"seq": cross}, partner, *[{"dp": spot} for spot in targets])
    n_dp = len(targets) + 1
    first = []
    for layer in range(layers):
        q_in, q_sum, q_line, o_in, o_seq, o_line = scratch[layer]
        first.append((wires.copy(q_refs[layer].at[1 - core], q_in, partner), wires.copy(o_refs[layer].at[1 - core], o_in, partner)))
    q_copies, o_copies = [], []
    for layer in range(layers):
        q_in, q_sum, q_line, o_in, o_seq, o_line = scratch[layer]
        q_ref, o_ref = q_refs[layer], o_refs[layer]
        first[layer][0].wait_recv()
        q_sum[...] = (wide(q_ref[core]) + wide(q_in[...])).astype(jnp.bfloat16)
        q_copies.append([wires.copy(q_sum.at[spot], q_line.at[line_me], {"dp": spot}) for spot in targets])
        q_line[line_me] = q_sum[line_me]
        first[layer][1].wait_recv()
        o_in[...] = (wide(o_ref[core]) + wide(o_in[...])).astype(jnp.bfloat16)
        o_copies.append([wires.copy(o_in.at[spot], o_seq.at[me], {"seq": spot}) for spot in others])
        o_seq[me] = o_in[me]
    line_copies, last = [], []
    for layer in range(layers):
        q_in, q_sum, q_line, o_in, o_seq, o_line = scratch[layer]
        for one in o_copies[layer]:
            one.wait_recv()
        o_seq[me] = (wide(o_seq[0]) + wide(o_seq[1]) + wide(o_seq[2]) + wide(o_seq[3])).astype(jnp.bfloat16)
        line_copies.append([wires.copy(o_seq.at[me, spot], o_line.at[line_me], {"dp": spot}) for spot in targets])
        o_line[line_me] = o_seq[me, line_me]
    for layer in range(layers):
        q_in, q_sum, q_line, o_in, o_seq, o_line = scratch[layer]
        for refs_in, copies, out in ((q_line, q_copies[layer], q_outs[layer]), (o_line, line_copies[layer], o_outs[layer])):
            for one in copies:
                one.wait_recv()
            total = wide(refs_in[0])
            for spot in range(1, n_dp):
                total = total + wide(refs_in[spot])
            out[core, me] = total.astype(jnp.bfloat16)
            mine = out.at[core, me]
            last.append((out, [wires.copy(mine, mine, {"seq": spot}) for spot in others], [wires.copy(mine, mine, partner)]))
    for out, copies, onward in last:
        for one, spot in zip(copies, others):
            one.wait_recv()
            block = out.at[core, spot]
            onward.append(wires.copy(block, block, partner))
    for out, copies, onward in last:
        for one in onward:
            one.wait_recv()
    wires.finish()


def share_kernel(count, *refs):
    in_refs, out_refs, (send, recv) = refs[:count], refs[count : 2 * count], refs[2 * count :]
    place = plane_place()
    wires = Wires(send, recv)
    greet({"seq": place[2]}, {"seq": place[3]})
    first, second = [], []
    for src, dst in zip(in_refs, out_refs):
        dst[place[0]] = src[...]
        first.append(seq_gather_start(wires, dst, place))
    for dst, one in zip(out_refs, first):
        second.extend(seq_gather_forward(wires, dst, place, one))
    for one in second:
        one.wait_recv()
    wires.finish()
def body(
    block_input,
    segments,
    routes,
    distance_bucket,
    first_gain,
    query_key_value,
    attention_out,
    bias_table,
    second_gain,
    router_weights,
    expert_up,
    expert_down,
    cotangent,
):
    low = jnp.bfloat16
    seq_count, piece, width = block_input.shape
    n_dp, n_seq, n_tensor = (lax.axis_size(name) for name in ("dp", "seq", "tensor"))
    n_plane = n_seq * n_tensor
    length = piece * n_seq
    local_heads = HEADS // n_seq
    head_width = local_heads * HD
    experts = expert_up.shape[1]
    assert seq_count == 1 and experts == n_seq
    shard = width // n_dp
    bucket_count = bias_table.shape[1] * n_dp
    bucket_shard = bias_table.shape[1]
    group_rows = n_tensor * piece
    capacity = group_rows * routes.shape[-1] // experts
    seq_index = lax.axis_index("seq")
    span = ROWS + length // 2


    assert n_seq == 4 and n_tensor == 2
    half = shard // n_tensor

    def padded(values):
        return jnp.pad(values, ((0, 0), (0, shard - values.shape[1])))

    small = jnp.concatenate(
        [
            first_gain,
            second_gain,
            router_weights.swapaxes(1, 2).reshape(-1, shard),
            padded(bias_table.reshape(LAYERS, -1)),
        ]
    )
    small_rows = small.shape[0]
    small = jnp.pad(small, ((0, -small_rows % 16), (0, 0)))
    own_qkv = lax.dynamic_index_in_dim(
        query_key_value.reshape(LAYERS, shard, 3, n_seq, head_width), seq_index, 3, keepdims=False
    ).reshape(LAYERS, n_tensor, half, 3 * head_width)
    own_out = attention_out.reshape(LAYERS, n_tensor, half, width)
    own_up = lax.dynamic_index_in_dim(expert_up, seq_index, 1, keepdims=False)
    own_down = lax.dynamic_index_in_dim(expert_down, seq_index, 1, keepdims=False).swapaxes(1, 2)

    def expert_weights(layer):
        up = lax.all_gather(own_up[layer], "dp", axis=0, tiled=True)
        down = lax.all_gather(own_down[layer], "dp", axis=0, tiled=True)
        return up, down

    small_all, qkv_all, out_all = comm_call(
        weights_kernel, "weights", 10, 25.0,
        [low_array(n_dp, *small.shape), low_array(n_dp, *own_qkv.shape[1:]), low_array(n_dp, *own_out.shape[1:])], [], 5 * (n_dp - 1),
        small, own_qkv[0], own_out[0]
    )
    qkv_weights, out_weights = [qkv_all], [out_all]
    whole_rows = small_all.swapaxes(0, 1).reshape(-1, width)
    gains = whole_rows[: 2 * LAYERS].astype(jnp.float32).reshape(2, LAYERS, 1, width)
    routers = whole_rows[2 * LAYERS : 2 * LAYERS + LAYERS * experts].reshape(LAYERS, experts, width)
    tables = whole_rows[2 * LAYERS + LAYERS * experts : small_rows].reshape(LAYERS, n_dp, shard)[:, :, : bucket_shard * HEADS]
    tables = tables.reshape(LAYERS, bucket_count, HEADS).astype(jnp.float32)
    own_tables = lax.dynamic_slice_in_dim(tables, seq_index * local_heads, local_heads, 2)
    routes_own = routes.reshape(-1, 128)
    seg_row = segments
    seg_col = segments.reshape(length, 1)
    bucket_line = distance_bucket[length // 2 - 1 :: -1][: length // 2]
    bucket_line = jnp.concatenate(
        [jnp.full((1,), -1, jnp.int32), bucket_line, jnp.full((span - 1 - length // 2,), -1, jnp.int32)]
    )
    line_hot = (bucket_line[None, :] == lax.iota(jnp.int32, bucket_count)[:, None]).astype(jnp.float32)
    lines = jnp.einsum("lbh,bs->lhs", own_tables, line_hot, precision=highest_precision)
    strict_upper = (
        lax.iota(jnp.int32, group_rows)[:, None] < lax.iota(jnp.int32, group_rows)[None, :]
    ).astype(low)

    own_hot = (lax.iota(jnp.int32, experts) == seq_index).astype(jnp.float32)[None]

    current = block_input[0]
    grad = cotangent[0]
    saved = []
    for layer in range(LAYERS):
        up, down = expert_weights(layer)
        gain_one, gain_two = gains[0, layer], gains[1, layer]
        qkv_weight = qkv_weights[layer].reshape(width, 3 * head_width)
        out_weight = out_weights[layer].reshape(n_seq, head_width, width)
        outs = [low_array(n_seq, piece, width), low_array(n_seq, piece, 3 * head_width)]
        if layer == 0:
            outs.append(jax.ShapeDtypeStruct((n_seq,) + routes_own.shape, jnp.int32))
            normed_all, qkv, routes_all = comm_call(
                project_kernel, "project", 1, 16.0, outs, [], 7, current, gain_one, qkv_weight, routes_own
            )
            routes_all = jnp.moveaxis(routes_all.reshape((n_seq,) + routes.shape), 0, 1).reshape(LAYERS, n_seq, group_rows, -1)
            mine = jnp.any(routes_all == seq_index, axis=-1)
            slot = dot(mine.reshape(-1, group_rows).astype(low), strict_upper).astype(jnp.int32).reshape(mine.shape)
            slot = jnp.where(mine & (slot < capacity), slot, -1)[:, :, None]
            chosen = jnp.any(routes_all[..., None] == lax.iota(jnp.int32, experts), axis=3).astype(jnp.float32)
        else:
            current, normed_all, qkv = comm_call(
                sum_project_kernel, "sum_project", 2, 32.0, [wide_array(piece, width)] + outs,
                [pltpu.VMEM((n_seq, piece, width), low)] + sum_scratch(piece, width), 14, part, middle, gain_one, qkv_weight
            )
        qkv = qkv.reshape(length, 3 * head_width)
        if layer == 0:
            mixed, log_total, grad_rows, qkv_all, out_all = attend_gather(
                qkv, seg_row, seg_col, lines[layer], grad, own_qkv[1], own_out[1], n_tensor, n_dp
            )
            qkv_weights.append(qkv_all)
            out_weights.append(out_all)
        else:
            mixed, log_total = attend(qkv, seg_row, seg_col, lines[layer])
        merged, middle, tokens = comm_call(
            merge_kernel, "merge", 3, 21.0,
            [low_array(n_seq, piece, head_width), wide_array(piece, width), low_array(n_seq, n_tensor, piece, width)], [], 12,
            mixed.reshape(n_seq, piece, head_width), current, out_weight, gain_two
        )
        tokens = tokens.reshape(n_seq, group_rows, width)
        part, slots, pre, shares = run_experts(tokens, slot[layer], chosen[layer], own_hot, routers[layer], up, down, capacity)
        part = part.reshape(n_seq, n_tensor, piece, width)
        saved.append((current, normed_all, qkv, log_total, merged, middle, tokens, shares, slots, pre, qkv_weight, out_weight, up, down))

    (block_output,) = comm_call(
        sum_kernel, "sum_last", 4, 16.0, [wide_array(piece, width)], [pltpu.VMEM((n_seq, piece, width), low)] + sum_scratch(piece, width),
        10, part, middle
    )

    def shard_sum(values):
        return lax.psum_scatter(values, "dp", scatter_dimension=0, tiled=True)

    up_shards, down_shards, qkv_grads, out_grads = ([None] * LAYERS for _ in range(4))
    out_rows = half // n_seq
    packed_rows = -(-(out_rows + 1) // 16) * 16
    for layer in range(LAYERS - 1, -1, -1):
        (layer_in, normed_all, qkv, log_total, merged, middle, tokens, shares, slots, pre, qkv_weight, out_weight, up, down) = saved[layer]
        gain_one, gain_two = gains[0, layer], gains[1, layer]
        part, up_grad, down_grad, router_grad = run_experts_back(
            grad_rows.reshape(n_seq, group_rows, width), tokens, slot[layer], shares, own_hot, routers[layer], up, down, slots, pre
        )
        down_shards[layer] = shard_sum(down_grad)
        up_shards[layer] = shard_sum(up_grad)
        middle_grad, out_grad, gain_two_grad, mixed_grad = comm_call(
            split_kernel, "split", 5, 22.0,
            [wide_array(piece, width), low_array(piece, width), wide_array(1, width), low_array(n_seq, piece, head_width)],
            [pltpu.VMEM((n_seq, piece, head_width), low), pltpu.VMEM((n_seq, piece, width), low)] + sum_scratch(piece, width), 13,
            part.reshape(n_seq, n_tensor, piece, width), middle, gain_two, grad, out_weight
        )
        out_weight_grad = jnp.einsum("gtd,te->gde", merged, out_grad, preferred_element_type=jnp.float32)
        operands = (qkv, seg_row, seg_col, lines[layer], log_total, mixed_grad.reshape(length, head_width))
        if layer == 0:
            qkv_grad, band, up_last = attend_back(*operands, up_shards[1])
        else:
            qkv_grad, band = attend_back(*operands)
        qkv_weight_grad = dot_tn(normed_all.reshape(length, width), qkv_grad)
        spread = layer > 0
        outs = [wide_array(piece, width), wide_array(1, width)]
        outs += [low_array(n_seq, n_tensor, piece, width)] if spread else []
        outs = comm_call(
            functools.partial(input_grad_kernel, spread), "input_grad_spread" if spread else "input_grad", 7 + spread, 32.0 if spread else 16.0,
            outs, sum_scratch(piece, width), 15, qkv_grad.reshape(n_seq, piece, -1), qkv_weight, layer_in, gain_one, middle_grad
        )
        grad, gain_one_grad = outs[:2]
        grad_rows = outs[2] if spread else None
        table_grad = jnp.dot(line_hot, band.T, precision=highest_precision)
        table_grad = lax.dynamic_update_slice_in_dim(
            jnp.zeros((bucket_count, HEADS), jnp.float32), table_grad, seq_index * local_heads, 1
        )
        table_grad = padded(table_grad.reshape(n_dp, -1)).reshape(1, width)
        packed = jnp.concatenate([gain_one_grad, gain_two_grad, router_grad, table_grad, jnp.zeros((1, width), jnp.float32)])
        packed = packed.reshape(n_plane, n_dp, shard).swapaxes(0, 1)[:, :, None]
        packed = jnp.pad(packed, ((0, 0), (0, 0), (0, packed_rows - out_rows - 1), (0, width - shard)))
        both = jnp.concatenate([out_weight_grad.reshape(n_dp, n_plane, out_rows, width), packed], axis=2).astype(low)
        out_grads[layer] = both.reshape(n_dp, n_tensor, n_seq, packed_rows, width).transpose(1, 2, 0, 3, 4)
        qkv_grads[layer] = qkv_weight_grad.astype(low).reshape(n_dp, n_tensor, half, 3 * head_width).swapaxes(0, 1)

    down_last = lax.all_gather(down_shards[1], "seq", axis=0)
    q_lines = [pltpu.VMEM((n_dp, half, 3 * head_width), low)] * 3
    o_blocks = [
        pltpu.VMEM((n_seq, n_dp, packed_rows, width), low),
        pltpu.VMEM((n_seq, n_dp, packed_rows, width), low),
        pltpu.VMEM((n_dp, packed_rows, width), low),
    ]
    totals = comm_call(
        functools.partial(reduce_kernel, LAYERS), "reduce_grads", 11, 40.0,
        [low_array(n_tensor, n_seq, half, 3 * head_width)] * LAYERS + [low_array(n_tensor, n_seq, packed_rows, width)] * LAYERS,
        (q_lines + o_blocks) * LAYERS, LAYERS * (2 * (n_dp - 1) + 19), *qkv_grads, *out_grads
    )
    up_first, down_first = comm_call(
        functools.partial(share_kernel, 2), "share", 12, 38.0, [low_array(n_seq, shard, up.shape[1])] * 2, [], 8, up_shards[0], down_shards[0]
    )
    qkv_total = jnp.stack(totals[:LAYERS]).astype(jnp.float32).reshape(LAYERS, n_tensor, n_seq, half, 3, head_width)
    qkv_total = qkv_total.transpose(0, 1, 3, 4, 2, 5).reshape(LAYERS, shard, 3 * width)
    both = jnp.stack(totals[LAYERS:]).astype(jnp.float32).reshape(LAYERS, n_plane, packed_rows, width)
    out_total = both[:, :, :out_rows].reshape(LAYERS, shard, width)
    small = both[:, :, out_rows, :shard]
    router_total = small[:, 2 : 2 + experts].swapaxes(1, 2)
    table_total = small[:, 2 + experts, : bucket_shard * HEADS].reshape(LAYERS, bucket_shard, HEADS)
    up_total = jnp.stack([up_first, up_last]).astype(jnp.float32)
    down_total = jnp.stack([down_first, down_last]).astype(jnp.float32).swapaxes(2, 3)
    return (block_output[None], grad[None], small[:, 0], qkv_total, out_total, table_total, small[:, 1], router_total, up_total, down_total)


def solution(mesh):
    in_specs = (
        P(("dp", "tensor"), "seq", None),
        P(("dp", "tensor"), None),
        P(None, "dp", "seq", None),
        P(),
        P(None, "dp"),
        P(None, "dp", None),
        P(None, "dp", None),
        P(None, "dp", None),
        P(None, "dp"),
        P(None, "dp", None),
        P(None, None, "dp", "tensor"),
        P(None, None, "tensor", "dp"),
        P(("dp", "tensor"), "seq", None),
    )
    out_specs = (
        P(("dp", "tensor"), "seq", None),
        P(("dp", "tensor"), "seq", None),
        P(None, "dp"),
        P(None, "dp", None),
        P(None, "dp", None),
        P(None, "dp", None),
        P(None, "dp"),
        P(None, "dp", None),
        P(None, None, "dp", "tensor"),
        P(None, None, "tensor", "dp"),
    )
    return jax.shard_map(body, mesh=mesh, in_specs=in_specs, out_specs=out_specs, check_vma=False)
```

```python
import functools

import jax
import jax.numpy as jnp
from jax import lax
from jax.experimental import pallas as pl
from jax.experimental.pallas import tpu as pltpu
from jax.sharding import PartitionSpec as P

HEADS = 12
LAYERS = 2
epsilon = 1e-06
negative = -1e30
highest_precision = lax.Precision.HIGHEST


def scaled(values, gain_vec):
    return values * lax.rsqrt(jnp.mean(values * values, axis=-1, keepdims=True) + epsilon) * gain_vec


HD = 64
ROWS = 128
NT = (((1,), (1,)), ((), ()))
TN = (((0,), (0,)), ((), ()))


def visit_blocks(length, span, one_block, hook, hooks_at):
    full, count = span // ROWS, length // ROWS

    def step(i, carry):
        start = pl.multiple_of(i * ROWS, ROWS)
        one_block(start, pl.multiple_of(start + ROWS - span, ROWS), span)
        return carry

    for i in range(full - 1):
        if i in hooks_at:
            hook()
        one_block(i * ROWS, 0, (i + 1) * ROWS)
    stops = [full - 1] + [i for i in range(full - 1, count) if i in hooks_at] + [count]
    for low, high in zip(stops, stops[1:]):
        if low in hooks_at:
            hook()
        lax.fori_loop(low, high, step, 0)


def background(tasks):
    tasks = list(tasks)

    def hook():
        tasks[:] = [task for task in tasks if next(task, wires_done) is not wires_done]

    return hook, lambda: run_all(*tasks)


def fill_mask(mask_ref, segr_ref, segc_ref, start, low, width):
    same = segc_ref[pl.ds(start, ROWS), :] == segr_ref[:, pl.ds(low, width)]
    back = lax.broadcasted_iota(jnp.int32, (ROWS, width), 0) + (width - ROWS)
    allowed = same & (back >= lax.broadcasted_iota(jnp.int32, (ROWS, width), 1))
    mask_ref[:, :width] = jnp.where(allowed, 0.0, -1e30)


def fill_slab(slab_ref, line_ref, heads, span):
    for h in range(heads):
        spread = jnp.broadcast_to(line_ref[h : h + 1, :], (ROWS, span))
        slab_ref[h] = pltpu.roll(spread, 0, 1, stride=1, stride_axis=0)


def split_heads(qkv_ref, parts_ref, heads):
    for h in range(3 * heads):
        part = qkv_ref[:, h * HD : (h + 1) * HD]
        parts_ref[h] = part * jnp.bfloat16(0.125) if h < heads else part


def fetch_steps(wires, place, own, whole):
    me, core, near, far, cross = place
    width = whole.shape[-1]
    columns = pl.ds(pl.multiple_of(core * (width // 2), width // 2), width // 2)
    around = [wires.copy(own, whole.at[:, me, :, columns], {"seq": spot}) for spot in (cross, near, far)]
    whole[:, me, :, columns] = own[...]
    yield
    for one in around:
        one.wait_recv()
    block = whole.at[:, :, :, columns]
    onward = wires.copy(block, block, {"tensor": 1 - core})
    yield
    onward.wait_recv()


def attn_fwd_kernel(heads, span, mode, *refs):
    qkv_ref, segr_ref, segc_ref, line_ref = refs[:4]
    place = plane_place()
    me, core, near, far, cross = place
    wires = Wires(*refs[-2:])
    if mode == "fetch":
        own_refs, (out_ref, lse_ref), whole_refs, scratch = refs[4:6], refs[6:8], refs[8:10], refs[10:14]
        greet({"seq": near}, {"seq": far}, {"seq": cross}, {"tensor": 1 - core})
        tasks = [fetch_steps(wires, place, *pair) for pair in zip(own_refs, whole_refs)]
        hooks_at = (6,)
    else:
        rows_ref, out_ref, lse_ref, gathered_ref = refs[4:8]
        scratch = refs[8:12]
        greet(*plane_peers(place))
        gathered_ref[me, core] = rows_ref[...].astype(jnp.bfloat16)
        tasks = [gather_steps(wires, gathered_ref, place, True)]
        hooks_at = (4, 6)
    hook, finish = background(tasks)
    hook()
    parts_ref, mixed_ref, slab_ref, mask_ref = scratch
    length = qkv_ref.shape[0]
    fill_slab(slab_ref, line_ref, heads, span)
    split_heads(qkv_ref, parts_ref, heads)

    def one_block(start, low, width):
        fill_mask(mask_ref, segr_ref, segc_ref, start, low, width)

        def one_head(h, carry):
            q = parts_ref[h, pl.ds(start, ROWS), :]
            k = parts_ref[heads + h, pl.ds(low, width), :]
            v = parts_ref[2 * heads + h, pl.ds(low, width), :]
            s = lax.dot_general(q, k, NT, preferred_element_type=jnp.float32)
            s = s + slab_ref[h, :, span - width :] + mask_ref[:, :width]
            top = jnp.max(s, axis=1, keepdims=True)
            e = jnp.exp(s - top)
            total = jnp.sum(e, axis=1, keepdims=True)
            mixed = jnp.dot(e.astype(jnp.bfloat16), v, preferred_element_type=jnp.float32)
            mixed_ref[h, pl.ds(start, ROWS), :] = (mixed / total).astype(jnp.bfloat16)
            lse_ref[h, pl.ds(start, ROWS), :] = top + jnp.log(total)
            return carry

        lax.fori_loop(0, heads, one_head, 0)

    visit_blocks(length, span, one_block, hook, hooks_at)
    out_ref[...] = jnp.concatenate([mixed_ref[h] for h in range(heads)], axis=1)
    finish()
    wires.finish()


def attn_bwd_kernel(heads, span, mode, *refs):
    qkv_ref, segr_ref, segc_ref, line_ref, lse_ref, grad_ref = refs[:6]
    place = plane_place()
    me, core, near, far, cross = place
    wires = Wires(*refs[-2:])
    if mode == "share":
        shard_ref, out_ref, band_ref, shared_ref = refs[6:10]
        greet({"seq": near}, {"seq": far})
        shared_ref[me] = shard_ref[...]
        tasks = [gather_steps(wires, shared_ref, place, False)]
        refs = refs[10:18]
    else:
        part_ref, base_ref, out_ref, band_ref, total_ref = refs[6:11]
        greet(*plane_peers(place))
        tasks = [plane_sum_steps(wires, place, part_ref, refs[19], refs[20:26], add_to(total_ref, base_ref))]
        refs = refs[11:19]
    hook, finish = background(tasks)
    hook()
    parts_ref, gparts_ref, qgrad_ref, kgrad_ref, vgrad_ref, slab_ref, mask_ref, band_acc = refs
    length = qkv_ref.shape[0]
    fill_slab(slab_ref, line_ref, heads, span)
    split_heads(qkv_ref, parts_ref, heads)
    for h in range(heads):
        gparts_ref[h] = grad_ref[:, h * HD : (h + 1) * HD]
    kgrad_ref[...] = jnp.zeros_like(kgrad_ref)
    vgrad_ref[...] = jnp.zeros_like(vgrad_ref)
    band_acc[...] = jnp.zeros_like(band_acc)

    def one_block(start, low, width):
        fill_mask(mask_ref, segr_ref, segc_ref, start, low, width)

        def one_head(h, carry):
            rows = pl.ds(start, ROWS)
            window = pl.ds(low, width)
            q = parts_ref[h, rows, :]
            k = parts_ref[heads + h, window, :]
            v = parts_ref[2 * heads + h, window, :]
            grad = gparts_ref[h, rows, :]
            s = lax.dot_general(q, k, NT, preferred_element_type=jnp.float32)
            s = s + slab_ref[h, :, span - width :] + mask_ref[:, :width]
            p = jnp.exp(s - lse_ref[h, rows, :])
            dp = lax.dot_general(grad, v, NT, preferred_element_type=jnp.float32)
            inner = jnp.sum(p * dp, axis=1, keepdims=True)
            ds = p * (dp - inner)
            band_acc[h, :, span - width :] += ds
            ds = ds.astype(jnp.bfloat16)
            qgrad = jnp.dot(ds, k, preferred_element_type=jnp.float32)
            qgrad_ref[h, rows, :] = (qgrad * 0.125).astype(jnp.bfloat16)
            kgrad_ref[h, window, :] += lax.dot_general(ds, q, TN, preferred_element_type=jnp.float32)
            vgrad_ref[h, window, :] += lax.dot_general(p.astype(jnp.bfloat16), grad, TN, preferred_element_type=jnp.float32)
            return carry

        lax.fori_loop(0, heads, one_head, 0)

    visit_blocks(length, span, one_block, hook, (5, 7) if mode == "share" else (3, 6))
    parts = [qgrad_ref[h] for h in range(heads)]
    parts += [kgrad_ref[h].astype(jnp.bfloat16) for h in range(heads)]
    parts += [vgrad_ref[h].astype(jnp.bfloat16) for h in range(heads)]
    out_ref[...] = jnp.concatenate(parts, axis=1)
    row = lax.broadcasted_iota(jnp.int32, (ROWS, span), 0)
    for h in range(heads):
        acc = band_acc[h]
        bit = 1
        while bit < ROWS:
            acc = jnp.where((row & bit) != 0, pltpu.roll(acc, span - bit, 1), acc)
            bit *= 2
        band_ref[h : h + 1, :] = jnp.sum(acc, axis=0, keepdims=True)
    finish()
    wires.finish()


def vmem(count):
    return [pl.BlockSpec(memory_space=pltpu.VMEM)] * count


def attend_scratch(heads, length, span):
    return [
        pltpu.VMEM((3 * heads, length, HD), jnp.bfloat16),
        pltpu.VMEM((heads, length, HD), jnp.bfloat16),
        pltpu.VMEM((heads, ROWS, span), jnp.float32),
        pltpu.VMEM((ROWS, span), jnp.float32),
    ]


def attend(qkv, seg_row, seg_col, line, extra, extra_outs, mode, number, wire_count):
    length, width = qkv.shape
    heads, span = line.shape
    outs = [low_array(length, heads * HD), wide_array(heads, length, 1)] + extra_outs
    return comm_call(functools.partial(attn_fwd_kernel, heads, span, mode), "attend_" + mode, number, 18.0, outs,
                     attend_scratch(heads, length, span), wire_count, qkv, seg_row, seg_col, line, *extra)


def attend_back(qkv, seg_row, seg_col, line, lse, grad, extra, extra_outs, extra_scratch, mode, number, wire_count):
    length, width = qkv.shape
    heads, span = line.shape
    outs = [low_array(length, width), wide_array(heads, span)] + extra_outs
    scratch = [
        pltpu.VMEM((3 * heads, length, HD), jnp.bfloat16),
        pltpu.VMEM((heads, length, HD), jnp.bfloat16),
        pltpu.VMEM((heads, length, HD), jnp.bfloat16),
        pltpu.VMEM((heads, length, HD), jnp.float32),
        pltpu.VMEM((heads, length, HD), jnp.float32),
        pltpu.VMEM((heads, ROWS, span), jnp.float32),
        pltpu.VMEM((ROWS, span), jnp.float32),
        pltpu.VMEM((heads, ROWS, span), jnp.float32),
    ]
    return comm_call(functools.partial(attn_bwd_kernel, heads, span, mode), "attend_back_" + mode, number, 23.0, outs,
                     scratch + extra_scratch, wire_count, qkv, seg_row, seg_col, line, lse, grad, *extra)


MESH_ID = pl.DeviceIdType.MESH


class Wires:
    def __init__(self, send, recv):
        self.send, self.recv, self.next, self.started = send, recv, 0, []

    def copy(self, src, dst, where):
        one = pltpu.make_async_remote_copy(
            src_ref=src, dst_ref=dst, send_sem=self.send.at[self.next], recv_sem=self.recv.at[self.next],
            device_id=where, device_id_type=MESH_ID,
        )
        self.next += 1
        one.start()
        self.started.append(one)
        return one

    def finish(self):
        for one in self.started:
            one.wait_send()


def plane_place():
    me = lax.axis_index("seq")
    core = lax.axis_index("tensor")
    near, far = me + 1 - 2 * lax.rem(me, 2), lax.rem(me + 2, 4)
    cross = lax.rem(near + 2, 4)
    return me, core, near, far, cross


def greet(*places):
    barrier = pltpu.get_barrier_semaphore()
    for where in places:
        pl.semaphore_signal(barrier, inc=1, device_id=where, device_id_type=MESH_ID)
    pl.semaphore_wait(barrier, len(places))


def gather_steps(wires, ref, place, paired):
    me, core, near, far, cross = place
    half = ref.shape[-2] // 2
    to_near, to_far, partner = {"seq": near}, {"seq": far}, {"tensor": 1 - core}

    def part(spot, start, size):
        return ref.at[spot, core, pl.ds(start, size)] if paired else ref.at[spot, pl.ds(start, size)]

    def send(spot, start, size, where):
        block = part(spot, start, size)
        return wires.copy(block, block, where)

    near_top = send(me, 0, half, to_near)
    far_low = send(me, half, half, to_far)
    near_low = send(me, half, half, to_near)
    far_top = send(me, 0, half, to_far)
    inside = [send(me, 0, 2 * half, partner)] if paired else []
    yield
    near_top.wait_recv()
    cross_top = send(near, 0, half, to_far)
    far_low.wait_recv()
    cross_low = send(far, half, half, to_near)
    yield
    near_low.wait_recv()
    inside += [send(near, 0, 2 * half, partner)] if paired else []
    far_top.wait_recv()
    inside += [send(far, 0, 2 * half, partner)] if paired else []
    yield
    cross_top.wait_recv()
    inside += [send(cross, 0, half, partner)] if paired else []
    cross_low.wait_recv()
    inside += [send(cross, half, half, partner)] if paired else []
    yield
    for one in inside:
        one.wait_recv()


def run_all(*tasks):
    tasks = list(tasks)
    while tasks:
        tasks = [task for task in tasks if next(task, wires_done) is not wires_done]


wires_done = object()


def wide(values):
    return values.astype(jnp.float32)


def cross_steps(wires, place, total_of, out_refs, done):
    me, core, near, far, cross = place
    cross_ref, near_ref, far_ref, cross_in, near_in, far_in = out_refs
    half = near_ref.shape[0] // 2
    top, bottom = pl.ds(0, half), pl.ds(half, half)
    cross_ref[...] = total_of(cross).astype(cross_ref.dtype)
    to_near = wires.copy(cross_ref.at[top], cross_in.at[top], {"seq": near})
    to_far = wires.copy(cross_ref.at[bottom], cross_in.at[bottom], {"seq": far})
    near_ref[...] = total_of(near).astype(near_ref.dtype)
    near_one = wires.copy(near_ref.at[top], near_in.at[top], {"seq": near})
    far_ref[...] = total_of(far).astype(far_ref.dtype)
    far_one = wires.copy(far_ref.at[bottom], far_in.at[bottom], {"seq": far})
    yield
    to_near.wait_recv()
    far_ref[top, :] = (wide(far_ref[top, :]) + wide(cross_in[top, :])).astype(far_ref.dtype)
    far_two = wires.copy(far_ref.at[top], far_in.at[top], {"seq": far})
    to_far.wait_recv()
    near_ref[bottom, :] = (wide(near_ref[bottom, :]) + wide(cross_in[bottom, :])).astype(near_ref.dtype)
    near_two = wires.copy(near_ref.at[bottom], near_in.at[bottom], {"seq": near})
    own = total_of(me)
    yield
    for one in (near_one, far_one, far_two, near_two):
        one.wait_recv()
    done(own + wide(near_in[...]) + wide(far_in[...]))


def plane_sum_steps(wires, place, part_ref, partner_in, out_refs, done):
    me, core, near, far, cross = place
    arrivals = {}
    for name, spot in (("cross", cross), ("near", near), ("far", far), ("me", me)):
        arrivals[name] = wires.copy(part_ref.at[spot, 1 - core], partner_in.at[spot], {"tensor": 1 - core})
    order = iter(("cross", "near", "far", "me"))

    def total_of(spot):
        arrivals[next(order)].wait_recv()
        return wide(part_ref[spot, core]) + wide(partner_in[spot])

    yield
    yield from cross_steps(wires, place, total_of, out_refs, done)


def plane_sum(wires, place, part_ref, partner_in, out_refs):
    totals = []
    run_all(plane_sum_steps(wires, place, part_ref, partner_in, out_refs, totals.append))
    return totals[0]


def sum_scratch(piece, width):
    return [pltpu.VMEM((piece, width), jnp.bfloat16)] * 6


def sems(count):
    return [pltpu.SemaphoreType.DMA((count,)), pltpu.SemaphoreType.DMA((count,))]


def plane_peers(place):
    me, core, near, far, cross = place
    return {"seq": near}, {"seq": far}, {"tensor": 1 - core}


def norm_of(values, gain_vec):
    return values * lax.rsqrt(jnp.mean(values * values, axis=-1, keepdims=True) + epsilon) * gain_vec


def norm_back(values, gain_vec, grad):
    inverse = lax.rsqrt(jnp.mean(values * values, axis=-1, keepdims=True) + epsilon)
    unit = values * inverse
    scaled_grad = grad * gain_vec
    gain_grad = jnp.sum(grad * unit, axis=0, keepdims=True)
    return inverse * (scaled_grad - unit * jnp.mean(scaled_grad * unit, axis=-1, keepdims=True)), gain_grad


def dot(left, right):
    return jnp.dot(left, right, preferred_element_type=jnp.float32)


def dot_nt(left, right):
    return lax.dot_general(left, right, NT, preferred_element_type=jnp.float32)


def dot_tn(left, right):
    return lax.dot_general(left, right, TN, preferred_element_type=jnp.float32)


def project_steps(place, x_ref, gain_ref, w_ref, normed_ref, qkv_ref, wires):
    me, core, near, far, cross = place
    normed_ref[me] = norm_of(x_ref[...], gain_ref[...]).astype(jnp.bfloat16)
    task = gather_steps(wires, normed_ref, place, False)
    next(task)
    qkv_ref[me] = dot(normed_ref[me], w_ref[...]).astype(jnp.bfloat16)
    next(task)
    next(task)
    qkv_ref[near] = dot(normed_ref[near], w_ref[...]).astype(jnp.bfloat16)
    qkv_ref[far] = dot(normed_ref[far], w_ref[...]).astype(jnp.bfloat16)
    next(task)
    qkv_ref[cross] = dot(normed_ref[cross], w_ref[...]).astype(jnp.bfloat16)


def add_to(out_ref, base_ref):
    def done(total):
        out_ref[...] = base_ref[...] + total

    return done


def project_kernel(x_ref, gain_ref, w_ref, routes_ref, normed_ref, qkv_ref, routes_all_ref, send, recv):
    place = plane_place()
    me, core, near, far, cross = place
    wires = Wires(send, recv)
    greet({"seq": near}, {"seq": far}, {"seq": cross})
    routes_all_ref[me] = routes_ref[...]
    picks = [wires.copy(routes_ref, routes_all_ref.at[me], {"seq": spot}) for spot in (near, far, cross)]
    project_steps(place, x_ref, gain_ref, w_ref, normed_ref, qkv_ref, wires)
    for one in picks:
        one.wait_recv()
    wires.finish()


def sum_project_kernel(part_ref, base_ref, gain_ref, w_ref, x_ref, normed_ref, qkv_ref, partner_in, *rest):
    out_refs, (send, recv) = rest[:6], rest[6:]
    place = plane_place()
    wires = Wires(send, recv)
    greet(*plane_peers(place))
    x_ref[...] = base_ref[...] + plane_sum(wires, place, part_ref, partner_in, out_refs)
    project_steps(place, x_ref, gain_ref, w_ref, normed_ref, qkv_ref, wires)
    wires.finish()


def merge_kernel(fetch, mixed_ref, base_ref, w_ref, gain_ref, *refs):
    place = plane_place()
    me, core, near, far, cross = place
    if fetch:
        qkv_next, merged_ref, middle_ref, tokens_ref, qkv_all, send, recv = refs
        line_me, targets, sources = dp_peers()
    else:
        merged_ref, middle_ref, tokens_ref, send, recv = refs
        targets = []
    wires = Wires(send, recv)
    greet({"seq": near}, {"seq": far}, {"seq": cross}, {"tensor": 1 - core}, *[{"dp": spot} for spot in targets])
    if fetch:
        lines = line_start(wires, qkv_next, qkv_all, core, line_me, targets)
    copies = [wires.copy(mixed_ref.at[spot], merged_ref.at[me], {"seq": spot}) for spot in (cross, near, far)]
    merged_ref[me] = mixed_ref[me]
    total = base_ref[...] + dot(mixed_ref[me], w_ref[me])
    for spot, one in ((near, copies[1]), (far, copies[2]), (cross, copies[0])):
        one.wait_recv()
        total = total + dot(merged_ref[spot], w_ref[spot])
    middle_ref[...] = total
    tokens_ref[me, core] = norm_of(total, gain_ref[...]).astype(jnp.bfloat16)
    run_all(gather_steps(wires, tokens_ref, place, True))
    if fetch:
        for one in line_forward(wires, qkv_all, core, lines, sources):
            one.wait_recv()
    wires.finish()


def split_kernel(part_ref, middle_ref, gain_ref, grad_ref, w_ref, middle_grad_ref, out_grad_ref, gain_grad_ref, mixed_grad_ref,
                 outgoing, partner_in, *rest):
    out_refs, (send, recv) = rest[:6], rest[6:]
    place = plane_place()
    me, core, near, far, cross = place
    wires = Wires(send, recv)
    greet({"seq": near}, {"seq": far}, {"seq": cross}, {"tensor": 1 - core})
    normed_grad = plane_sum(wires, place, part_ref, partner_in, out_refs)
    part, gain_grad_ref[...] = norm_back(middle_ref[...], gain_ref[...], normed_grad)
    middle_grad = grad_ref[...] + part
    middle_grad_ref[...] = middle_grad
    out_grad_ref[...] = middle_grad.astype(jnp.bfloat16)
    copies = []
    for spot in (cross, near, far):
        outgoing[spot] = dot_nt(out_grad_ref[...], w_ref[spot]).astype(jnp.bfloat16)
        copies.append(wires.copy(outgoing.at[spot], mixed_grad_ref.at[me], {"seq": spot}))
    mixed_grad_ref[me] = dot_nt(out_grad_ref[...], w_ref[me]).astype(jnp.bfloat16)
    for one in copies:
        one.wait_recv()
    wires.finish()


def input_grad_kernel(spread, qkv_grad_ref, w_ref, x_ref, gain_ref, middle_grad_ref, *rest):
    grad_ref, gain_grad_ref = rest[:2]
    rows_ref = rest[2] if spread else None
    rest = rest[3:] if spread else rest[2:]
    out_refs, (send, recv) = rest[:6], rest[6:]
    place = plane_place()
    me, core, near, far, cross = place
    wires = Wires(send, recv)
    greet(*plane_peers(place)[: 3 if spread else 2])
    totals = []
    run_all(cross_steps(wires, place, lambda spot: dot_nt(qkv_grad_ref[spot], w_ref[...]), out_refs, totals.append))
    normed_grad = totals[0]
    part, gain_grad_ref[...] = norm_back(x_ref[...], gain_ref[...], normed_grad)
    grad = middle_grad_ref[...] + part
    grad_ref[...] = grad
    if spread:
        rows_ref[me, core] = grad.astype(jnp.bfloat16)
        run_all(gather_steps(wires, rows_ref, place, True))
    wires.finish()


def comm_call(kernel, name, number, time, outs, scratch, wire_count, *operands):
    return pl.pallas_call(
        kernel,
        out_shape=tuple(outs),
        in_specs=vmem(len(operands)),
        out_specs=tuple(vmem(len(outs))),
        scratch_shapes=scratch + sems(wire_count),
        compiler_params=pltpu.CompilerParams(collective_id=number, has_side_effects=True),
        cost_estimate=cost(time),
        name=name,
    )(*operands)


def cost(time):
    return pl.CostEstimate(flops=0, bytes_accessed=int(time * 3e6), transcendentals=0)


def low_array(*shape):
    return jax.ShapeDtypeStruct(shape, jnp.bfloat16)


def wide_array(*shape):
    return jax.ShapeDtypeStruct(shape, jnp.float32)


def gelu_parts(values):
    square = values * values
    inner = jnp.tanh(values * (0.7978845608028654 + (0.7978845608028654 * 0.044715) * square))
    lift = 0.5 + 0.5 * inner
    slope = lift + (0.5 * values) * (1.0 - inner * inner) * (0.7978845608028654 + (3.0 * 0.7978845608028654 * 0.044715) * square)
    return values * lift, slope


def slot_hot(slot_row, capacity):
    rows = lax.broadcasted_iota(jnp.int32, (capacity, slot_row.shape[1]), 0)
    return (rows == slot_row).astype(jnp.bfloat16)


def experts_kernel(tokens_ref, slot_ref, chosen_ref, own_ref, router_ref, up_ref, down_ref, part_ref, slots_ref, pre_ref, shares_ref):
    capacity = slots_ref.shape[0]
    tokens = tokens_ref[...]
    logits = jnp.where(chosen_ref[...] > 0, dot_nt(tokens, router_ref[...]), negative)
    raised = jnp.exp(logits - jnp.max(logits, axis=1, keepdims=True))
    shares = raised / jnp.sum(raised, axis=1, keepdims=True)
    shares_ref[...] = shares
    own_share = jnp.sum(shares * own_ref[...], axis=1, keepdims=True)
    hot = slot_hot(slot_ref[...], capacity)
    slots = dot(hot, tokens).astype(jnp.bfloat16)
    slots_ref[...] = slots
    pre = dot(slots, up_ref[...])
    pre_ref[...] = pre.astype(jnp.bfloat16)
    hidden = gelu_parts(pre)[0].astype(jnp.bfloat16)
    result = dot_nt(hidden, down_ref[...]).astype(jnp.bfloat16)
    part_ref[...] = (own_share * dot_tn(hot, result)).astype(jnp.bfloat16)


class Replay(Wires):
    def __init__(self, send, recv, ref, place, stage):
        super().__init__(send, recv)
        self.stage, self.now = stage, 0
        task = gather_steps(self, ref, place, False)
        for self.now in range(1, stage + 1):
            next(task, None)
        if stage == 5:
            self.finish()

    def copy(self, src, dst, where):
        one = pltpu.make_async_remote_copy(
            src_ref=src, dst_ref=dst, send_sem=self.send.at[self.next], recv_sem=self.recv.at[self.next],
            device_id=where, device_id_type=MESH_ID,
        )
        self.next += 1
        if self.now == self.stage:
            one.start()
        self.started.append(one)
        return Held(one, self)


class Held:
    def __init__(self, one, owner):
        self.one, self.owner = one, owner

    def wait_recv(self):
        if self.owner.now == self.owner.stage or self.owner.stage == 5 and self.owner.now > 2:
            self.one.wait_recv()


def experts_back_kernel(rows_ref, tokens_ref, slot_ref, shares_ref, own_ref, router_ref, up_ref, down_ref, slots_ref, pre_ref,
                        *refs):
    group, last = pl.program_id(0), pl.num_programs(0) - 1
    if len(refs) > 6:
        shard_ref, part_ref, up_grad_ref, down_grad_ref, router_grad_ref, shared_ref, up_acc, down_acc, landing, send, recv = refs

        @pl.when(group == 0)
        def _():
            place = plane_place()
            greet({"seq": place[2]}, {"seq": place[3]})
            landing[place[0]] = shard_ref[...]
            Replay(send, recv, landing, plane_place(), 1)

        @pl.when(group == 2)
        def _():
            Replay(send, recv, landing, plane_place(), 2)

    else:
        part_ref, up_grad_ref, down_grad_ref, router_grad_ref, up_acc, down_acc = refs
        shared_ref = None

    @pl.when(group == 0)
    def _():
        up_acc[...] = jnp.zeros_like(up_acc)
        down_acc[...] = jnp.zeros_like(down_acc)
        router_grad_ref[...] = jnp.zeros_like(router_grad_ref)

    capacity = slots_ref.shape[0]
    shares = shares_ref[...]
    own = own_ref[...]
    own_share = jnp.sum(shares * own, axis=1, keepdims=True)
    hot = slot_hot(slot_ref[...], capacity)
    scaled_rows = (own_share * rows_ref[...].astype(jnp.float32)).astype(jnp.bfloat16)
    result_grad = dot(hot, scaled_rows).astype(jnp.bfloat16)
    hidden_grad = dot(result_grad, down_ref[...])
    hidden, slope = gelu_parts(pre_ref[...].astype(jnp.float32))
    pre_grad = (slope * hidden_grad).astype(jnp.bfloat16)
    pair_sum = jnp.sum(hidden * hidden_grad, axis=1, keepdims=True)
    down_acc[...] += dot_tn(result_grad, hidden.astype(jnp.bfloat16))
    up_acc[...] += dot_tn(slots_ref[...], pre_grad)
    slot_grad = dot_nt(pre_grad, up_ref[...]).astype(jnp.bfloat16)
    high = pair_sum.astype(jnp.bfloat16)
    rest = (pair_sum - high.astype(jnp.float32)).astype(jnp.bfloat16)
    token_pair = dot_tn(hot, jnp.concatenate([jnp.broadcast_to(high, (capacity, 128)), jnp.broadcast_to(rest, (capacity, 128))], axis=1))
    token_pair = token_pair[:, :1] + token_pair[:, 128:129]
    logit_grad = (token_pair * (own - shares)).astype(jnp.bfloat16)
    router_grad_ref[...] += dot_tn(logit_grad, tokens_ref[...])
    part_ref[...] = (dot_tn(hot, slot_grad) + dot(logit_grad, router_ref[...])).astype(jnp.bfloat16)

    @pl.when(group == last)
    def _():
        up_grad_ref[...] = up_acc[...].astype(jnp.bfloat16)
        down_grad_ref[...] = down_acc[...].astype(jnp.bfloat16)

    if shared_ref is not None:

        @pl.when(group == last)
        def _():
            Replay(send, recv, landing, plane_place(), 5)
            shared_ref[...] = landing[...]


def by_group(*shape):
    return pl.BlockSpec((None,) + shape, lambda g: (g,) + (0,) * len(shape))


def held(*shape):
    return pl.BlockSpec(shape, lambda g: (0,) * len(shape), pipeline_mode=pl.Buffered(1))


def run_experts(tokens, slot, chosen, own, router, up, down, capacity):
    groups, rows, width = tokens.shape
    experts, wide_ff = router.shape[0], up.shape[1]
    return pl.pallas_call(
        experts_kernel,
        grid=(groups,),
        out_shape=(low_array(groups, rows, width), low_array(groups, capacity, width), low_array(groups, capacity, wide_ff),
                   wide_array(groups, rows, experts)),
        in_specs=[by_group(rows, width), by_group(1, rows), by_group(rows, experts), held(1, experts), held(experts, width),
                  held(width, wide_ff), held(width, wide_ff)],
        out_specs=(by_group(rows, width), by_group(capacity, width), by_group(capacity, wide_ff), by_group(rows, experts)),
        compiler_params=pltpu.CompilerParams(dimension_semantics=("arbitrary",)),
        cost_estimate=cost(14.0),
        name="experts",
    )(tokens, slot, chosen, own, router, up, down)


def run_experts_back(rows_grad, tokens, slot, shares, own, router, up, down, slots, pre, shard=None):
    groups, rows, width = tokens.shape
    experts, wide_ff = router.shape[0], up.shape[1]
    capacity = slots.shape[1]
    outs = [low_array(groups, rows, width), low_array(width, wide_ff), low_array(width, wide_ff), wide_array(experts, width)]
    out_specs = [by_group(rows, width), held(width, wide_ff), held(width, wide_ff), held(experts, width)]
    in_specs = [by_group(rows, width), by_group(rows, width), by_group(1, rows), by_group(rows, experts), held(1, experts),
                held(experts, width), held(width, wide_ff), held(width, wide_ff), by_group(capacity, width), by_group(capacity, wide_ff)]
    scratch = [pltpu.VMEM((width, wide_ff), jnp.float32), pltpu.VMEM((width, wide_ff), jnp.float32)]
    operands = [rows_grad, tokens, slot, shares, own, router, up, down, slots, pre]
    options = {}
    if shard is not None:
        operands.append(shard)
        in_specs.append(held(*shard.shape))
        outs.append(low_array(4, *shard.shape))
        out_specs.append(held(4, *shard.shape))
        scratch += [pltpu.VMEM((4,) + shard.shape, jnp.bfloat16)] + sems(6)
        options = {"collective_id": 13, "has_side_effects": True}
    return pl.pallas_call(
        experts_back_kernel,
        grid=(groups,),
        out_shape=tuple(outs),
        in_specs=in_specs,
        out_specs=tuple(out_specs),
        scratch_shapes=scratch,
        compiler_params=pltpu.CompilerParams(dimension_semantics=("arbitrary",), **options),
        cost_estimate=cost(25.0),
        name="experts_back" if shard is None else "experts_back_share",
    )(*operands)


def dp_peers():
    me, count = lax.axis_index("dp"), lax.axis_size("dp")
    return me, [lax.rem(me + step, count) for step in range(1, count)], [lax.rem(me + count - step, count) for step in range(1, count)]


def line_start(wires, own_ref, all_ref, core, me, targets):
    half = own_ref.at[core]
    copies = [wires.copy(half, all_ref.at[me, core], {"dp": spot}) for spot in targets]
    all_ref[me] = own_ref[...]
    return copies


def line_forward(wires, all_ref, core, copies, sources):
    onward = []
    for one, spot in zip(copies, sources):
        one.wait_recv()
        block = all_ref.at[spot, core]
        onward.append(wires.copy(block, block, {"tensor": 1 - core}))
    return onward


def weights_kernel(small_ref, whole_ref, outs_ref, small_all, qkv_all, qkv_next, one_piece, two_piece, own_ref, send, recv):
    core, place = lax.axis_index("tensor"), lax.axis_index("seq")
    me, targets, sources = dp_peers()
    wires = Wires(send, recv)
    greet(*[{"dp": spot} for spot in targets], {"tensor": 1 - core})
    smalls = [wires.copy(small_ref, small_all.at[me], {"dp": spot}) for spot in targets]
    small_all[me] = small_ref[...]
    layers, rows, columns = whole_ref.shape
    part, parts = columns // 3, lax.axis_size("seq")
    size = part // parts
    for spot in range(parts):

        @pl.when(place == spot)
        def _():
            for layer, target in enumerate((own_ref, qkv_next)):
                pieces = [whole_ref[layer, :, kind * part + spot * size : kind * part + (spot + 1) * size] for kind in range(3)]
                pieces = jnp.concatenate(pieces, axis=1)
                target[0] = pieces[: rows // 2]
                target[1] = pieces[rows // 2 :]

    qkvs = line_start(wires, own_ref, qkv_all, core, me, targets)
    half = one_piece.shape[-1]
    chosen = pl.ds(pl.multiple_of(core * half, half), half)
    for layer, piece in enumerate((one_piece, two_piece)):
        smalls += [wires.copy(outs_ref.at[layer, place, :, chosen], piece.at[me], {"dp": spot}) for spot in targets]
        piece[me] = outs_ref[layer, place, :, chosen]
    onward = line_forward(wires, qkv_all, core, qkvs, sources)
    for one in smalls + onward:
        one.wait_recv()
    wires.finish()


def reduce_steps(wires, place, line, plane_first, q_ref, o_ref, o_out, scratch):
    me, core, near, far, cross = place
    line_me, targets, sources = line
    q_in, q_sum, q_line, q_out, o_in, o_line, o_sum, o_seq = scratch
    others, partner = (cross, near, far), {"tensor": 1 - core}
    q_first = wires.copy(q_ref.at[1 - core], q_in, partner)
    o_first = wires.copy(o_ref.at[1 - core], o_in, partner)
    yield
    q_first.wait_recv()
    q_sum[...] = (wide(q_ref[core]) + wide(q_in[...])).astype(jnp.bfloat16)
    q_copies = [wires.copy(q_sum.at[spot], q_line.at[line_me], {"dp": spot}) for spot in targets]
    q_line[line_me] = q_sum[line_me]
    o_first.wait_recv()
    o_in[...] = (wide(o_ref[core]) + wide(o_in[...])).astype(jnp.bfloat16)
    if plane_first:
        o_copies = [wires.copy(o_in.at[:, spot], o_seq.at[me], {"seq": spot}) for spot in others]
        o_seq[me] = o_in[:, me]
    else:
        o_copies = [wires.copy(o_in.at[spot], o_line.at[line_me], {"dp": spot}) for spot in targets]
        o_line[line_me] = o_in[line_me]
    yield

    def line_total(ref, copies):
        for one in copies:
            one.wait_recv()
        total = wide(ref[0])
        for spot in range(1, len(targets) + 1):
            total = total + wide(ref[spot])
        return total.astype(jnp.bfloat16)

    def spread(out):
        mine = out.at[core, me]
        return (out, [wires.copy(mine, mine, {"seq": spot}) for spot in others], [wires.copy(mine, mine, partner)])

    def plane_total(copies):
        for one in copies:
            one.wait_recv()
        return (wide(o_seq[0]) + wide(o_seq[1]) + wide(o_seq[2]) + wide(o_seq[3])).astype(jnp.bfloat16)

    if plane_first:
        o_sum[...] = plane_total(o_copies)
        next_copies = [wires.copy(o_sum.at[spot], o_line.at[line_me], {"dp": spot}) for spot in targets]
        o_line[line_me] = o_sum[line_me]
        yield
        q_out[core, me] = line_total(q_line, q_copies)
        last = [spread(q_out)]
        yield
        o_out[core, me] = line_total(o_line, next_copies)
    else:
        q_out[core, me] = line_total(q_line, q_copies)
        last = [spread(q_out)]
        yield
        o_sum[...] = line_total(o_line, o_copies)
        next_copies = [wires.copy(o_sum.at[spot], o_seq.at[me], {"seq": spot}) for spot in others]
        o_seq[me] = o_sum[me]
        yield
        o_out[core, me] = plane_total(next_copies)
    last.append(spread(o_out))
    yield
    for out, copies, onward in last:
        for one, spot in zip(copies, others):
            one.wait_recv()
            block = out.at[core, spot]
            onward.append(wires.copy(block, block, partner))
    yield
    for out, copies, onward in last:
        for one in onward:
            one.wait_recv()


def finish_kernel(layers, count, *refs):
    def take(number):
        nonlocal refs
        first, refs = refs[:number], refs[number:]
        return first

    q_refs, o_refs, shard_refs = take(layers), take(layers), take(count)
    (total_ref,), o_outs, share_outs = take(1), take(layers), take(count)
    scratch = [take(8) for _ in range(layers)]
    place, line = plane_place(), dp_peers()
    me, core, near, far, cross = place
    wires = Wires(*refs)
    greet({"seq": near}, {"seq": far}, {"seq": cross}, {"tensor": 1 - core}, *[{"dp": spot} for spot in line[1]])
    tasks = [reduce_steps(wires, place, line, at > 0, *one) for at, one in enumerate(zip(q_refs, o_refs, o_outs, scratch))]
    for _ in range(2):
        for task in tasks:
            next(task)
    shares = []
    for src, dst in zip(shard_refs, share_outs):
        dst[me] = src[...]
        shares.append(gather_steps(wires, dst, place, False))
    run_all(*shares, *tasks)
    rows = total_ref.shape[1] // 2
    for layer in range(layers):
        whole = scratch[layer][3]
        size = whole.shape[-1] // 3
        for half in range(2):
            pieces = [whole[half, spot][:, kind * size : (kind + 1) * size] for kind in range(3) for spot in range(4)]
            total_ref[layer, half * rows : (half + 1) * rows, :] = wide(jnp.concatenate(pieces, axis=1))
    wires.finish()
def body(
    block_input,
    segments,
    routes,
    distance_bucket,
    first_gain,
    query_key_value,
    attention_out,
    bias_table,
    second_gain,
    router_weights,
    expert_up,
    expert_down,
    cotangent,
):
    low = jnp.bfloat16
    seq_count, piece, width = block_input.shape
    n_dp, n_seq, n_tensor = (lax.axis_size(name) for name in ("dp", "seq", "tensor"))
    n_plane = n_seq * n_tensor
    length = piece * n_seq
    local_heads = HEADS // n_seq
    head_width = local_heads * HD
    experts = expert_up.shape[1]
    assert seq_count == 1 and experts == n_seq
    shard = width // n_dp
    bucket_count = bias_table.shape[1] * n_dp
    bucket_shard = bias_table.shape[1]
    group_rows = n_tensor * piece
    capacity = group_rows * routes.shape[-1] // experts
    seq_index = lax.axis_index("seq")
    span = ROWS + length // 2


    assert n_seq == 4 and n_tensor == 2
    half = shard // n_tensor

    def padded(values):
        return jnp.pad(values, ((0, 0), (0, shard - values.shape[1])))

    small = jnp.concatenate(
        [
            first_gain,
            second_gain,
            router_weights.swapaxes(1, 2).reshape(-1, shard),
            padded(bias_table.reshape(LAYERS, -1)),
        ]
    )
    small_rows = small.shape[0]
    small = jnp.pad(small, ((0, -small_rows % 16), (0, 0)))
    own_out = attention_out.reshape(LAYERS, n_seq, shard // n_seq, width)
    own_up = lax.dynamic_index_in_dim(expert_up, seq_index, 1, keepdims=False)
    own_down = lax.dynamic_index_in_dim(expert_down, seq_index, 1, keepdims=False).swapaxes(1, 2)

    def expert_weights(layer):
        up = lax.all_gather(own_up[layer], "dp", axis=0, tiled=True)
        down = lax.all_gather(own_down[layer], "dp", axis=0, tiled=True)
        return up, down

    own_shape = (n_tensor, half, 3 * head_width)
    small_all, qkv_all, qkv_next, *out_pieces = comm_call(
        weights_kernel, "weights", 10, 22.0,
        [low_array(n_dp, *small.shape), low_array(n_dp, *own_shape), low_array(*own_shape)]
        + [low_array(n_dp, shard // n_seq, width // n_tensor)] * LAYERS,
        [pltpu.VMEM(own_shape, low)], 5 * (n_dp - 1), small, query_key_value, own_out
    )
    own_up, own_down, small_all = lax.optimization_barrier((own_up, own_down, small_all))
    qkv_weights = [qkv_all]
    whole_rows = small_all.swapaxes(0, 1).reshape(-1, width)
    gains = whole_rows[: 2 * LAYERS].astype(jnp.float32).reshape(2, LAYERS, 1, width)
    routers = whole_rows[2 * LAYERS : 2 * LAYERS + LAYERS * experts].reshape(LAYERS, experts, width)
    tables = whole_rows[2 * LAYERS + LAYERS * experts : small_rows].reshape(LAYERS, n_dp, shard)[:, :, : bucket_shard * HEADS]
    tables = tables.reshape(LAYERS, bucket_count, HEADS).astype(jnp.float32)
    own_tables = lax.dynamic_slice_in_dim(tables, seq_index * local_heads, local_heads, 2)
    routes_own = routes.reshape(-1, 128)
    seg_row = segments
    seg_col = segments.reshape(length, 1)
    bucket_line = distance_bucket[length // 2 - 1 :: -1][: length // 2]
    bucket_line = jnp.concatenate(
        [jnp.full((1,), -1, jnp.int32), bucket_line, jnp.full((span - 1 - length // 2,), -1, jnp.int32)]
    )
    line_hot = (bucket_line[None, :] == lax.iota(jnp.int32, bucket_count)[:, None]).astype(jnp.float32)
    lines = jnp.einsum("lbh,bs->lhs", own_tables, line_hot, precision=highest_precision)
    strict_upper = (
        lax.iota(jnp.int32, group_rows)[:, None] < lax.iota(jnp.int32, group_rows)[None, :]
    ).astype(low)

    own_hot = (lax.iota(jnp.int32, experts) == seq_index).astype(jnp.float32)[None]

    current = block_input[0]
    grad = cotangent[0]
    saved = []
    for layer in range(LAYERS):
        up, down = expert_weights(layer)
        gain_one, gain_two = gains[0, layer], gains[1, layer]
        qkv_weight = qkv_weights[layer].reshape(width, 3 * head_width)
        outs = [low_array(n_seq, piece, width), low_array(n_seq, piece, 3 * head_width)]
        if layer == 0:
            outs.append(jax.ShapeDtypeStruct((n_seq,) + routes_own.shape, jnp.int32))
            normed_all, qkv, routes_all = comm_call(
                project_kernel, "project", 1, 16.0, outs, [], 9, current, gain_one, qkv_weight, routes_own
            )
            routes_all = jnp.moveaxis(routes_all.reshape((n_seq,) + routes.shape), 0, 1).reshape(LAYERS, n_seq, group_rows, -1)
            mine = jnp.any(routes_all == seq_index, axis=-1)
            slot = dot(mine.reshape(-1, group_rows).astype(low), strict_upper).astype(jnp.int32).reshape(mine.shape)
            slot = jnp.where(mine & (slot < capacity), slot, -1)[:, :, None]
            chosen = jnp.any(routes_all[..., None] == lax.iota(jnp.int32, experts), axis=3).astype(jnp.float32)
        else:
            current, normed_all, qkv = comm_call(
                sum_project_kernel, "sum_project", 2, 32.0, [wide_array(piece, width)] + outs,
                [pltpu.VMEM((n_seq, piece, width), low)] + sum_scratch(piece, width), 16, part, middle, gain_one, qkv_weight
            )
        qkv = qkv.reshape(length, 3 * head_width)
        if layer == 0:
            outs = [low_array(n_dp, *own_out.shape[1:])] * LAYERS
            mixed, log_total, *out_weights = attend(qkv, seg_row, seg_col, lines[layer], out_pieces, outs, "fetch", 6, 8)
        else:
            outs = [low_array(n_seq, n_tensor, piece, width)]
            mixed, log_total, grad_rows = attend(qkv, seg_row, seg_col, lines[layer], (grad,), outs, "gather", 14, 11)
        out_weight = out_weights[layer].reshape(n_seq, head_width, width)
        fetch = layer == 0
        outs = [low_array(n_seq, piece, head_width), wide_array(piece, width), low_array(n_seq, n_tensor, piece, width)]
        outs += [low_array(n_dp, *own_shape)] if fetch else []
        operands = (mixed.reshape(n_seq, piece, head_width), current, out_weight, gain_two) + ((qkv_next,) if fetch else ())
        merged, middle, tokens, *more = comm_call(
            functools.partial(merge_kernel, fetch), "merge_fetch" if fetch else "merge", 15 if fetch else 3, 25.0, outs, [],
            14 + (2 * (n_dp - 1) if fetch else 0), *operands
        )
        qkv_weights += more
        tokens = tokens.reshape(n_seq, group_rows, width)
        part, slots, pre, shares = run_experts(tokens, slot[layer], chosen[layer], own_hot, routers[layer], up, down, capacity)
        part = part.reshape(n_seq, n_tensor, piece, width)
        saved.append((current, normed_all, qkv, log_total, merged, middle, tokens, shares, slots, pre, qkv_weight, out_weight, up, down))

    last_part, last_middle = part, middle

    def shard_sum(values):
        return lax.psum_scatter(values, "dp", scatter_dimension=0, tiled=True)

    up_shards, down_shards, qkv_grads, out_grads = ([None] * LAYERS for _ in range(4))
    out_rows = half // n_seq
    packed_rows = -(-(out_rows + 1) // 16) * 16
    for layer in range(LAYERS - 1, -1, -1):
        (layer_in, normed_all, qkv, log_total, merged, middle, tokens, shares, slots, pre, qkv_weight, out_weight, up, down) = saved[layer]
        gain_one, gain_two = gains[0, layer], gains[1, layer]
        part, up_grad, down_grad, router_grad, *shared = run_experts_back(
            grad_rows.reshape(n_seq, group_rows, width), tokens, slot[layer], shares, own_hot, routers[layer], up, down, slots, pre,
            down_shards[1] if layer == 0 else None
        )
        down_shards[layer] = shard_sum(down_grad)
        up_shards[layer] = shard_sum(up_grad)
        middle_grad, out_grad, gain_two_grad, mixed_grad = comm_call(
            split_kernel, "split", 5, 22.0,
            [wide_array(piece, width), low_array(piece, width), wide_array(1, width), low_array(n_seq, piece, head_width)],
            [pltpu.VMEM((n_seq, piece, head_width), low), pltpu.VMEM((n_seq, piece, width), low)] + sum_scratch(piece, width), 13,
            part.reshape(n_seq, n_tensor, piece, width), middle, gain_two, grad, out_weight
        )
        out_weight_grad = jnp.einsum("gtd,te->gde", merged, out_grad, preferred_element_type=jnp.float32)
        operands = (qkv, seg_row, seg_col, lines[layer], log_total, mixed_grad.reshape(length, head_width))
        if layer == 0:
            (down_last,) = shared
            outs = [low_array(n_seq, *up_shards[1].shape)]
            qkv_grad, band, up_last = attend_back(*operands, (up_shards[1],), outs, [], "share", 9, 6)
        else:
            outs = [wide_array(piece, width)]
            extra_scratch = [pltpu.VMEM((n_seq, piece, width), low)] + sum_scratch(piece, width)
            qkv_grad, band, block_output = attend_back(*operands, (last_part, last_middle), outs, extra_scratch, "sum", 4, 10)
        qkv_weight_grad = dot_tn(normed_all.reshape(length, width), qkv_grad)
        spread = layer > 0
        outs = [wide_array(piece, width), wide_array(1, width)]
        outs += [low_array(n_seq, n_tensor, piece, width)] if spread else []
        outs = comm_call(
            functools.partial(input_grad_kernel, spread), "input_grad_spread" if spread else "input_grad", 7 + spread, 32.0 if spread else 16.0,
            outs, sum_scratch(piece, width), 17, qkv_grad.reshape(n_seq, piece, -1), qkv_weight, layer_in, gain_one, middle_grad
        )
        grad, gain_one_grad = outs[:2]
        grad_rows = outs[2] if spread else None
        table_grad = jnp.dot(line_hot, band.T, precision=highest_precision)
        table_grad = lax.dynamic_update_slice_in_dim(
            jnp.zeros((bucket_count, HEADS), jnp.float32), table_grad, seq_index * local_heads, 1
        )
        table_grad = padded(table_grad.reshape(n_dp, -1)).reshape(1, width)
        packed = jnp.concatenate([gain_one_grad, gain_two_grad, router_grad, table_grad, jnp.zeros((1, width), jnp.float32)])
        packed = packed.reshape(n_plane, n_dp, shard).swapaxes(0, 1)[:, :, None]
        packed = jnp.pad(packed, ((0, 0), (0, 0), (0, packed_rows - out_rows - 1), (0, width - shard)))
        both = jnp.concatenate([out_weight_grad.reshape(n_dp, n_plane, out_rows, width), packed], axis=2).astype(low)
        out_grads[layer] = both.reshape(n_dp, n_tensor, n_seq, packed_rows, width).swapaxes(0, 1)
        qkv_grads[layer] = qkv_weight_grad.astype(low).reshape(n_dp, n_tensor, half, 3 * head_width).swapaxes(0, 1)

    def reduce_scratch(plane_first):
        line = pltpu.VMEM((n_dp, half, 3 * head_width), low)
        blocks = pltpu.VMEM((n_dp, n_seq, packed_rows, width), low)
        over_dp, over_seq = (pltpu.VMEM((count, packed_rows, width), low) for count in (n_dp, n_seq))
        found = [line] * 3 + [pltpu.VMEM((n_tensor, n_seq, half, 3 * head_width), low), blocks]
        if plane_first:
            return found + [over_dp, over_dp, pltpu.VMEM((n_seq, n_dp, packed_rows, width), low)]
        return found + [blocks, over_seq, over_seq]

    qkv_total, *totals = comm_call(
        functools.partial(finish_kernel, LAYERS, 2), "finish", 11, 70.0,
        [wide_array(LAYERS, shard, 3 * width)] + [low_array(n_tensor, n_seq, packed_rows, width)] * LAYERS
        + [low_array(n_seq, shard, up.shape[1])] * 2,
        reduce_scratch(False) + reduce_scratch(True), LAYERS * (2 * (n_dp - 1) + 19) + 12, *qkv_grads, *out_grads, up_shards[0], down_shards[0]
    )
    up_first, down_first = totals[LAYERS:]
    both = jnp.stack(totals[:LAYERS]).astype(jnp.float32).reshape(LAYERS, n_plane, packed_rows, width)
    out_total = both[:, :, :out_rows].reshape(LAYERS, shard, width)
    small = both[:, :, out_rows, :shard]
    router_total = small[:, 2 : 2 + experts].swapaxes(1, 2)
    table_total = small[:, 2 + experts, : bucket_shard * HEADS].reshape(LAYERS, bucket_shard, HEADS)
    up_total = jnp.stack([up_first, up_last]).astype(jnp.float32)
    down_total = jnp.stack([down_first, down_last]).astype(jnp.float32).swapaxes(2, 3)
    return (block_output[None], grad[None], small[:, 0], qkv_total, out_total, table_total, small[:, 1], router_total, up_total, down_total)


def solution(mesh):
    in_specs = (
        P(("dp", "tensor"), "seq", None),
        P(("dp", "tensor"), None),
        P(None, "dp", "seq", None),
        P(),
        P(None, "dp"),
        P(None, "dp", None),
        P(None, "dp", None),
        P(None, "dp", None),
        P(None, "dp"),
        P(None, "dp", None),
        P(None, None, "dp", "tensor"),
        P(None, None, "tensor", "dp"),
        P(("dp", "tensor"), "seq", None),
    )
    out_specs = (
        P(("dp", "tensor"), "seq", None),
        P(("dp", "tensor"), "seq", None),
        P(None, "dp"),
        P(None, "dp", None),
        P(None, "dp", None),
        P(None, "dp", None),
        P(None, "dp"),
        P(None, "dp", None),
        P(None, None, "dp", "tensor"),
        P(None, None, "tensor", "dp"),
    )
    return jax.shard_map(body, mesh=mesh, in_specs=in_specs, out_specs=out_specs, check_vma=False)
```

```python
import functools

import jax
import jax.numpy as jnp
from jax import lax
from jax.experimental import pallas as pl
from jax.experimental.pallas import tpu as pltpu
from jax.sharding import PartitionSpec as P

HEADS = 12
LAYERS = 2
epsilon = 1e-06
negative = -1e30
highest_precision = lax.Precision.HIGHEST


def scaled(values, gain_vec):
    return values * lax.rsqrt(jnp.mean(values * values, axis=-1, keepdims=True) + epsilon) * gain_vec


HD = 64
ROWS = 128
NT = (((1,), (1,)), ((), ()))
TN = (((0,), (0,)), ((), ()))


def visit_blocks(length, span, one_block, hook, hooks_at):
    full, count = span // ROWS, length // ROWS

    def step(i, carry):
        start = pl.multiple_of(i * ROWS, ROWS)
        one_block(start, pl.multiple_of(start + ROWS - span, ROWS), span)
        return carry

    for i in range(full - 1):
        if i in hooks_at:
            hook()
        one_block(i * ROWS, 0, (i + 1) * ROWS)
    stops = [full - 1] + [i for i in range(full - 1, count) if i in hooks_at] + [count]
    for low, high in zip(stops, stops[1:]):
        if low in hooks_at:
            hook()
        lax.fori_loop(low, high, step, 0)


def background(tasks):
    tasks = list(tasks)

    def hook():
        tasks[:] = [task for task in tasks if next(task, wires_done) is not wires_done]

    return hook, lambda: run_all(*tasks)


def fill_mask(mask_ref, segr_ref, segc_ref, start, low, width):
    same = segc_ref[pl.ds(start, ROWS), :] == segr_ref[:, pl.ds(low, width)]
    back = lax.broadcasted_iota(jnp.int32, (ROWS, width), 0) + (width - ROWS)
    allowed = same & (back >= lax.broadcasted_iota(jnp.int32, (ROWS, width), 1))
    mask_ref[:, :width] = jnp.where(allowed, 0.0, -1e30)


def fill_slab(slab_ref, line_ref, heads, span):
    for h in range(heads):
        spread = jnp.broadcast_to(line_ref[h : h + 1, :], (ROWS, span))
        slab_ref[h] = pltpu.roll(spread, 0, 1, stride=1, stride_axis=0)


def split_heads(qkv_ref, parts_ref, heads):
    for h in range(3 * heads):
        part = qkv_ref[:, h * HD : (h + 1) * HD]
        parts_ref[h] = part * jnp.bfloat16(0.125) if h < heads else part


def fetch_steps(wires, place, own, whole):
    me, core, near, far, cross = place
    width = whole.shape[-1]
    columns = pl.ds(pl.multiple_of(core * (width // 2), width // 2), width // 2)
    around = [wires.copy(own, whole.at[:, me, :, columns], {"seq": spot}) for spot in (cross, near, far)]
    whole[:, me, :, columns] = own[...]
    yield
    for one in around:
        one.wait_recv()
    block = whole.at[:, :, :, columns]
    onward = wires.copy(block, block, {"tensor": 1 - core})
    yield
    onward.wait_recv()


def attn_fwd_kernel(heads, span, mode, *refs):
    qkv_ref, segr_ref, segc_ref, line_ref = refs[:4]
    place = plane_place()
    me, core, near, far, cross = place
    wires = Wires(*refs[-2:])
    if mode == "fetch":
        own_refs, (out_ref, lse_ref), whole_refs, scratch = refs[4:6], refs[6:8], refs[8:10], refs[10:14]
        greet({"seq": near}, {"seq": far}, {"seq": cross}, {"tensor": 1 - core})
        tasks = [fetch_steps(wires, place, *pair) for pair in zip(own_refs, whole_refs)]
        hooks_at = (6,)
    else:
        rows_ref, out_ref, lse_ref, gathered_ref = refs[4:8]
        scratch = refs[8:12]
        greet(*plane_peers(place))
        gathered_ref[me, core] = rows_ref[...].astype(jnp.bfloat16)
        tasks = [gather_steps(wires, gathered_ref, place, True)]
        hooks_at = (4, 6)
    hook, finish = background(tasks)
    hook()
    parts_ref, mixed_ref, slab_ref, mask_ref = scratch
    length = qkv_ref.shape[0]
    fill_slab(slab_ref, line_ref, heads, span)
    split_heads(qkv_ref, parts_ref, heads)

    def one_block(start, low, width):
        fill_mask(mask_ref, segr_ref, segc_ref, start, low, width)

        def one_head(h, carry):
            q = parts_ref[h, pl.ds(start, ROWS), :]
            k = parts_ref[heads + h, pl.ds(low, width), :]
            v = parts_ref[2 * heads + h, pl.ds(low, width), :]
            s = lax.dot_general(q, k, NT, preferred_element_type=jnp.float32)
            s = s + slab_ref[h, :, span - width :] + mask_ref[:, :width]
            top = jnp.max(s, axis=1, keepdims=True)
            e = jnp.exp(s - top)
            total = jnp.sum(e, axis=1, keepdims=True)
            mixed = jnp.dot(e.astype(jnp.bfloat16), v, preferred_element_type=jnp.float32)
            mixed_ref[h, pl.ds(start, ROWS), :] = (mixed / total).astype(jnp.bfloat16)
            lse_ref[h, pl.ds(start, ROWS), :] = top + jnp.log(total)
            return carry

        lax.fori_loop(0, heads, one_head, 0, unroll=True)

    visit_blocks(length, span, one_block, hook, hooks_at)
    out_ref[...] = jnp.concatenate([mixed_ref[h] for h in range(heads)], axis=1)
    finish()
    wires.finish()


def attn_bwd_kernel(heads, span, mode, *refs):
    qkv_ref, segr_ref, segc_ref, line_ref, lse_ref, grad_ref, normed_ref = refs[:7]
    place = plane_place()
    me, core, near, far, cross = place
    wires = Wires(*refs[-2:])
    if mode == "share":
        shard_ref, out_ref, band_ref, weight_ref, shared_ref = refs[7:12]
        greet({"seq": near}, {"seq": far})
        shared_ref[me] = shard_ref[0]
        tasks = [gather_steps(wires, shared_ref, place, False)]
        refs = refs[12:20]
    else:
        part_ref, base_ref, out_ref, band_ref, weight_ref, total_ref = refs[7:13]
        greet(*plane_peers(place))
        tasks = [plane_sum_steps(wires, place, part_ref, refs[21], refs[22:28], add_to(total_ref, base_ref))]
        refs = refs[13:21]
    hook, finish = background(tasks)
    hook()
    parts_ref, gparts_ref, qgrad_ref, kgrad_ref, vgrad_ref, slab_ref, mask_ref, band_acc = refs
    length = qkv_ref.shape[0]
    fill_slab(slab_ref, line_ref, heads, span)
    split_heads(qkv_ref, parts_ref, heads)
    for h in range(heads):
        gparts_ref[h] = grad_ref[:, h * HD : (h + 1) * HD]
    kgrad_ref[...] = jnp.zeros_like(kgrad_ref)
    vgrad_ref[...] = jnp.zeros_like(vgrad_ref)
    band_acc[...] = jnp.zeros_like(band_acc)

    def one_block(start, low, width):
        fill_mask(mask_ref, segr_ref, segc_ref, start, low, width)

        def one_head(h, carry):
            rows = pl.ds(start, ROWS)
            window = pl.ds(low, width)
            q = parts_ref[h, rows, :]
            k = parts_ref[heads + h, window, :]
            v = parts_ref[2 * heads + h, window, :]
            grad = gparts_ref[h, rows, :]
            s = lax.dot_general(q, k, NT, preferred_element_type=jnp.float32)
            s = s + slab_ref[h, :, span - width :] + mask_ref[:, :width]
            p = jnp.exp(s - lse_ref[h, rows, :])
            dp = lax.dot_general(grad, v, NT, preferred_element_type=jnp.float32)
            inner = jnp.sum(p * dp, axis=1, keepdims=True)
            ds = p * (dp - inner)
            band_acc[h, :, span - width :] += ds
            ds = ds.astype(jnp.bfloat16)
            qgrad = jnp.dot(ds, k, preferred_element_type=jnp.float32)
            qgrad_ref[h, rows, :] = (qgrad * 0.125).astype(jnp.bfloat16)
            kgrad_ref[h, window, :] += lax.dot_general(ds, q, TN, preferred_element_type=jnp.float32)
            vgrad_ref[h, window, :] += lax.dot_general(p.astype(jnp.bfloat16), grad, TN, preferred_element_type=jnp.float32)
            return carry

        lax.fori_loop(0, heads, one_head, 0, unroll=True)

    visit_blocks(length, span, one_block, hook, (5, 7) if mode == "share" else (3, 6))
    parts = [qgrad_ref[h] for h in range(heads)]
    parts += [kgrad_ref[h].astype(jnp.bfloat16) for h in range(heads)]
    parts += [vgrad_ref[h].astype(jnp.bfloat16) for h in range(heads)]
    out_ref[...] = jnp.concatenate(parts, axis=1)
    weight_grad = dot_tn(normed_ref[...], out_ref[...])
    rows = weight_ref.shape[2]
    for at in range(weight_ref.shape[1]):
        for core_at in range(weight_ref.shape[0]):
            first = (at * weight_ref.shape[0] + core_at) * rows
            weight_ref[core_at, at] = weight_grad[first : first + rows].astype(jnp.bfloat16)
    row = lax.broadcasted_iota(jnp.int32, (ROWS, span), 0)
    for h in range(heads):
        acc = band_acc[h]
        bit = 1
        while bit < ROWS:
            acc = jnp.where((row & bit) != 0, pltpu.roll(acc, span - bit, 1), acc)
            bit *= 2
        band_ref[h : h + 1, :] = jnp.sum(acc, axis=0, keepdims=True)
    finish()
    wires.finish()


def vmem(count):
    return [pl.BlockSpec(memory_space=pltpu.VMEM)] * count


def attend_scratch(heads, length, span):
    return [
        pltpu.VMEM((3 * heads, length, HD), jnp.bfloat16),
        pltpu.VMEM((heads, length, HD), jnp.bfloat16),
        pltpu.VMEM((heads, ROWS, span), jnp.float32),
        pltpu.VMEM((ROWS, span), jnp.float32),
    ]


def attend(qkv, seg_row, seg_col, line, extra, extra_outs, mode, number, wire_count):
    length, width = qkv.shape
    heads, span = line.shape
    outs = [low_array(length, heads * HD), wide_array(heads, length, 1)] + extra_outs
    return comm_call(functools.partial(attn_fwd_kernel, heads, span, mode), "attend_" + mode, number, 18.0, outs,
                     attend_scratch(heads, length, span), wire_count, qkv, seg_row, seg_col, line, *extra)


def attend_back(qkv, seg_row, seg_col, line, lse, grad, normed, weight_shape, extra, extra_outs, extra_scratch, mode, number, wire_count):
    length, width = qkv.shape
    heads, span = line.shape
    outs = [low_array(length, width), wide_array(heads, span), low_array(*weight_shape)] + extra_outs
    scratch = [
        pltpu.VMEM((3 * heads, length, HD), jnp.bfloat16),
        pltpu.VMEM((heads, length, HD), jnp.bfloat16),
        pltpu.VMEM((heads, length, HD), jnp.bfloat16),
        pltpu.VMEM((heads, length, HD), jnp.float32),
        pltpu.VMEM((heads, length, HD), jnp.float32),
        pltpu.VMEM((heads, ROWS, span), jnp.float32),
        pltpu.VMEM((ROWS, span), jnp.float32),
        pltpu.VMEM((heads, ROWS, span), jnp.float32),
    ]
    return comm_call(functools.partial(attn_bwd_kernel, heads, span, mode), "attend_back_" + mode, number, 23.0, outs,
                     scratch + extra_scratch, wire_count, qkv, seg_row, seg_col, line, lse, grad, normed, *extra)


MESH_ID = pl.DeviceIdType.MESH


class Wires:
    def __init__(self, send, recv):
        self.send, self.recv, self.next, self.started = send, recv, 0, []

    def copy(self, src, dst, where):
        one = pltpu.make_async_remote_copy(
            src_ref=src, dst_ref=dst, send_sem=self.send.at[self.next], recv_sem=self.recv.at[self.next],
            device_id=where, device_id_type=MESH_ID,
        )
        self.next += 1
        one.start()
        self.started.append(one)
        return one

    def finish(self):
        for one in self.started:
            one.wait_send()


def plane_place():
    me = lax.axis_index("seq")
    core = lax.axis_index("tensor")
    near, far = me + 1 - 2 * lax.rem(me, 2), lax.rem(me + 2, 4)
    cross = lax.rem(near + 2, 4)
    return me, core, near, far, cross


def greet(*places):
    barrier = pltpu.get_barrier_semaphore()
    for where in places:
        pl.semaphore_signal(barrier, inc=1, device_id=where, device_id_type=MESH_ID)
    pl.semaphore_wait(barrier, len(places))


def gather_steps(wires, ref, place, paired):
    me, core, near, far, cross = place
    half = ref.shape[-2] // 2
    to_near, to_far, partner = {"seq": near}, {"seq": far}, {"tensor": 1 - core}

    def part(spot, start, size):
        return ref.at[spot, core, pl.ds(start, size)] if paired else ref.at[spot, pl.ds(start, size)]

    def send(spot, start, size, where):
        block = part(spot, start, size)
        return wires.copy(block, block, where)

    near_top = send(me, 0, half, to_near)
    far_low = send(me, half, half, to_far)
    near_low = send(me, half, half, to_near)
    far_top = send(me, 0, half, to_far)
    inside = [send(me, 0, 2 * half, partner)] if paired else []
    yield
    near_top.wait_recv()
    cross_top = send(near, 0, half, to_far)
    far_low.wait_recv()
    cross_low = send(far, half, half, to_near)
    yield
    near_low.wait_recv()
    inside += [send(near, 0, 2 * half, partner)] if paired else []
    far_top.wait_recv()
    inside += [send(far, 0, 2 * half, partner)] if paired else []
    yield
    cross_top.wait_recv()
    inside += [send(cross, 0, half, partner)] if paired else []
    cross_low.wait_recv()
    inside += [send(cross, half, half, partner)] if paired else []
    yield
    for one in inside:
        one.wait_recv()


def run_all(*tasks):
    tasks = list(tasks)
    while tasks:
        tasks = [task for task in tasks if next(task, wires_done) is not wires_done]


wires_done = object()


def wide(values):
    return values.astype(jnp.float32)


def cross_steps(wires, place, total_of, out_refs, done):
    me, core, near, far, cross = place
    cross_ref, near_ref, far_ref, cross_in, near_in, far_in = out_refs
    half = near_ref.shape[0] // 2
    top, bottom = pl.ds(0, half), pl.ds(half, half)
    cross_ref[...] = total_of(cross).astype(cross_ref.dtype)
    to_near = wires.copy(cross_ref.at[top], cross_in.at[top], {"seq": near})
    to_far = wires.copy(cross_ref.at[bottom], cross_in.at[bottom], {"seq": far})
    near_ref[...] = total_of(near).astype(near_ref.dtype)
    near_one = wires.copy(near_ref.at[top], near_in.at[top], {"seq": near})
    far_ref[...] = total_of(far).astype(far_ref.dtype)
    far_one = wires.copy(far_ref.at[bottom], far_in.at[bottom], {"seq": far})
    yield
    to_near.wait_recv()
    far_ref[top, :] = (wide(far_ref[top, :]) + wide(cross_in[top, :])).astype(far_ref.dtype)
    far_two = wires.copy(far_ref.at[top], far_in.at[top], {"seq": far})
    to_far.wait_recv()
    near_ref[bottom, :] = (wide(near_ref[bottom, :]) + wide(cross_in[bottom, :])).astype(near_ref.dtype)
    near_two = wires.copy(near_ref.at[bottom], near_in.at[bottom], {"seq": near})
    own = total_of(me)
    yield
    for one in (near_one, far_one, far_two, near_two):
        one.wait_recv()
    done(own + wide(near_in[...]) + wide(far_in[...]))


def plane_sum_steps(wires, place, part_ref, partner_in, out_refs, done):
    me, core, near, far, cross = place
    arrivals = {}
    for name, spot in (("cross", cross), ("near", near), ("far", far), ("me", me)):
        arrivals[name] = wires.copy(part_ref.at[spot, 1 - core], partner_in.at[spot], {"tensor": 1 - core})
    order = iter(("cross", "near", "far", "me"))

    def total_of(spot):
        arrivals[next(order)].wait_recv()
        return wide(part_ref[spot, core]) + wide(partner_in[spot])

    yield
    yield from cross_steps(wires, place, total_of, out_refs, done)


def plane_sum(wires, place, part_ref, partner_in, out_refs):
    totals = []
    run_all(plane_sum_steps(wires, place, part_ref, partner_in, out_refs, totals.append))
    return totals[0]


def sum_scratch(piece, width):
    return [pltpu.VMEM((piece, width), jnp.bfloat16)] * 6


def sems(count):
    return [pltpu.SemaphoreType.DMA((count,)), pltpu.SemaphoreType.DMA((count,))]


def plane_peers(place):
    me, core, near, far, cross = place
    return {"seq": near}, {"seq": far}, {"tensor": 1 - core}


def norm_of(values, gain_vec):
    return values * lax.rsqrt(jnp.mean(values * values, axis=-1, keepdims=True) + epsilon) * gain_vec


def norm_back(values, gain_vec, grad):
    inverse = lax.rsqrt(jnp.mean(values * values, axis=-1, keepdims=True) + epsilon)
    unit = values * inverse
    scaled_grad = grad * gain_vec
    gain_grad = jnp.sum(grad * unit, axis=0, keepdims=True)
    return inverse * (scaled_grad - unit * jnp.mean(scaled_grad * unit, axis=-1, keepdims=True)), gain_grad


def dot(left, right):
    return jnp.dot(left, right, preferred_element_type=jnp.float32)


def dot_nt(left, right):
    return lax.dot_general(left, right, NT, preferred_element_type=jnp.float32)


def dot_tn(left, right):
    return lax.dot_general(left, right, TN, preferred_element_type=jnp.float32)


def project_steps(place, x_ref, gain_ref, w_ref, normed_ref, qkv_ref, wires):
    me, core, near, far, cross = place
    normed_ref[me] = norm_of(x_ref[...], gain_ref[...]).astype(jnp.bfloat16)
    task = gather_steps(wires, normed_ref, place, False)
    next(task)
    qkv_ref[me] = dot(normed_ref[me], w_ref[...]).astype(jnp.bfloat16)
    next(task)
    next(task)
    qkv_ref[near] = dot(normed_ref[near], w_ref[...]).astype(jnp.bfloat16)
    qkv_ref[far] = dot(normed_ref[far], w_ref[...]).astype(jnp.bfloat16)
    next(task)
    qkv_ref[cross] = dot(normed_ref[cross], w_ref[...]).astype(jnp.bfloat16)


def add_to(out_ref, base_ref):
    def done(total):
        out_ref[...] = base_ref[...] + total

    return done


def project_kernel(x_ref, gain_ref, w_ref, routes_ref, normed_ref, qkv_ref, routes_all_ref, send, recv):
    place = plane_place()
    me, core, near, far, cross = place
    wires = Wires(send, recv)
    greet({"seq": near}, {"seq": far}, {"seq": cross})
    routes_all_ref[me] = routes_ref[...]
    picks = [wires.copy(routes_ref, routes_all_ref.at[me], {"seq": spot}) for spot in (near, far, cross)]
    project_steps(place, x_ref, gain_ref, w_ref, normed_ref, qkv_ref, wires)
    for one in picks:
        one.wait_recv()
    wires.finish()


def sum_project_kernel(part_ref, base_ref, gain_ref, w_ref, x_ref, normed_ref, qkv_ref, partner_in, *rest):
    out_refs, (send, recv) = rest[:6], rest[6:]
    place = plane_place()
    wires = Wires(send, recv)
    greet(*plane_peers(place))
    x_ref[...] = base_ref[...] + plane_sum(wires, place, part_ref, partner_in, out_refs)
    project_steps(place, x_ref, gain_ref, w_ref, normed_ref, qkv_ref, wires)
    wires.finish()


def merge_kernel(fetch, mixed_ref, base_ref, w_ref, gain_ref, *refs):
    place = plane_place()
    me, core, near, far, cross = place
    if fetch:
        qkv_next, merged_ref, middle_ref, tokens_ref, qkv_all, send, recv = refs
        line_me, targets, sources = dp_peers()
    else:
        merged_ref, middle_ref, tokens_ref, send, recv = refs
        targets = []
    wires = Wires(send, recv)
    greet({"seq": near}, {"seq": far}, {"seq": cross}, {"tensor": 1 - core}, *[{"dp": spot} for spot in targets])
    if fetch:
        lines = line_start(wires, qkv_next, qkv_all, core, line_me, targets)
    copies = [wires.copy(mixed_ref.at[spot], merged_ref.at[me], {"seq": spot}) for spot in (cross, near, far)]
    merged_ref[me] = mixed_ref[me]
    total = base_ref[...] + dot(mixed_ref[me], w_ref[me])
    for spot, one in ((near, copies[1]), (far, copies[2]), (cross, copies[0])):
        one.wait_recv()
        total = total + dot(merged_ref[spot], w_ref[spot])
    middle_ref[...] = total
    tokens_ref[me, core] = norm_of(total, gain_ref[...]).astype(jnp.bfloat16)
    run_all(gather_steps(wires, tokens_ref, place, True))
    if fetch:
        for one in line_forward(wires, qkv_all, core, lines, sources):
            one.wait_recv()
    wires.finish()


def split_kernel(part_ref, middle_ref, gain_ref, grad_ref, w_ref, merged_ref, middle_grad_ref, gain_grad_ref, mixed_grad_ref,
                 weight_ref, out_grad_ref, outgoing, partner_in, *rest):
    out_refs, (send, recv) = rest[:6], rest[6:]
    place = plane_place()
    me, core, near, far, cross = place
    wires = Wires(send, recv)
    greet({"seq": near}, {"seq": far}, {"seq": cross}, {"tensor": 1 - core})
    normed_grad = plane_sum(wires, place, part_ref, partner_in, out_refs)
    part, gain_grad_ref[...] = norm_back(middle_ref[...], gain_ref[...], normed_grad)
    middle_grad = grad_ref[...] + part
    middle_grad_ref[...] = middle_grad
    out_grad_ref[...] = middle_grad.astype(jnp.bfloat16)
    copies = []
    for spot in (cross, near, far):
        outgoing[spot] = dot_nt(out_grad_ref[...], w_ref[spot]).astype(jnp.bfloat16)
        copies.append(wires.copy(outgoing.at[spot], mixed_grad_ref.at[me], {"seq": spot}))
    mixed_grad_ref[me] = dot_nt(out_grad_ref[...], w_ref[me]).astype(jnp.bfloat16)
    cores, count, parts, rows = weight_ref.shape[:4]
    block = merged_ref.shape[2]
    for at in range(merged_ref.shape[0]):
        weight_grad = dot_tn(merged_ref[at], out_grad_ref[...])
        for inner in range(block // rows):
            index = (at * block + inner * rows) // rows
            dp_at, core_at, part_at = index // (cores * parts), index // parts % cores, index % parts
            weight_ref[core_at, dp_at, part_at] = weight_grad[inner * rows : (inner + 1) * rows].astype(jnp.bfloat16)
    for one in copies:
        one.wait_recv()
    wires.finish()


def input_grad_kernel(spread, qkv_grad_ref, w_ref, x_ref, gain_ref, middle_grad_ref, *rest):
    grad_ref, gain_grad_ref = rest[:2]
    rows_ref = rest[2] if spread else None
    rest = rest[3:] if spread else rest[2:]
    out_refs, (send, recv) = rest[:6], rest[6:]
    place = plane_place()
    me, core, near, far, cross = place
    wires = Wires(send, recv)
    greet(*plane_peers(place)[: 3 if spread else 2])
    totals = []
    run_all(cross_steps(wires, place, lambda spot: dot_nt(qkv_grad_ref[spot], w_ref[...]), out_refs, totals.append))
    normed_grad = totals[0]
    part, gain_grad_ref[...] = norm_back(x_ref[...], gain_ref[...], normed_grad)
    grad = middle_grad_ref[...] + part
    grad_ref[...] = grad
    if spread:
        rows_ref[me, core] = grad.astype(jnp.bfloat16)
        run_all(gather_steps(wires, rows_ref, place, True))
    wires.finish()


def comm_call(kernel, name, number, time, outs, scratch, wire_count, *operands):
    return pl.pallas_call(
        kernel,
        out_shape=tuple(outs),
        in_specs=vmem(len(operands)),
        out_specs=tuple(vmem(len(outs))),
        scratch_shapes=scratch + sems(wire_count),
        compiler_params=pltpu.CompilerParams(collective_id=number, has_side_effects=True),
        cost_estimate=cost(time),
        name=name,
    )(*operands)


def cost(time):
    return pl.CostEstimate(flops=0, bytes_accessed=int(time * 3e6), transcendentals=0)


def low_array(*shape):
    return jax.ShapeDtypeStruct(shape, jnp.bfloat16)


def wide_array(*shape):
    return jax.ShapeDtypeStruct(shape, jnp.float32)


def gelu_parts(values):
    square = values * values
    inner = jnp.tanh(values * (0.7978845608028654 + (0.7978845608028654 * 0.044715) * square))
    lift = 0.5 + 0.5 * inner
    slope = lift + (0.5 * values) * (1.0 - inner * inner) * (0.7978845608028654 + (3.0 * 0.7978845608028654 * 0.044715) * square)
    return values * lift, slope


def slot_hot(slot_row, capacity):
    rows = lax.broadcasted_iota(jnp.int32, (capacity, slot_row.shape[1]), 0)
    return (rows == slot_row).astype(jnp.bfloat16)


def one_of(pair_ref, index):
    values = pair_ref[:, index]
    return values.reshape(values.shape[0] * values.shape[1], values.shape[2])


def experts_kernel(tokens_ref, slot_ref, chosen_ref, own_ref, router_ref, pair_ref, part_ref, slots_ref, pre_ref, shares_ref):
    capacity = slots_ref.shape[0]
    tokens = tokens_ref[...]
    logits = jnp.where(chosen_ref[...] > 0, dot_nt(tokens, router_ref[...]), negative)
    raised = jnp.exp(logits - jnp.max(logits, axis=1, keepdims=True))
    shares = raised / jnp.sum(raised, axis=1, keepdims=True)
    shares_ref[...] = shares
    own_share = jnp.sum(shares * own_ref[...], axis=1, keepdims=True)
    hot = slot_hot(slot_ref[...], capacity)
    slots = dot(hot, tokens).astype(jnp.bfloat16)
    slots_ref[...] = slots
    pre = dot(slots, one_of(pair_ref, 0))
    pre_ref[...] = pre.astype(jnp.bfloat16)
    hidden = gelu_parts(pre)[0].astype(jnp.bfloat16)
    result = dot_nt(hidden, one_of(pair_ref, 1)).astype(jnp.bfloat16)
    part_ref[...] = (own_share * dot_tn(hot, result)).astype(jnp.bfloat16)


class Replay(Wires):
    def __init__(self, send, recv, ref, place, stage):
        super().__init__(send, recv)
        self.stage, self.now = stage, 0
        task = gather_steps(self, ref, place, False)
        for self.now in range(1, stage + 1):
            next(task, None)
        if stage == 5:
            self.finish()

    def copy(self, src, dst, where):
        one = pltpu.make_async_remote_copy(
            src_ref=src, dst_ref=dst, send_sem=self.send.at[self.next], recv_sem=self.recv.at[self.next],
            device_id=where, device_id_type=MESH_ID,
        )
        self.next += 1
        if self.now == self.stage:
            one.start()
        self.started.append(one)
        return Held(one, self)


class Held:
    def __init__(self, one, owner):
        self.one, self.owner = one, owner

    def wait_recv(self):
        if self.owner.now == self.owner.stage or self.owner.stage == 5 and self.owner.now > 2:
            self.one.wait_recv()


def experts_back_kernel(rows_ref, tokens_ref, slot_ref, shares_ref, own_ref, router_ref, pair_ref, slots_ref, pre_ref,
                        *refs):
    group, last = pl.program_id(0), pl.num_programs(0) - 1
    if len(refs) > 6:
        shard_ref, part_ref, pair_grad_ref, router_grad_ref, shared_ref, up_acc, down_acc, landing, send, recv = refs

        @pl.when(group == 0)
        def _():
            place = plane_place()
            greet({"seq": place[2]}, {"seq": place[3]})
            landing[place[0]] = shard_ref[1]
            Replay(send, recv, landing, plane_place(), 1)

        @pl.when(group == 2)
        def _():
            Replay(send, recv, landing, plane_place(), 2)

    else:
        part_ref, pair_grad_ref, router_grad_ref, up_acc, down_acc = refs
        shared_ref = None

    @pl.when(group == 0)
    def _():
        up_acc[...] = jnp.zeros_like(up_acc)
        down_acc[...] = jnp.zeros_like(down_acc)
        router_grad_ref[...] = jnp.zeros_like(router_grad_ref)

    capacity = slots_ref.shape[0]
    shares = shares_ref[...]
    own = own_ref[...]
    own_share = jnp.sum(shares * own, axis=1, keepdims=True)
    hot = slot_hot(slot_ref[...], capacity)
    scaled_rows = (own_share * rows_ref[...].astype(jnp.float32)).astype(jnp.bfloat16)
    result_grad = dot(hot, scaled_rows).astype(jnp.bfloat16)
    hidden_grad = dot(result_grad, one_of(pair_ref, 1))
    hidden, slope = gelu_parts(pre_ref[...].astype(jnp.float32))
    pre_grad = (slope * hidden_grad).astype(jnp.bfloat16)
    pair_sum = jnp.sum(hidden * hidden_grad, axis=1, keepdims=True)
    down_acc[...] += dot_tn(result_grad, hidden.astype(jnp.bfloat16))
    up_acc[...] += dot_tn(slots_ref[...], pre_grad)
    slot_grad = dot_nt(pre_grad, one_of(pair_ref, 0)).astype(jnp.bfloat16)
    high = pair_sum.astype(jnp.bfloat16)
    rest = (pair_sum - high.astype(jnp.float32)).astype(jnp.bfloat16)
    token_pair = dot_tn(hot, jnp.concatenate([jnp.broadcast_to(high, (capacity, 128)), jnp.broadcast_to(rest, (capacity, 128))], axis=1))
    token_pair = token_pair[:, :1] + token_pair[:, 128:129]
    logit_grad = (token_pair * (own - shares)).astype(jnp.bfloat16)
    router_grad_ref[...] += dot_tn(logit_grad, tokens_ref[...])
    part_ref[...] = (dot_tn(hot, slot_grad) + dot(logit_grad, router_ref[...])).astype(jnp.bfloat16)

    @pl.when(group == last)
    def _():
        shape = pair_grad_ref.shape[:1] + pair_grad_ref.shape[2:]
        pair_grad_ref[:, 0] = up_acc[...].astype(jnp.bfloat16).reshape(shape)
        pair_grad_ref[:, 1] = down_acc[...].astype(jnp.bfloat16).reshape(shape)

    if shared_ref is not None:

        @pl.when(group == last)
        def _():
            Replay(send, recv, landing, plane_place(), 5)
            shared_ref[...] = landing[...]


def by_group(*shape):
    return pl.BlockSpec((None,) + shape, lambda g: (g,) + (0,) * len(shape))


def held(*shape):
    return pl.BlockSpec(shape, lambda g: (0,) * len(shape), pipeline_mode=pl.Buffered(1))


def run_experts(tokens, slot, chosen, own, router, pair, capacity):
    groups, rows, width = tokens.shape
    experts, wide_ff = router.shape[0], pair.shape[3]
    return pl.pallas_call(
        experts_kernel,
        grid=(groups,),
        out_shape=(low_array(groups, rows, width), low_array(groups, capacity, width), low_array(groups, capacity, wide_ff),
                   wide_array(groups, rows, experts)),
        in_specs=[by_group(rows, width), by_group(1, rows), by_group(rows, experts), held(1, experts), held(experts, width),
                  held(*pair.shape)],
        out_specs=(by_group(rows, width), by_group(capacity, width), by_group(capacity, wide_ff), by_group(rows, experts)),
        compiler_params=pltpu.CompilerParams(dimension_semantics=("arbitrary",)),
        cost_estimate=cost(14.0),
        name="experts",
    )(tokens, slot, chosen, own, router, pair)


def run_experts_back(rows_grad, tokens, slot, shares, own, router, pair, slots, pre, shard=None):
    groups, rows, width = tokens.shape
    experts, wide_ff = router.shape[0], pair.shape[3]
    capacity = slots.shape[1]
    outs = [low_array(groups, rows, width), low_array(*pair.shape), wide_array(experts, width)]
    out_specs = [by_group(rows, width), held(*pair.shape), held(experts, width)]
    in_specs = [by_group(rows, width), by_group(rows, width), by_group(1, rows), by_group(rows, experts), held(1, experts),
                held(experts, width), held(*pair.shape), by_group(capacity, width), by_group(capacity, wide_ff)]
    scratch = [pltpu.VMEM((width, wide_ff), jnp.float32), pltpu.VMEM((width, wide_ff), jnp.float32)]
    operands = [rows_grad, tokens, slot, shares, own, router, pair, slots, pre]
    options = {}
    if shard is not None:
        operands.append(shard)
        in_specs.append(held(*shard.shape))
        outs.append(low_array(4, *shard.shape[1:]))
        out_specs.append(held(4, *shard.shape[1:]))
        scratch += [pltpu.VMEM((4,) + shard.shape[1:], jnp.bfloat16)] + sems(6)
        options = {"collective_id": 13, "has_side_effects": True}
    return pl.pallas_call(
        experts_back_kernel,
        grid=(groups,),
        out_shape=tuple(outs),
        in_specs=in_specs,
        out_specs=tuple(out_specs),
        scratch_shapes=scratch,
        compiler_params=pltpu.CompilerParams(dimension_semantics=("arbitrary",), **options),
        cost_estimate=cost(25.0),
        name="experts_back" if shard is None else "experts_back_share",
    )(*operands)


def dp_peers():
    me, count = lax.axis_index("dp"), lax.axis_size("dp")
    return me, [lax.rem(me + step, count) for step in range(1, count)], [lax.rem(me + count - step, count) for step in range(1, count)]


def line_start(wires, own_ref, all_ref, core, me, targets):
    half = own_ref.at[core]
    copies = [wires.copy(half, all_ref.at[me, core], {"dp": spot}) for spot in targets]
    all_ref[me] = own_ref[...]
    return copies


def line_forward(wires, all_ref, core, copies, sources):
    onward = []
    for one, spot in zip(copies, sources):
        one.wait_recv()
        block = all_ref.at[spot, core]
        onward.append(wires.copy(block, block, {"tensor": 1 - core}))
    return onward


def weights_kernel(small_ref, whole_ref, outs_ref, small_all, qkv_all, qkv_next, one_piece, two_piece, own_ref, send, recv):
    core, place = lax.axis_index("tensor"), lax.axis_index("seq")
    me, targets, sources = dp_peers()
    wires = Wires(send, recv)
    greet(*[{"dp": spot} for spot in targets], {"tensor": 1 - core})
    smalls = [wires.copy(small_ref, small_all.at[me], {"dp": spot}) for spot in targets]
    small_all[me] = small_ref[...]
    layers, rows, columns = whole_ref.shape
    part, parts = columns // 3, lax.axis_size("seq")
    size = part // parts
    for spot in range(parts):

        @pl.when(place == spot)
        def _():
            for layer, target in enumerate((own_ref, qkv_next)):
                pieces = [whole_ref[layer, :, kind * part + spot * size : kind * part + (spot + 1) * size] for kind in range(3)]
                pieces = jnp.concatenate(pieces, axis=1)
                target[0] = pieces[: rows // 2]
                target[1] = pieces[rows // 2 :]

    qkvs = line_start(wires, own_ref, qkv_all, core, me, targets)
    half = one_piece.shape[-1]
    chosen = pl.ds(pl.multiple_of(core * half, half), half)
    for layer, piece in enumerate((one_piece, two_piece)):
        smalls += [wires.copy(outs_ref.at[layer, place, :, chosen], piece.at[me], {"dp": spot}) for spot in targets]
        piece[me] = outs_ref[layer, place, :, chosen]
    onward = line_forward(wires, qkv_all, core, qkvs, sources)
    for one in smalls + onward:
        one.wait_recv()
    wires.finish()


def reduce_steps(wires, place, line, plane_first, q_ref, o_ref, o_out, scratch):
    me, core, near, far, cross = place
    line_me, targets, sources = line
    q_in, q_sum, q_line, q_out, o_in, o_line, o_sum, o_seq = scratch
    others, partner = (cross, near, far), {"tensor": 1 - core}
    q_first = wires.copy(q_ref.at[1 - core], q_in, partner)
    o_first = wires.copy(o_ref.at[1 - core], o_in, partner)
    yield
    q_first.wait_recv()
    q_sum[...] = (wide(q_ref[core]) + wide(q_in[...])).astype(jnp.bfloat16)
    q_copies = [wires.copy(q_sum.at[spot], q_line.at[line_me], {"dp": spot}) for spot in targets]
    q_line[line_me] = q_sum[line_me]
    o_first.wait_recv()
    o_in[...] = (wide(o_ref[core]) + wide(o_in[...])).astype(jnp.bfloat16)
    if plane_first:
        o_copies = [wires.copy(o_in.at[:, spot], o_seq.at[me], {"seq": spot}) for spot in others]
        o_seq[me] = o_in[:, me]
    else:
        o_copies = [wires.copy(o_in.at[spot], o_line.at[line_me], {"dp": spot}) for spot in targets]
        o_line[line_me] = o_in[line_me]
    yield

    def line_total(ref, copies):
        for one in copies:
            one.wait_recv()
        total = wide(ref[0])
        for spot in range(1, len(targets) + 1):
            total = total + wide(ref[spot])
        return total.astype(jnp.bfloat16)

    def spread(out):
        mine = out.at[core, me]
        return (out, [wires.copy(mine, mine, {"seq": spot}) for spot in others], [wires.copy(mine, mine, partner)])

    def plane_total(copies):
        for one in copies:
            one.wait_recv()
        return (wide(o_seq[0]) + wide(o_seq[1]) + wide(o_seq[2]) + wide(o_seq[3])).astype(jnp.bfloat16)

    if plane_first:
        o_sum[...] = plane_total(o_copies)
        next_copies = [wires.copy(o_sum.at[spot], o_line.at[line_me], {"dp": spot}) for spot in targets]
        o_line[line_me] = o_sum[line_me]
        yield
        q_out[core, me] = line_total(q_line, q_copies)
        last = [spread(q_out)]
        yield
        o_out[core, me] = line_total(o_line, next_copies)
    else:
        q_out[core, me] = line_total(q_line, q_copies)
        last = [spread(q_out)]
        yield
        o_sum[...] = line_total(o_line, o_copies)
        next_copies = [wires.copy(o_sum.at[spot], o_seq.at[me], {"seq": spot}) for spot in others]
        o_seq[me] = o_sum[me]
        yield
        o_out[core, me] = plane_total(next_copies)
    last.append(spread(o_out))
    yield
    for out, copies, onward in last:
        for one, spot in zip(copies, others):
            one.wait_recv()
            block = out.at[core, spot]
            onward.append(wires.copy(block, block, partner))
    yield
    for out, copies, onward in last:
        for one in onward:
            one.wait_recv()


def small_steps(wires, place, line, s_ref, s_out, scratch):
    me, core, near, far, cross = place
    line_me, targets, sources = line
    s_in, s_sum, s_line, s_tot, s_seq = scratch
    partner = {"tensor": 1 - core}
    one = wires.copy(s_ref.at[1 - core], s_in, partner)
    yield
    one.wait_recv()
    s_sum[...] = s_ref[core] + s_in[...]
    copies = [wires.copy(s_sum.at[spot], s_line.at[line_me], {"dp": spot}) for spot in targets]
    s_line[line_me] = s_sum[line_me]
    yield
    for one in copies:
        one.wait_recv()
    s_tot[...] = jnp.sum(s_line[...], axis=0)
    copies = [wires.copy(s_tot, s_seq.at[me], {"seq": spot}) for spot in (cross, near, far)]
    s_seq[me] = s_tot[...]
    yield
    for one in copies:
        one.wait_recv()
    s_out[core] = jnp.sum(s_seq[...], axis=0)
    mine = s_out.at[core]
    one = wires.copy(mine, mine, partner)
    yield
    one.wait_recv()


def finish_kernel(layers, *refs):
    def take(number):
        nonlocal refs
        first, refs = refs[:number], refs[number:]
        return first

    q_refs, o_refs, s_refs = take(layers), take(layers), take(layers)
    qkv_grad_ref, w_ref, x_ref, gain_ref, middle_grad_ref = take(5)
    (total_ref, grad_ref), o_outs, s_outs = take(2), take(layers), take(layers)
    scratch = [take(8) for _ in range(layers)]
    small_scratch = [take(5) for _ in range(layers)]
    (s_own,), out_refs = take(1), take(6)
    place, line = plane_place(), dp_peers()
    me, core, near, far, cross = place
    wires = Wires(*refs)
    greet({"seq": near}, {"seq": far}, {"seq": cross}, {"tensor": 1 - core}, *[{"dp": spot} for spot in line[1]])

    def input_steps():
        totals = []
        yield from cross_steps(wires, place, lambda spot: dot_nt(qkv_grad_ref[spot], w_ref[...]), out_refs, totals.append)
        part, gain_grad = norm_back(x_ref[...], gain_ref[...], totals[0])
        grad_ref[...] = middle_grad_ref[...] + part
        s_own[...] = s_refs[0][...]
        size = s_own.shape[3]
        for at in range(s_own.shape[1]):
            s_own[0, at, 0:1, :] = gain_grad[:, at * size : (at + 1) * size]
        yield
        yield from small_steps(wires, place, line, s_own, s_outs[0], small_scratch[0])

    reduces = [reduce_steps(wires, place, line, True, *one) for at, one in enumerate(zip(q_refs, o_refs, o_outs, scratch))]
    inputs = input_steps()
    for task in reduces:
        next(task)
    next(inputs)
    for task in reduces:
        next(task)
    smalls = [small_steps(wires, place, line, s_refs[at], s_outs[at], small_scratch[at]) for at in range(1, layers)]
    run_all(inputs, *reduces, *smalls)
    rows = total_ref.shape[1] // 2
    for layer in range(layers):
        whole = scratch[layer][3]
        size = whole.shape[-1] // 3
        for half in range(2):
            pieces = [whole[half, spot][:, kind * size : (kind + 1) * size] for kind in range(3) for spot in range(4)]
            total_ref[layer, half * rows : (half + 1) * rows, :] = wide(jnp.concatenate(pieces, axis=1))
    wires.finish()


def share_kernel(pair_ref, one_ref, two_ref, send, recv):
    place = plane_place()
    wires = Wires(send, recv)
    greet({"seq": place[2]}, {"seq": place[3]})
    tasks = []
    for at, dst in enumerate((one_ref, two_ref)):
        dst[place[0]] = pair_ref[at]
        tasks.append(gather_steps(wires, dst, place, False))
    run_all(*tasks)
    wires.finish()
def body(
    block_input,
    segments,
    routes,
    distance_bucket,
    first_gain,
    query_key_value,
    attention_out,
    bias_table,
    second_gain,
    router_weights,
    expert_up,
    expert_down,
    cotangent,
):
    low = jnp.bfloat16
    seq_count, piece, width = block_input.shape
    n_dp, n_seq, n_tensor = (lax.axis_size(name) for name in ("dp", "seq", "tensor"))
    n_plane = n_seq * n_tensor
    length = piece * n_seq
    local_heads = HEADS // n_seq
    head_width = local_heads * HD
    experts = expert_up.shape[1]
    assert seq_count == 1 and experts == n_seq
    shard = width // n_dp
    bucket_count = bias_table.shape[1] * n_dp
    bucket_shard = bias_table.shape[1]
    group_rows = n_tensor * piece
    capacity = group_rows * routes.shape[-1] // experts
    seq_index = lax.axis_index("seq")
    span = ROWS + length // 2


    assert n_seq == 4 and n_tensor == 2
    half = shard // n_tensor

    def padded(values):
        return jnp.pad(values, ((0, 0), (0, shard - values.shape[1])))

    small = jnp.concatenate(
        [
            first_gain,
            second_gain,
            router_weights.swapaxes(1, 2).reshape(-1, shard),
            padded(bias_table.reshape(LAYERS, -1)),
        ]
    )
    small_rows = small.shape[0]
    small = jnp.pad(small, ((0, -small_rows % 16), (0, 0)))
    own_out = attention_out.reshape(LAYERS, n_seq, shard // n_seq, width)
    own_up = lax.dynamic_index_in_dim(expert_up, seq_index, 1, keepdims=False)
    own_down = lax.dynamic_index_in_dim(expert_down, seq_index, 1, keepdims=False).swapaxes(1, 2)

    own_shape = (n_tensor, half, 3 * head_width)
    small_all, qkv_all, qkv_next, *out_pieces = comm_call(
        weights_kernel, "weights", 10, 22.0,
        [low_array(n_dp, *small.shape), low_array(n_dp, *own_shape), low_array(*own_shape)]
        + [low_array(n_dp, shard // n_seq, width // n_tensor)] * LAYERS,
        [pltpu.VMEM(own_shape, low)], 5 * (n_dp - 1), small, query_key_value, own_out
    )
    qkv_weights = [qkv_all]
    own_pair, small_all = lax.optimization_barrier((jnp.stack([own_up, own_down], axis=1), small_all))
    whole_rows = small_all.swapaxes(0, 1).reshape(-1, width)
    gains = whole_rows[: 2 * LAYERS].astype(jnp.float32).reshape(2, LAYERS, 1, width)
    routers = whole_rows[2 * LAYERS : 2 * LAYERS + LAYERS * experts].reshape(LAYERS, experts, width)
    tables = whole_rows[2 * LAYERS + LAYERS * experts : small_rows].reshape(LAYERS, n_dp, shard)[:, :, : bucket_shard * HEADS]
    tables = tables.reshape(LAYERS, bucket_count, HEADS).astype(jnp.float32)
    own_tables = lax.dynamic_slice_in_dim(tables, seq_index * local_heads, local_heads, 2)
    routes_own = routes.reshape(-1, 128)
    seg_row = segments
    seg_col = segments.reshape(length, 1)
    bucket_line = distance_bucket[length // 2 - 1 :: -1][: length // 2]
    bucket_line = jnp.concatenate(
        [jnp.full((1,), -1, jnp.int32), bucket_line, jnp.full((span - 1 - length // 2,), -1, jnp.int32)]
    )
    line_hot = (bucket_line[None, :] == lax.iota(jnp.int32, bucket_count)[:, None]).astype(jnp.float32)
    lines = jnp.einsum("lbh,bs->lhs", own_tables, line_hot, precision=highest_precision)
    strict_upper = (
        lax.iota(jnp.int32, group_rows)[:, None] < lax.iota(jnp.int32, group_rows)[None, :]
    ).astype(low)

    own_hot = (lax.iota(jnp.int32, experts) == seq_index).astype(jnp.float32)[None]

    current = block_input[0]
    grad = cotangent[0]
    saved = []
    for layer in range(LAYERS):
        pair = lax.all_gather(own_pair[layer], "dp", axis=0)
        gain_one, gain_two = gains[0, layer], gains[1, layer]
        qkv_weight = qkv_weights[layer].reshape(width, 3 * head_width)
        outs = [low_array(n_seq, piece, width), low_array(n_seq, piece, 3 * head_width)]
        if layer == 0:
            outs.append(jax.ShapeDtypeStruct((n_seq,) + routes_own.shape, jnp.int32))
            normed_all, qkv, routes_all = comm_call(
                project_kernel, "project", 1, 16.0, outs, [], 9, current, gain_one, qkv_weight, routes_own
            )
        else:
            current, normed_all, qkv = comm_call(
                sum_project_kernel, "sum_project", 2, 32.0, [wide_array(piece, width)] + outs,
                [pltpu.VMEM((n_seq, piece, width), low)] + sum_scratch(piece, width), 16, part, middle, gain_one, qkv_weight
            )
        qkv = qkv.reshape(length, 3 * head_width)
        if layer == 0:
            outs = [low_array(n_dp, *own_out.shape[1:])] * LAYERS
            mixed, log_total, *out_weights = attend(qkv, seg_row, seg_col, lines[layer], out_pieces, outs, "fetch", 6, 8)
        else:
            outs = [low_array(n_seq, n_tensor, piece, width)]
            mixed, log_total, grad_rows = attend(qkv, seg_row, seg_col, lines[layer], (grad,), outs, "gather", 14, 11)
        out_weight = out_weights[layer].reshape(n_seq, head_width, width)
        fetch = layer == 0
        outs = [low_array(n_seq, piece, head_width), wide_array(piece, width), low_array(n_seq, n_tensor, piece, width)]
        outs += [low_array(n_dp, *own_shape)] if fetch else []
        operands = (mixed.reshape(n_seq, piece, head_width), current, out_weight, gain_two) + ((qkv_next,) if fetch else ())
        merged, middle, tokens, *more = comm_call(
            functools.partial(merge_kernel, fetch), "merge_fetch" if fetch else "merge", 15 if fetch else 3, 25.0, outs, [],
            14 + (2 * (n_dp - 1) if fetch else 0), *operands
        )
        qkv_weights += more
        if layer == 0:
            routes_all, tokens = lax.optimization_barrier((routes_all, tokens))
            routes_all = jnp.moveaxis(routes_all.reshape((n_seq,) + routes.shape), 0, 1).reshape(LAYERS, n_seq, group_rows, -1)
            mine = jnp.any(routes_all == seq_index, axis=-1)
            slot = dot(mine.reshape(-1, group_rows).astype(low), strict_upper).astype(jnp.int32).reshape(mine.shape)
            slot = jnp.where(mine & (slot < capacity), slot, -1)[:, :, None]
            chosen = jnp.any(routes_all[..., None] == lax.iota(jnp.int32, experts), axis=3).astype(jnp.float32)
        tokens = tokens.reshape(n_seq, group_rows, width)
        part, slots, pre, shares = run_experts(tokens, slot[layer], chosen[layer], own_hot, routers[layer], pair, capacity)
        part = part.reshape(n_seq, n_tensor, piece, width)
        saved.append((current, normed_all, qkv, log_total, merged, middle, tokens, shares, slots, pre, qkv_weight, out_weight, pair))

    last_part, last_middle = part, middle

    pair_shards, qkv_grads, out_grads, smalls = ([None] * LAYERS for _ in range(4))
    out_rows = half // n_seq
    for layer in range(LAYERS - 1, -1, -1):
        (layer_in, normed_all, qkv, log_total, merged, middle, tokens, shares, slots, pre, qkv_weight, out_weight, pair) = saved[layer]
        gain_one, gain_two = gains[0, layer], gains[1, layer]
        part, pair_grad, router_grad, *shared = run_experts_back(
            grad_rows.reshape(n_seq, group_rows, width), tokens, slot[layer], shares, own_hot, routers[layer], pair, slots, pre,
            pair_shards[1] if layer == 0 else None
        )
        pair_shards[layer] = lax.psum_scatter(pair_grad, "dp", scatter_dimension=0, tiled=True)[0]
        middle_grad, gain_two_grad, mixed_grad, out_grads[layer] = comm_call(
            split_kernel, "split", 5, 25.0,
            [wide_array(piece, width), wide_array(1, width), low_array(n_seq, piece, head_width),
             low_array(n_tensor, n_dp, n_seq, out_rows, width)],
            [pltpu.VMEM((piece, width), low), pltpu.VMEM((n_seq, piece, head_width), low), pltpu.VMEM((n_seq, piece, width), low)]
            + sum_scratch(piece, width), 13,
            part.reshape(n_seq, n_tensor, piece, width), middle, gain_two, grad, out_weight, merged
        )
        operands = (qkv, seg_row, seg_col, lines[layer], log_total, mixed_grad.reshape(length, head_width))
        operands += (normed_all.reshape(length, width), (n_tensor, n_dp, half, 3 * head_width))
        if layer == 0:
            (down_last,) = shared
            outs = [low_array(n_seq, *pair_shards[1].shape[1:])]
            qkv_grad, band, qkv_grads[layer], up_last = attend_back(*operands, (pair_shards[1],), outs, [], "share", 9, 6)
            gain_one_grad = jnp.zeros((1, width), jnp.float32)
        else:
            outs = [wide_array(piece, width)]
            extra_scratch = [pltpu.VMEM((n_seq, piece, width), low)] + sum_scratch(piece, width)
            qkv_grad, band, qkv_grads[layer], block_output = attend_back(
                *operands, (last_part, last_middle), outs, extra_scratch, "sum", 4, 10
            )
            outs = [wide_array(piece, width), wide_array(1, width), low_array(n_seq, n_tensor, piece, width)]
            grad, gain_one_grad, grad_rows = comm_call(
                functools.partial(input_grad_kernel, True), "input_grad", 7, 32.0, outs, sum_scratch(piece, width), 17,
                qkv_grad.reshape(n_seq, piece, -1), qkv_weight, layer_in, gain_one, middle_grad
            )
        table_grad = jnp.dot(line_hot, band.T, precision=highest_precision)
        table_grad = lax.dynamic_update_slice_in_dim(
            jnp.zeros((bucket_count, HEADS), jnp.float32), table_grad, seq_index * local_heads, 1
        )
        table_grad = padded(table_grad.reshape(n_dp, -1)).reshape(1, width)
        packed = jnp.concatenate([gain_one_grad, gain_two_grad, router_grad, table_grad, jnp.zeros((1, width), jnp.float32)])
        smalls[layer] = packed.reshape(n_tensor, n_seq, n_dp, shard).swapaxes(1, 2)

    def reduce_scratch(plane_first):
        line = pltpu.VMEM((n_dp, half, 3 * head_width), low)
        blocks = pltpu.VMEM((n_dp, n_seq, out_rows, width), low)
        over_dp, over_seq = (pltpu.VMEM((count, out_rows, width), low) for count in (n_dp, n_seq))
        found = [line] * 3 + [pltpu.VMEM((n_tensor, n_seq, half, 3 * head_width), low), blocks]
        if plane_first:
            return found + [over_dp, over_dp, pltpu.VMEM((n_seq, n_dp, out_rows, width), low)]
        return found + [blocks, over_seq, over_seq]

    small_scratch = [pltpu.VMEM((n_dp, n_seq, shard), jnp.float32)] * 3 + [pltpu.VMEM((n_seq, shard), jnp.float32)]
    small_scratch += [pltpu.VMEM((n_seq, n_seq, shard), jnp.float32)]
    qkv_total, input_grad, *totals = comm_call(
        functools.partial(finish_kernel, LAYERS), "finish", 11, 75.0,
        [wide_array(LAYERS, shard, 3 * width), wide_array(piece, width)]
        + [low_array(n_tensor, n_seq, out_rows, width)] * LAYERS + [wide_array(n_tensor, n_seq, shard)] * LAYERS,
        reduce_scratch(True) + reduce_scratch(True) + small_scratch * LAYERS
        + [pltpu.VMEM((n_tensor, n_dp, n_seq, shard), jnp.float32)] + sum_scratch(piece, width),
        LAYERS * (2 * (n_dp - 1) + 19 + n_dp + 4) + 6,
        *qkv_grads, *out_grads, *smalls, qkv_grad.reshape(n_seq, piece, -1), qkv_weight, layer_in, gain_one, middle_grad
    )
    out_total = jnp.stack(totals[:LAYERS]).astype(jnp.float32).reshape(LAYERS, shard, width)
    small = jnp.stack(totals[LAYERS : 2 * LAYERS]).reshape(LAYERS, n_plane, shard)
    pair_last, small = lax.optimization_barrier((pair_shards[0], small))
    up_first, down_first = comm_call(
        share_kernel, "share", 12, 42.0, [low_array(n_seq, *pair_last.shape[1:])] * 2, [], 12, pair_last
    )
    router_total = small[:, 2 : 2 + experts].swapaxes(1, 2)
    table_total = small[:, 2 + experts, : bucket_shard * HEADS].reshape(LAYERS, bucket_shard, HEADS)
    up_total = jnp.stack([up_first, up_last]).astype(jnp.float32)
    down_total = jnp.stack([down_first, down_last]).astype(jnp.float32).swapaxes(2, 3)
    return (block_output[None], input_grad[None], small[:, 0], qkv_total, out_total, table_total, small[:, 1], router_total, up_total, down_total)


def solution(mesh):
    in_specs = (
        P(("dp", "tensor"), "seq", None),
        P(("dp", "tensor"), None),
        P(None, "dp", "seq", None),
        P(),
        P(None, "dp"),
        P(None, "dp", None),
        P(None, "dp", None),
        P(None, "dp", None),
        P(None, "dp"),
        P(None, "dp", None),
        P(None, None, "dp", "tensor"),
        P(None, None, "tensor", "dp"),
        P(("dp", "tensor"), "seq", None),
    )
    out_specs = (
        P(("dp", "tensor"), "seq", None),
        P(("dp", "tensor"), "seq", None),
        P(None, "dp"),
        P(None, "dp", None),
        P(None, "dp", None),
        P(None, "dp", None),
        P(None, "dp"),
        P(None, "dp", None),
        P(None, None, "dp", "tensor"),
        P(None, None, "tensor", "dp"),
    )
    return jax.shard_map(body, mesh=mesh, in_specs=in_specs, out_specs=out_specs, check_vma=False)
```

```python
import functools

import jax
import jax.numpy as jnp
from jax import lax
from jax.experimental import pallas as pl
from jax.experimental.pallas import tpu as pltpu
from jax.sharding import PartitionSpec as P

HEADS = 12
LAYERS = 2
epsilon = 1e-06
negative = -1e30
highest_precision = lax.Precision.HIGHEST


def scaled(values, gain_vec):
    return values * lax.rsqrt(jnp.mean(values * values, axis=-1, keepdims=True) + epsilon) * gain_vec


HD = 64
ROWS = 128
NT = (((1,), (1,)), ((), ()))
TN = (((0,), (0,)), ((), ()))


def visit_blocks(length, span, one_block, hook, hooks_at):
    full, count = span // ROWS, length // ROWS

    def step(i, carry):
        start = pl.multiple_of(i * ROWS, ROWS)
        one_block(start, pl.multiple_of(start + ROWS - span, ROWS), span)
        return carry

    for i in range(full - 1):
        if i in hooks_at:
            hook()
        one_block(i * ROWS, 0, (i + 1) * ROWS)
    stops = [full - 1] + [i for i in range(full - 1, count) if i in hooks_at] + [count]
    for low, high in zip(stops, stops[1:]):
        if low in hooks_at:
            hook()
        lax.fori_loop(low, high, step, 0)


def background(tasks):
    tasks = list(tasks)

    def hook():
        tasks[:] = [task for task in tasks if next(task, wires_done) is not wires_done]

    return hook, lambda: run_all(*tasks)


def fill_mask(mask_ref, segr_ref, segc_ref, start, low, width):
    same = segc_ref[pl.ds(start, ROWS), :] == segr_ref[:, pl.ds(low, width)]
    back = lax.broadcasted_iota(jnp.int32, (ROWS, width), 0) + (width - ROWS)
    allowed = same & (back >= lax.broadcasted_iota(jnp.int32, (ROWS, width), 1))
    mask_ref[:, :width] = jnp.where(allowed, 0.0, -1e30)


def fill_slab(slab_ref, line_ref, heads, span):
    for h in range(heads):
        spread = jnp.broadcast_to(line_ref[h : h + 1, :], (ROWS, span))
        slab_ref[h] = pltpu.roll(spread, 0, 1, stride=1, stride_axis=0)


def split_heads(qkv_ref, parts_ref, heads):
    for h in range(3 * heads):
        part = qkv_ref[:, h * HD : (h + 1) * HD]
        parts_ref[h] = part * jnp.bfloat16(0.125) if h < heads else part


def fetch_steps(wires, place, own, whole):
    me, core, near, far, cross = place
    width = whole.shape[-1]
    columns = pl.ds(pl.multiple_of(core * (width // 2), width // 2), width // 2)
    around = [wires.copy(own, whole.at[:, me, :, columns], {"seq": spot}) for spot in (cross, near, far)]
    whole[:, me, :, columns] = own[...]
    yield
    for one in around:
        one.wait_recv()
    block = whole.at[:, :, :, columns]
    onward = wires.copy(block, block, {"tensor": 1 - core})
    yield
    onward.wait_recv()


def attn_fwd_kernel(heads, span, mode, *refs):
    qkv_ref, segr_ref, segc_ref, line_ref = refs[:4]
    place = plane_place()
    me, core, near, far, cross = place
    wires = Wires(*refs[-2:])
    if mode == "fetch":
        own_refs, (out_ref, lse_ref), whole_refs, scratch = refs[4:6], refs[6:8], refs[8:10], refs[10:14]
        greet({"seq": near}, {"seq": far}, {"seq": cross}, {"tensor": 1 - core})
        tasks = [fetch_steps(wires, place, *pair) for pair in zip(own_refs, whole_refs)]
        hooks_at = (6,)
    else:
        rows_ref, out_ref, lse_ref, gathered_ref = refs[4:8]
        scratch = refs[8:12]
        greet(*plane_peers(place))
        gathered_ref[me, core] = rows_ref[...].astype(jnp.bfloat16)
        tasks = [gather_steps(wires, gathered_ref, place, True)]
        hooks_at = (4, 6)
    hook, finish = background(tasks)
    hook()
    parts_ref, mixed_ref, slab_ref, mask_ref = scratch
    length = qkv_ref.shape[0]
    fill_slab(slab_ref, line_ref, heads, span)
    split_heads(qkv_ref, parts_ref, heads)

    def one_block(start, low, width):
        fill_mask(mask_ref, segr_ref, segc_ref, start, low, width)

        def one_head(h, carry):
            q = parts_ref[h, pl.ds(start, ROWS), :]
            k = parts_ref[heads + h, pl.ds(low, width), :]
            v = parts_ref[2 * heads + h, pl.ds(low, width), :]
            s = lax.dot_general(q, k, NT, preferred_element_type=jnp.float32)
            s = s + slab_ref[h, :, span - width :] + mask_ref[:, :width]
            top = jnp.max(s, axis=1, keepdims=True)
            e = jnp.exp(s - top)
            total = jnp.sum(e, axis=1, keepdims=True)
            mixed = jnp.dot(e.astype(jnp.bfloat16), v, preferred_element_type=jnp.float32)
            mixed_ref[h, pl.ds(start, ROWS), :] = (mixed / total).astype(jnp.bfloat16)
            lse_ref[h, pl.ds(start, ROWS), :] = top + jnp.log(total)
            return carry

        lax.fori_loop(0, heads, one_head, 0, unroll=True)

    visit_blocks(length, span, one_block, hook, hooks_at)
    out_ref[...] = jnp.concatenate([mixed_ref[h] for h in range(heads)], axis=1)
    finish()
    wires.finish()


def attn_bwd_kernel(heads, span, mode, *refs):
    qkv_ref, segr_ref, segc_ref, line_ref, lse_ref, grad_ref, normed_ref = refs[:7]
    place = plane_place()
    me, core, near, far, cross = place
    wires = Wires(*refs[-2:])
    if mode == "share":
        shard_ref, out_ref, band_ref, weight_ref, shared_ref = refs[7:12]
        greet({"seq": near}, {"seq": far})
        shared_ref[me] = shard_ref[0]
        tasks = [gather_steps(wires, shared_ref, place, False)]
        refs = refs[12:20]
    else:
        part_ref, base_ref, out_ref, band_ref, weight_ref, total_ref = refs[7:13]
        greet(*plane_peers(place))
        tasks = [plane_sum_steps(wires, place, part_ref, refs[21], refs[22:28], add_to(total_ref, base_ref))]
        refs = refs[13:21]
    hook, finish = background(tasks)
    hook()
    parts_ref, gparts_ref, qgrad_ref, kgrad_ref, vgrad_ref, slab_ref, mask_ref, band_acc = refs
    length = qkv_ref.shape[0]
    fill_slab(slab_ref, line_ref, heads, span)
    split_heads(qkv_ref, parts_ref, heads)
    for h in range(heads):
        gparts_ref[h] = grad_ref[:, h * HD : (h + 1) * HD]
    kgrad_ref[...] = jnp.zeros_like(kgrad_ref)
    vgrad_ref[...] = jnp.zeros_like(vgrad_ref)
    band_acc[...] = jnp.zeros_like(band_acc)

    def one_block(start, low, width):
        fill_mask(mask_ref, segr_ref, segc_ref, start, low, width)

        def one_head(h, carry):
            rows = pl.ds(start, ROWS)
            window = pl.ds(low, width)
            q = parts_ref[h, rows, :]
            k = parts_ref[heads + h, window, :]
            v = parts_ref[2 * heads + h, window, :]
            grad = gparts_ref[h, rows, :]
            s = lax.dot_general(q, k, NT, preferred_element_type=jnp.float32)
            s = s + slab_ref[h, :, span - width :] + mask_ref[:, :width]
            p = jnp.exp(s - lse_ref[h, rows, :])
            dp = lax.dot_general(grad, v, NT, preferred_element_type=jnp.float32)
            inner = jnp.sum(p * dp, axis=1, keepdims=True)
            ds = p * (dp - inner)
            band_acc[h, :, span - width :] += ds
            ds = ds.astype(jnp.bfloat16)
            qgrad = jnp.dot(ds, k, preferred_element_type=jnp.float32)
            qgrad_ref[h, rows, :] = (qgrad * 0.125).astype(jnp.bfloat16)
            kgrad_ref[h, window, :] += lax.dot_general(ds, q, TN, preferred_element_type=jnp.float32)
            vgrad_ref[h, window, :] += lax.dot_general(p.astype(jnp.bfloat16), grad, TN, preferred_element_type=jnp.float32)
            return carry

        lax.fori_loop(0, heads, one_head, 0, unroll=True)

    visit_blocks(length, span, one_block, hook, (5, 7) if mode == "share" else (3, 6))
    parts = [qgrad_ref[h] for h in range(heads)]
    parts += [kgrad_ref[h].astype(jnp.bfloat16) for h in range(heads)]
    parts += [vgrad_ref[h].astype(jnp.bfloat16) for h in range(heads)]
    out_ref[...] = jnp.concatenate(parts, axis=1)
    weight_grad = dot_tn(normed_ref[...], out_ref[...])
    rows = weight_ref.shape[2]
    for at in range(weight_ref.shape[1]):
        for core_at in range(weight_ref.shape[0]):
            first = (at * weight_ref.shape[0] + core_at) * rows
            weight_ref[core_at, at] = weight_grad[first : first + rows].astype(jnp.bfloat16)
    row = lax.broadcasted_iota(jnp.int32, (ROWS, span), 0)
    for h in range(heads):
        acc = band_acc[h]
        bit = 1
        while bit < ROWS:
            acc = jnp.where((row & bit) != 0, pltpu.roll(acc, span - bit, 1), acc)
            bit *= 2
        band_ref[h : h + 1, :] = jnp.sum(acc, axis=0, keepdims=True)
    finish()
    wires.finish()


def vmem(count):
    return [pl.BlockSpec(memory_space=pltpu.VMEM)] * count


def attend_scratch(heads, length, span):
    return [
        pltpu.VMEM((3 * heads, length, HD), jnp.bfloat16),
        pltpu.VMEM((heads, length, HD), jnp.bfloat16),
        pltpu.VMEM((heads, ROWS, span), jnp.float32),
        pltpu.VMEM((ROWS, span), jnp.float32),
    ]


def attend(qkv, seg_row, seg_col, line, extra, extra_outs, mode, number, wire_count):
    length, width = qkv.shape
    heads, span = line.shape
    outs = [low_array(length, heads * HD), wide_array(heads, length, 1)] + extra_outs
    return comm_call(functools.partial(attn_fwd_kernel, heads, span, mode), "attend_" + mode, number, 18.0, outs,
                     attend_scratch(heads, length, span), wire_count, qkv, seg_row, seg_col, line, *extra)


def attend_back(qkv, seg_row, seg_col, line, lse, grad, normed, weight_shape, extra, extra_outs, extra_scratch, mode, number, wire_count):
    length, width = qkv.shape
    heads, span = line.shape
    outs = [low_array(length, width), wide_array(heads, span), low_array(*weight_shape)] + extra_outs
    scratch = [
        pltpu.VMEM((3 * heads, length, HD), jnp.bfloat16),
        pltpu.VMEM((heads, length, HD), jnp.bfloat16),
        pltpu.VMEM((heads, length, HD), jnp.bfloat16),
        pltpu.VMEM((heads, length, HD), jnp.float32),
        pltpu.VMEM((heads, length, HD), jnp.float32),
        pltpu.VMEM((heads, ROWS, span), jnp.float32),
        pltpu.VMEM((ROWS, span), jnp.float32),
        pltpu.VMEM((heads, ROWS, span), jnp.float32),
    ]
    return comm_call(functools.partial(attn_bwd_kernel, heads, span, mode), "attend_back_" + mode, number, 23.0, outs,
                     scratch + extra_scratch, wire_count, qkv, seg_row, seg_col, line, lse, grad, normed, *extra)


MESH_ID = pl.DeviceIdType.MESH


class Wires:
    def __init__(self, send, recv):
        self.send, self.recv, self.next, self.started = send, recv, 0, []

    def copy(self, src, dst, where):
        one = pltpu.make_async_remote_copy(
            src_ref=src, dst_ref=dst, send_sem=self.send.at[self.next], recv_sem=self.recv.at[self.next],
            device_id=where, device_id_type=MESH_ID,
        )
        self.next += 1
        one.start()
        self.started.append(one)
        return one

    def finish(self):
        for one in self.started:
            one.wait_send()


def plane_place():
    me = lax.axis_index("seq")
    core = lax.axis_index("tensor")
    near, far = me + 1 - 2 * lax.rem(me, 2), lax.rem(me + 2, 4)
    cross = lax.rem(near + 2, 4)
    return me, core, near, far, cross


def greet(*places):
    barrier = pltpu.get_barrier_semaphore()
    for where in places:
        pl.semaphore_signal(barrier, inc=1, device_id=where, device_id_type=MESH_ID)
    pl.semaphore_wait(barrier, len(places))


def gather_steps(wires, ref, place, paired):
    me, core, near, far, cross = place
    half = ref.shape[-2] // 2
    to_near, to_far, partner = {"seq": near}, {"seq": far}, {"tensor": 1 - core}

    def part(spot, start, size):
        return ref.at[spot, core, pl.ds(start, size)] if paired else ref.at[spot, pl.ds(start, size)]

    def send(spot, start, size, where):
        block = part(spot, start, size)
        return wires.copy(block, block, where)

    near_top = send(me, 0, half, to_near)
    far_low = send(me, half, half, to_far)
    near_low = send(me, half, half, to_near)
    far_top = send(me, 0, half, to_far)
    inside = [send(me, 0, 2 * half, partner)] if paired else []
    yield
    near_top.wait_recv()
    cross_top = send(near, 0, half, to_far)
    far_low.wait_recv()
    cross_low = send(far, half, half, to_near)
    yield
    near_low.wait_recv()
    inside += [send(near, 0, 2 * half, partner)] if paired else []
    far_top.wait_recv()
    inside += [send(far, 0, 2 * half, partner)] if paired else []
    yield
    cross_top.wait_recv()
    inside += [send(cross, 0, half, partner)] if paired else []
    cross_low.wait_recv()
    inside += [send(cross, half, half, partner)] if paired else []
    yield
    for one in inside:
        one.wait_recv()


def run_all(*tasks):
    tasks = list(tasks)
    while tasks:
        tasks = [task for task in tasks if next(task, wires_done) is not wires_done]


wires_done = object()


def wide(values):
    return values.astype(jnp.float32)


def cross_steps(wires, place, total_of, out_refs, done):
    me, core, near, far, cross = place
    cross_ref, near_ref, far_ref, cross_in, near_in, far_in = out_refs
    half = near_ref.shape[0] // 2
    top, bottom = pl.ds(0, half), pl.ds(half, half)
    cross_ref[...] = total_of(cross).astype(cross_ref.dtype)
    to_near = wires.copy(cross_ref.at[top], cross_in.at[top], {"seq": near})
    to_far = wires.copy(cross_ref.at[bottom], cross_in.at[bottom], {"seq": far})
    near_ref[...] = total_of(near).astype(near_ref.dtype)
    near_one = wires.copy(near_ref.at[top], near_in.at[top], {"seq": near})
    far_ref[...] = total_of(far).astype(far_ref.dtype)
    far_one = wires.copy(far_ref.at[bottom], far_in.at[bottom], {"seq": far})
    yield
    to_near.wait_recv()
    far_ref[top, :] = (wide(far_ref[top, :]) + wide(cross_in[top, :])).astype(far_ref.dtype)
    far_two = wires.copy(far_ref.at[top], far_in.at[top], {"seq": far})
    to_far.wait_recv()
    near_ref[bottom, :] = (wide(near_ref[bottom, :]) + wide(cross_in[bottom, :])).astype(near_ref.dtype)
    near_two = wires.copy(near_ref.at[bottom], near_in.at[bottom], {"seq": near})
    own = total_of(me)
    yield
    for one in (near_one, far_one, far_two, near_two):
        one.wait_recv()
    done(own + wide(near_in[...]) + wide(far_in[...]))


def plane_sum_steps(wires, place, part_ref, partner_in, out_refs, done):
    me, core, near, far, cross = place
    arrivals = {}
    for name, spot in (("cross", cross), ("near", near), ("far", far), ("me", me)):
        arrivals[name] = wires.copy(part_ref.at[spot, 1 - core], partner_in.at[spot], {"tensor": 1 - core})
    order = iter(("cross", "near", "far", "me"))

    def total_of(spot):
        arrivals[next(order)].wait_recv()
        return wide(part_ref[spot, core]) + wide(partner_in[spot])

    yield
    yield from cross_steps(wires, place, total_of, out_refs, done)


def plane_sum(wires, place, part_ref, partner_in, out_refs):
    totals = []
    run_all(plane_sum_steps(wires, place, part_ref, partner_in, out_refs, totals.append))
    return totals[0]


def sum_scratch(piece, width):
    return [pltpu.VMEM((piece, width), jnp.bfloat16)] * 6


def sems(count):
    return [pltpu.SemaphoreType.DMA((count,)), pltpu.SemaphoreType.DMA((count,))]


def plane_peers(place):
    me, core, near, far, cross = place
    return {"seq": near}, {"seq": far}, {"tensor": 1 - core}


def norm_of(values, gain_vec):
    return values * lax.rsqrt(jnp.mean(values * values, axis=-1, keepdims=True) + epsilon) * gain_vec


def norm_back(values, gain_vec, grad):
    inverse = lax.rsqrt(jnp.mean(values * values, axis=-1, keepdims=True) + epsilon)
    unit = values * inverse
    scaled_grad = grad * gain_vec
    gain_grad = jnp.sum(grad * unit, axis=0, keepdims=True)
    return inverse * (scaled_grad - unit * jnp.mean(scaled_grad * unit, axis=-1, keepdims=True)), gain_grad


def dot(left, right):
    return jnp.dot(left, right, preferred_element_type=jnp.float32)


def dot_nt(left, right):
    return lax.dot_general(left, right, NT, preferred_element_type=jnp.float32)


def dot_tn(left, right):
    return lax.dot_general(left, right, TN, preferred_element_type=jnp.float32)


def project_steps(place, x_ref, gain_ref, w_ref, normed_ref, qkv_ref, wires):
    me, core, near, far, cross = place
    normed_ref[me] = norm_of(x_ref[...], gain_ref[...]).astype(jnp.bfloat16)
    task = gather_steps(wires, normed_ref, place, False)
    next(task)
    qkv_ref[me] = dot(normed_ref[me], w_ref[...]).astype(jnp.bfloat16)
    next(task)
    next(task)
    qkv_ref[near] = dot(normed_ref[near], w_ref[...]).astype(jnp.bfloat16)
    qkv_ref[far] = dot(normed_ref[far], w_ref[...]).astype(jnp.bfloat16)
    next(task)
    qkv_ref[cross] = dot(normed_ref[cross], w_ref[...]).astype(jnp.bfloat16)


def add_to(out_ref, base_ref):
    def done(total):
        out_ref[...] = base_ref[...] + total

    return done


def project_kernel(x_ref, gain_ref, w_ref, routes_ref, normed_ref, qkv_ref, routes_all_ref, send, recv):
    place = plane_place()
    me, core, near, far, cross = place
    wires = Wires(send, recv)
    greet({"seq": near}, {"seq": far}, {"seq": cross})
    routes_all_ref[me] = routes_ref[...]
    picks = [wires.copy(routes_ref, routes_all_ref.at[me], {"seq": spot}) for spot in (near, far, cross)]
    project_steps(place, x_ref, gain_ref, w_ref, normed_ref, qkv_ref, wires)
    for one in picks:
        one.wait_recv()
    wires.finish()


def sum_project_kernel(part_ref, base_ref, gain_ref, w_ref, x_ref, normed_ref, qkv_ref, partner_in, *rest):
    out_refs, (send, recv) = rest[:6], rest[6:]
    place = plane_place()
    wires = Wires(send, recv)
    greet(*plane_peers(place))
    x_ref[...] = base_ref[...] + plane_sum(wires, place, part_ref, partner_in, out_refs)
    project_steps(place, x_ref, gain_ref, w_ref, normed_ref, qkv_ref, wires)
    wires.finish()


def merge_kernel(fetch, mixed_ref, base_ref, w_ref, gain_ref, *refs):
    place = plane_place()
    me, core, near, far, cross = place
    if fetch:
        qkv_next, merged_ref, middle_ref, tokens_ref, qkv_all, send, recv = refs
        line_me, targets, sources = dp_peers()
    else:
        merged_ref, middle_ref, tokens_ref, send, recv = refs
        targets = []
    wires = Wires(send, recv)
    greet({"seq": near}, {"seq": far}, {"seq": cross}, {"tensor": 1 - core}, *[{"dp": spot} for spot in targets])
    if fetch:
        lines = line_start(wires, qkv_next, qkv_all, core, line_me, targets)
    copies = [wires.copy(mixed_ref.at[spot], merged_ref.at[me], {"seq": spot}) for spot in (cross, near, far)]
    merged_ref[me] = mixed_ref[me]
    total = base_ref[...] + dot(mixed_ref[me], w_ref[me])
    for spot, one in ((near, copies[1]), (far, copies[2]), (cross, copies[0])):
        one.wait_recv()
        total = total + dot(merged_ref[spot], w_ref[spot])
    middle_ref[...] = total
    tokens_ref[me, core] = norm_of(total, gain_ref[...]).astype(jnp.bfloat16)
    run_all(gather_steps(wires, tokens_ref, place, True))
    if fetch:
        for one in line_forward(wires, qkv_all, core, lines, sources):
            one.wait_recv()
    wires.finish()


def split_kernel(part_ref, middle_ref, gain_ref, grad_ref, w_ref, merged_ref, middle_grad_ref, gain_grad_ref, mixed_grad_ref,
                 weight_ref, out_grad_ref, outgoing, partner_in, *rest):
    out_refs, (send, recv) = rest[:6], rest[6:]
    place = plane_place()
    me, core, near, far, cross = place
    wires = Wires(send, recv)
    greet({"seq": near}, {"seq": far}, {"seq": cross}, {"tensor": 1 - core})
    normed_grad = plane_sum(wires, place, part_ref, partner_in, out_refs)
    part, gain_grad_ref[...] = norm_back(middle_ref[...], gain_ref[...], normed_grad)
    middle_grad = grad_ref[...] + part
    middle_grad_ref[...] = middle_grad
    out_grad_ref[...] = middle_grad.astype(jnp.bfloat16)
    copies = []
    for spot in (cross, near, far):
        outgoing[spot] = dot_nt(out_grad_ref[...], w_ref[spot]).astype(jnp.bfloat16)
        copies.append(wires.copy(outgoing.at[spot], mixed_grad_ref.at[me], {"seq": spot}))
    mixed_grad_ref[me] = dot_nt(out_grad_ref[...], w_ref[me]).astype(jnp.bfloat16)
    cores, count, parts, rows = weight_ref.shape[:4]
    block = merged_ref.shape[2]
    for at in range(merged_ref.shape[0]):
        weight_grad = dot_tn(merged_ref[at], out_grad_ref[...])
        for inner in range(block // rows):
            index = (at * block + inner * rows) // rows
            dp_at, core_at, part_at = index // (cores * parts), index // parts % cores, index % parts
            weight_ref[core_at, dp_at, part_at] = weight_grad[inner * rows : (inner + 1) * rows].astype(jnp.bfloat16)
    for one in copies:
        one.wait_recv()
    wires.finish()


def input_grad_kernel(spread, qkv_grad_ref, w_ref, x_ref, gain_ref, middle_grad_ref, *rest):
    grad_ref, gain_grad_ref = rest[:2]
    rows_ref = rest[2] if spread else None
    rest = rest[3:] if spread else rest[2:]
    out_refs, (send, recv) = rest[:6], rest[6:]
    place = plane_place()
    me, core, near, far, cross = place
    wires = Wires(send, recv)
    greet(*plane_peers(place)[: 3 if spread else 2])
    totals = []
    run_all(cross_steps(wires, place, lambda spot: dot_nt(qkv_grad_ref[spot], w_ref[...]), out_refs, totals.append))
    normed_grad = totals[0]
    part, gain_grad_ref[...] = norm_back(x_ref[...], gain_ref[...], normed_grad)
    grad = middle_grad_ref[...] + part
    grad_ref[...] = grad
    if spread:
        rows_ref[me, core] = grad.astype(jnp.bfloat16)
        run_all(gather_steps(wires, rows_ref, place, True))
    wires.finish()


def comm_call(kernel, name, number, time, outs, scratch, wire_count, *operands):
    return pl.pallas_call(
        kernel,
        out_shape=tuple(outs),
        in_specs=vmem(len(operands)),
        out_specs=tuple(vmem(len(outs))),
        scratch_shapes=scratch + sems(wire_count),
        compiler_params=pltpu.CompilerParams(collective_id=number, has_side_effects=True),
        cost_estimate=cost(time),
        name=name,
    )(*operands)


def cost(time):
    return pl.CostEstimate(flops=0, bytes_accessed=int(time * 3e6), transcendentals=0)


def low_array(*shape):
    return jax.ShapeDtypeStruct(shape, jnp.bfloat16)


def wide_array(*shape):
    return jax.ShapeDtypeStruct(shape, jnp.float32)


def gelu_parts(values):
    square = values * values
    inner = jnp.tanh(values * (0.7978845608028654 + (0.7978845608028654 * 0.044715) * square))
    lift = 0.5 + 0.5 * inner
    slope = lift + (0.5 * values) * (1.0 - inner * inner) * (0.7978845608028654 + (3.0 * 0.7978845608028654 * 0.044715) * square)
    return values * lift, slope


def slot_hot(slot_row, capacity):
    rows = lax.broadcasted_iota(jnp.int32, (capacity, slot_row.shape[1]), 0)
    return (rows == slot_row).astype(jnp.bfloat16)


def one_of(pair_ref, index):
    values = pair_ref[:, index]
    return values.reshape(values.shape[0] * values.shape[1], values.shape[2])


def experts_kernel(tokens_ref, slot_ref, chosen_ref, own_ref, router_ref, pair_ref, part_ref, slots_ref, pre_ref, shares_ref):
    capacity = slots_ref.shape[0]
    tokens = tokens_ref[...]
    logits = jnp.where(chosen_ref[...] > 0, dot_nt(tokens, router_ref[...]), negative)
    raised = jnp.exp(logits - jnp.max(logits, axis=1, keepdims=True))
    shares = raised / jnp.sum(raised, axis=1, keepdims=True)
    shares_ref[...] = shares
    own_share = jnp.sum(shares * own_ref[...], axis=1, keepdims=True)
    hot = slot_hot(slot_ref[...], capacity)
    slots = dot(hot, tokens).astype(jnp.bfloat16)
    slots_ref[...] = slots
    pre = dot(slots, one_of(pair_ref, 0))
    pre_ref[...] = pre.astype(jnp.bfloat16)
    hidden = gelu_parts(pre)[0].astype(jnp.bfloat16)
    result = dot_nt(hidden, one_of(pair_ref, 1)).astype(jnp.bfloat16)
    part_ref[...] = (own_share * dot_tn(hot, result)).astype(jnp.bfloat16)


class Replay(Wires):
    def __init__(self, send, recv, ref, place, stage):
        super().__init__(send, recv)
        self.stage, self.now = stage, 0
        task = gather_steps(self, ref, place, False)
        for self.now in range(1, stage + 1):
            next(task, None)
        if stage == 5:
            self.finish()

    def copy(self, src, dst, where):
        one = pltpu.make_async_remote_copy(
            src_ref=src, dst_ref=dst, send_sem=self.send.at[self.next], recv_sem=self.recv.at[self.next],
            device_id=where, device_id_type=MESH_ID,
        )
        self.next += 1
        if self.now == self.stage:
            one.start()
        self.started.append(one)
        return Held(one, self)


class Held:
    def __init__(self, one, owner):
        self.one, self.owner = one, owner

    def wait_recv(self):
        if self.owner.now == self.owner.stage or self.owner.stage == 5 and self.owner.now > 2:
            self.one.wait_recv()


def experts_back_kernel(rows_ref, tokens_ref, slot_ref, shares_ref, own_ref, router_ref, pair_ref, slots_ref, pre_ref,
                        *refs):
    group, last = pl.program_id(0), pl.num_programs(0) - 1
    if len(refs) > 6:
        shard_ref, part_ref, pair_grad_ref, router_grad_ref, shared_ref, up_acc, down_acc, landing, send, recv = refs

        @pl.when(group == 0)
        def _():
            place = plane_place()
            greet({"seq": place[2]}, {"seq": place[3]})
            landing[place[0]] = shard_ref[1]
            Replay(send, recv, landing, plane_place(), 1)

        @pl.when(group == 2)
        def _():
            Replay(send, recv, landing, plane_place(), 2)

    else:
        part_ref, pair_grad_ref, router_grad_ref, up_acc, down_acc = refs
        shared_ref = None

    @pl.when(group == 0)
    def _():
        up_acc[...] = jnp.zeros_like(up_acc)
        down_acc[...] = jnp.zeros_like(down_acc)
        router_grad_ref[...] = jnp.zeros_like(router_grad_ref)

    capacity = slots_ref.shape[0]
    shares = shares_ref[...]
    own = own_ref[...]
    own_share = jnp.sum(shares * own, axis=1, keepdims=True)
    hot = slot_hot(slot_ref[...], capacity)
    scaled_rows = (own_share * rows_ref[...].astype(jnp.float32)).astype(jnp.bfloat16)
    result_grad = dot(hot, scaled_rows).astype(jnp.bfloat16)
    hidden_grad = dot(result_grad, one_of(pair_ref, 1))
    hidden, slope = gelu_parts(pre_ref[...].astype(jnp.float32))
    pre_grad = (slope * hidden_grad).astype(jnp.bfloat16)
    pair_sum = jnp.sum(hidden * hidden_grad, axis=1, keepdims=True)
    down_acc[...] += dot_tn(result_grad, hidden.astype(jnp.bfloat16))
    up_acc[...] += dot_tn(slots_ref[...], pre_grad)
    slot_grad = dot_nt(pre_grad, one_of(pair_ref, 0)).astype(jnp.bfloat16)
    high = pair_sum.astype(jnp.bfloat16)
    rest = (pair_sum - high.astype(jnp.float32)).astype(jnp.bfloat16)
    token_pair = dot_tn(hot, jnp.concatenate([jnp.broadcast_to(high, (capacity, 128)), jnp.broadcast_to(rest, (capacity, 128))], axis=1))
    token_pair = token_pair[:, :1] + token_pair[:, 128:129]
    logit_grad = (token_pair * (own - shares)).astype(jnp.bfloat16)
    router_grad_ref[...] += dot_tn(logit_grad, tokens_ref[...])
    part_ref[...] = (dot_tn(hot, slot_grad) + dot(logit_grad, router_ref[...])).astype(jnp.bfloat16)

    @pl.when(group == last)
    def _():
        shape = pair_grad_ref.shape[:1] + pair_grad_ref.shape[2:]
        pair_grad_ref[:, 0] = up_acc[...].astype(jnp.bfloat16).reshape(shape)
        pair_grad_ref[:, 1] = down_acc[...].astype(jnp.bfloat16).reshape(shape)

    if shared_ref is not None:

        @pl.when(group == last)
        def _():
            Replay(send, recv, landing, plane_place(), 5)
            shared_ref[...] = landing[...]


def by_group(*shape):
    return pl.BlockSpec((None,) + shape, lambda g: (g,) + (0,) * len(shape))


def held(*shape):
    return pl.BlockSpec(shape, lambda g: (0,) * len(shape), pipeline_mode=pl.Buffered(1))


def run_experts(tokens, slot, chosen, own, router, pair, capacity):
    groups, rows, width = tokens.shape
    experts, wide_ff = router.shape[0], pair.shape[3]
    return pl.pallas_call(
        experts_kernel,
        grid=(groups,),
        out_shape=(low_array(groups, rows, width), low_array(groups, capacity, width), low_array(groups, capacity, wide_ff),
                   wide_array(groups, rows, experts)),
        in_specs=[by_group(rows, width), by_group(1, rows), by_group(rows, experts), held(1, experts), held(experts, width),
                  held(*pair.shape)],
        out_specs=(by_group(rows, width), by_group(capacity, width), by_group(capacity, wide_ff), by_group(rows, experts)),
        compiler_params=pltpu.CompilerParams(dimension_semantics=("arbitrary",)),
        cost_estimate=cost(14.0),
        name="experts",
    )(tokens, slot, chosen, own, router, pair)


def run_experts_back(rows_grad, tokens, slot, shares, own, router, pair, slots, pre, shard=None):
    groups, rows, width = tokens.shape
    experts, wide_ff = router.shape[0], pair.shape[3]
    capacity = slots.shape[1]
    outs = [low_array(groups, rows, width), low_array(*pair.shape), wide_array(experts, width)]
    out_specs = [by_group(rows, width), held(*pair.shape), held(experts, width)]
    in_specs = [by_group(rows, width), by_group(rows, width), by_group(1, rows), by_group(rows, experts), held(1, experts),
                held(experts, width), held(*pair.shape), by_group(capacity, width), by_group(capacity, wide_ff)]
    scratch = [pltpu.VMEM((width, wide_ff), jnp.float32), pltpu.VMEM((width, wide_ff), jnp.float32)]
    operands = [rows_grad, tokens, slot, shares, own, router, pair, slots, pre]
    options = {}
    if shard is not None:
        operands.append(shard)
        in_specs.append(held(*shard.shape))
        outs.append(low_array(4, *shard.shape[1:]))
        out_specs.append(held(4, *shard.shape[1:]))
        scratch += [pltpu.VMEM((4,) + shard.shape[1:], jnp.bfloat16)] + sems(6)
        options = {"collective_id": 13, "has_side_effects": True}
    return pl.pallas_call(
        experts_back_kernel,
        grid=(groups,),
        out_shape=tuple(outs),
        in_specs=in_specs,
        out_specs=tuple(out_specs),
        scratch_shapes=scratch,
        compiler_params=pltpu.CompilerParams(dimension_semantics=("arbitrary",), **options),
        cost_estimate=cost(25.0),
        name="experts_back" if shard is None else "experts_back_share",
    )(*operands)


def dp_peers():
    me, count = lax.axis_index("dp"), lax.axis_size("dp")
    return me, [lax.rem(me + step, count) for step in range(1, count)], [lax.rem(me + count - step, count) for step in range(1, count)]


def line_start(wires, own_ref, all_ref, core, me, targets):
    half = own_ref.at[core]
    copies = [wires.copy(half, all_ref.at[me, core], {"dp": spot}) for spot in targets]
    all_ref[me] = own_ref[...]
    return copies


def line_forward(wires, all_ref, core, copies, sources):
    onward = []
    for one, spot in zip(copies, sources):
        one.wait_recv()
        block = all_ref.at[spot, core]
        onward.append(wires.copy(block, block, {"tensor": 1 - core}))
    return onward


def weights_kernel(small_ref, whole_ref, outs_ref, small_all, qkv_all, qkv_next, one_piece, two_piece, own_ref, send, recv):
    core, place = lax.axis_index("tensor"), lax.axis_index("seq")
    me, targets, sources = dp_peers()
    wires = Wires(send, recv)
    greet(*[{"dp": spot} for spot in targets], {"tensor": 1 - core})
    smalls = [wires.copy(small_ref, small_all.at[me], {"dp": spot}) for spot in targets]
    small_all[me] = small_ref[...]
    layers, rows, columns = whole_ref.shape
    part, parts = columns // 3, lax.axis_size("seq")
    size = part // parts
    for spot in range(parts):

        @pl.when(place == spot)
        def _():
            for layer, target in enumerate((own_ref, qkv_next)):
                pieces = [whole_ref[layer, :, kind * part + spot * size : kind * part + (spot + 1) * size] for kind in range(3)]
                pieces = jnp.concatenate(pieces, axis=1)
                target[0] = pieces[: rows // 2]
                target[1] = pieces[rows // 2 :]

    qkvs = line_start(wires, own_ref, qkv_all, core, me, targets)
    half = one_piece.shape[-1]
    chosen = pl.ds(pl.multiple_of(core * half, half), half)
    for layer, piece in enumerate((one_piece, two_piece)):
        smalls += [wires.copy(outs_ref.at[layer, place, :, chosen], piece.at[me], {"dp": spot}) for spot in targets]
        piece[me] = outs_ref[layer, place, :, chosen]
    onward = line_forward(wires, qkv_all, core, qkvs, sources)
    for one in smalls + onward:
        one.wait_recv()
    wires.finish()


def reduce_steps(wires, place, line, plane_first, q_ref, o_ref, o_out, scratch):
    me, core, near, far, cross = place
    line_me, targets, sources = line
    q_in, q_sum, q_line, q_out, o_in, o_line, o_sum, o_seq = scratch
    others, partner = (cross, near, far), {"tensor": 1 - core}
    q_first = wires.copy(q_ref.at[1 - core], q_in, partner)
    o_first = wires.copy(o_ref.at[1 - core], o_in, partner)
    yield
    q_first.wait_recv()
    q_sum[...] = (wide(q_ref[core]) + wide(q_in[...])).astype(jnp.bfloat16)
    q_copies = [wires.copy(q_sum.at[spot], q_line.at[line_me], {"dp": spot}) for spot in targets]
    q_line[line_me] = q_sum[line_me]
    o_first.wait_recv()
    o_in[...] = (wide(o_ref[core]) + wide(o_in[...])).astype(jnp.bfloat16)
    if plane_first:
        o_copies = [wires.copy(o_in.at[:, spot], o_seq.at[me], {"seq": spot}) for spot in others]
        o_seq[me] = o_in[:, me]
    else:
        o_copies = [wires.copy(o_in.at[spot], o_line.at[line_me], {"dp": spot}) for spot in targets]
        o_line[line_me] = o_in[line_me]
    yield

    def line_total(ref, copies):
        for one in copies:
            one.wait_recv()
        total = wide(ref[0])
        for spot in range(1, len(targets) + 1):
            total = total + wide(ref[spot])
        return total.astype(jnp.bfloat16)

    def spread(out):
        mine = out.at[core, me]
        return (out, [wires.copy(mine, mine, {"seq": spot}) for spot in others], [wires.copy(mine, mine, partner)])

    def plane_total(copies):
        for one in copies:
            one.wait_recv()
        return (wide(o_seq[0]) + wide(o_seq[1]) + wide(o_seq[2]) + wide(o_seq[3])).astype(jnp.bfloat16)

    if plane_first:
        o_sum[...] = plane_total(o_copies)
        next_copies = [wires.copy(o_sum.at[spot], o_line.at[line_me], {"dp": spot}) for spot in targets]
        o_line[line_me] = o_sum[line_me]
        yield
        q_out[core, me] = line_total(q_line, q_copies)
        last = [spread(q_out)]
        yield
        o_out[core, me] = line_total(o_line, next_copies)
    else:
        q_out[core, me] = line_total(q_line, q_copies)
        last = [spread(q_out)]
        yield
        o_sum[...] = line_total(o_line, o_copies)
        next_copies = [wires.copy(o_sum.at[spot], o_seq.at[me], {"seq": spot}) for spot in others]
        o_seq[me] = o_sum[me]
        yield
        o_out[core, me] = plane_total(next_copies)
    last.append(spread(o_out))
    yield
    for out, copies, onward in last:
        for one, spot in zip(copies, others):
            one.wait_recv()
            block = out.at[core, spot]
            onward.append(wires.copy(block, block, partner))
    yield
    for out, copies, onward in last:
        for one in onward:
            one.wait_recv()


def small_steps(wires, place, line, s_ref, s_out, scratch):
    me, core, near, far, cross = place
    line_me, targets, sources = line
    s_in, s_sum, s_line, s_tot, s_seq = scratch
    partner = {"tensor": 1 - core}
    one = wires.copy(s_ref.at[1 - core], s_in, partner)
    yield
    one.wait_recv()
    s_sum[...] = s_ref[core] + s_in[...]
    copies = [wires.copy(s_sum.at[spot], s_line.at[line_me], {"dp": spot}) for spot in targets]
    s_line[line_me] = s_sum[line_me]
    yield
    for one in copies:
        one.wait_recv()
    s_tot[...] = jnp.sum(s_line[...], axis=0)
    copies = [wires.copy(s_tot, s_seq.at[me], {"seq": spot}) for spot in (cross, near, far)]
    s_seq[me] = s_tot[...]
    yield
    for one in copies:
        one.wait_recv()
    s_out[core] = jnp.sum(s_seq[...], axis=0)
    mine = s_out.at[core]
    one = wires.copy(mine, mine, partner)
    yield
    one.wait_recv()


def finish_kernel(layers, *refs):
    def take(number):
        nonlocal refs
        first, refs = refs[:number], refs[number:]
        return first

    q_refs, o_refs, s_refs, (pair_ref,) = take(layers), take(layers), take(layers), take(1)
    (total_ref,), o_outs, s_outs, share_outs = take(1), take(layers), take(layers), take(2)
    scratch = [take(8) for _ in range(layers)]
    small_scratch = [take(5) for _ in range(layers)]
    place, line = plane_place(), dp_peers()
    me, core, near, far, cross = place
    wires = Wires(*refs)
    greet({"seq": near}, {"seq": far}, {"seq": cross}, {"tensor": 1 - core}, *[{"dp": spot} for spot in line[1]])
    reduces = [reduce_steps(wires, place, line, True, *one) for one in zip(q_refs, o_refs, o_outs, scratch)]
    smalls = [small_steps(wires, place, line, *one) for one in zip(s_refs, s_outs, small_scratch)]
    for task in reduces + smalls:
        next(task)
    for task in reduces:
        next(task)
    shares = []
    for at, dst in enumerate(share_outs):
        dst[me] = pair_ref[at]
        shares.append(gather_steps(wires, dst, place, False))
        next(shares[at])
    run_all(*reduces, *smalls, *shares)
    rows = total_ref.shape[1] // 2
    for layer in range(layers):
        whole = scratch[layer][3]
        size = whole.shape[-1] // 3
        for half in range(2):
            pieces = [whole[half, spot][:, kind * size : (kind + 1) * size] for kind in range(3) for spot in range(4)]
            total_ref[layer, half * rows : (half + 1) * rows, :] = wide(jnp.concatenate(pieces, axis=1))
    wires.finish()

def body(
    block_input,
    segments,
    routes,
    distance_bucket,
    first_gain,
    query_key_value,
    attention_out,
    bias_table,
    second_gain,
    router_weights,
    expert_up,
    expert_down,
    cotangent,
):
    low = jnp.bfloat16
    seq_count, piece, width = block_input.shape
    n_dp, n_seq, n_tensor = (lax.axis_size(name) for name in ("dp", "seq", "tensor"))
    n_plane = n_seq * n_tensor
    length = piece * n_seq
    local_heads = HEADS // n_seq
    head_width = local_heads * HD
    experts = expert_up.shape[1]
    assert seq_count == 1 and experts == n_seq
    shard = width // n_dp
    bucket_count = bias_table.shape[1] * n_dp
    bucket_shard = bias_table.shape[1]
    group_rows = n_tensor * piece
    capacity = group_rows * routes.shape[-1] // experts
    seq_index = lax.axis_index("seq")
    span = ROWS + length // 2


    assert n_seq == 4 and n_tensor == 2
    half = shard // n_tensor

    def padded(values):
        return jnp.pad(values, ((0, 0), (0, shard - values.shape[1])))

    small = jnp.concatenate(
        [
            first_gain,
            second_gain,
            router_weights.swapaxes(1, 2).reshape(-1, shard),
            padded(bias_table.reshape(LAYERS, -1)),
        ]
    )
    small_rows = small.shape[0]
    small = jnp.pad(small, ((0, -small_rows % 16), (0, 0)))
    own_out = attention_out.reshape(LAYERS, n_seq, shard // n_seq, width)
    own_up = lax.dynamic_index_in_dim(expert_up, seq_index, 1, keepdims=False)
    own_down = lax.dynamic_index_in_dim(expert_down, seq_index, 1, keepdims=False).swapaxes(1, 2)

    own_shape = (n_tensor, half, 3 * head_width)
    small_all, qkv_all, qkv_next, *out_pieces = comm_call(
        weights_kernel, "weights", 10, 22.0,
        [low_array(n_dp, *small.shape), low_array(n_dp, *own_shape), low_array(*own_shape)]
        + [low_array(n_dp, shard // n_seq, width // n_tensor)] * LAYERS,
        [pltpu.VMEM(own_shape, low)], 5 * (n_dp - 1), small, query_key_value, own_out
    )
    qkv_weights = [qkv_all]
    own_pair, small_all = lax.optimization_barrier((jnp.stack([own_up, own_down], axis=1), small_all))
    whole_rows = small_all.swapaxes(0, 1).reshape(-1, width)
    gains = whole_rows[: 2 * LAYERS].astype(jnp.float32).reshape(2, LAYERS, 1, width)
    routers = whole_rows[2 * LAYERS : 2 * LAYERS + LAYERS * experts].reshape(LAYERS, experts, width)
    tables = whole_rows[2 * LAYERS + LAYERS * experts : small_rows].reshape(LAYERS, n_dp, shard)[:, :, : bucket_shard * HEADS]
    tables = tables.reshape(LAYERS, bucket_count, HEADS).astype(jnp.float32)
    own_tables = lax.dynamic_slice_in_dim(tables, seq_index * local_heads, local_heads, 2)
    routes_own = routes.reshape(-1, 128)
    seg_row = segments
    seg_col = segments.reshape(length, 1)
    bucket_line = distance_bucket[length // 2 - 1 :: -1][: length // 2]
    bucket_line = jnp.concatenate(
        [jnp.full((1,), -1, jnp.int32), bucket_line, jnp.full((span - 1 - length // 2,), -1, jnp.int32)]
    )
    line_hot = (bucket_line[None, :] == lax.iota(jnp.int32, bucket_count)[:, None]).astype(jnp.float32)
    lines = jnp.einsum("lbh,bs->lhs", own_tables, line_hot, precision=highest_precision)
    strict_upper = (
        lax.iota(jnp.int32, group_rows)[:, None] < lax.iota(jnp.int32, group_rows)[None, :]
    ).astype(low)

    own_hot = (lax.iota(jnp.int32, experts) == seq_index).astype(jnp.float32)[None]

    current = block_input[0]
    grad = cotangent[0]
    saved = []
    for layer in range(LAYERS):
        pair = lax.all_gather(own_pair[layer], "dp", axis=0)
        gain_one, gain_two = gains[0, layer], gains[1, layer]
        qkv_weight = qkv_weights[layer].reshape(width, 3 * head_width)
        outs = [low_array(n_seq, piece, width), low_array(n_seq, piece, 3 * head_width)]
        if layer == 0:
            outs.append(jax.ShapeDtypeStruct((n_seq,) + routes_own.shape, jnp.int32))
            normed_all, qkv, routes_all = comm_call(
                project_kernel, "project", 1, 16.0, outs, [], 9, current, gain_one, qkv_weight, routes_own
            )
        else:
            current, normed_all, qkv = comm_call(
                sum_project_kernel, "sum_project", 2, 32.0, [wide_array(piece, width)] + outs,
                [pltpu.VMEM((n_seq, piece, width), low)] + sum_scratch(piece, width), 16, part, middle, gain_one, qkv_weight
            )
        qkv = qkv.reshape(length, 3 * head_width)
        if layer == 0:
            outs = [low_array(n_dp, *own_out.shape[1:])] * LAYERS
            mixed, log_total, *out_weights = attend(qkv, seg_row, seg_col, lines[layer], out_pieces, outs, "fetch", 6, 8)
        else:
            outs = [low_array(n_seq, n_tensor, piece, width)]
            mixed, log_total, grad_rows = attend(qkv, seg_row, seg_col, lines[layer], (grad,), outs, "gather", 14, 11)
        out_weight = out_weights[layer].reshape(n_seq, head_width, width)
        fetch = layer == 0
        outs = [low_array(n_seq, piece, head_width), wide_array(piece, width), low_array(n_seq, n_tensor, piece, width)]
        outs += [low_array(n_dp, *own_shape)] if fetch else []
        operands = (mixed.reshape(n_seq, piece, head_width), current, out_weight, gain_two) + ((qkv_next,) if fetch else ())
        merged, middle, tokens, *more = comm_call(
            functools.partial(merge_kernel, fetch), "merge_fetch" if fetch else "merge", 15 if fetch else 3, 25.0, outs, [],
            14 + (2 * (n_dp - 1) if fetch else 0), *operands
        )
        qkv_weights += more
        if layer == 0:
            routes_all, tokens = lax.optimization_barrier((routes_all, tokens))
            routes_all = jnp.moveaxis(routes_all.reshape((n_seq,) + routes.shape), 0, 1).reshape(LAYERS, n_seq, group_rows, -1)
            mine = jnp.any(routes_all == seq_index, axis=-1)
            slot = dot(mine.reshape(-1, group_rows).astype(low), strict_upper).astype(jnp.int32).reshape(mine.shape)
            slot = jnp.where(mine & (slot < capacity), slot, -1)[:, :, None]
            chosen = jnp.any(routes_all[..., None] == lax.iota(jnp.int32, experts), axis=3).astype(jnp.float32)
        tokens = tokens.reshape(n_seq, group_rows, width)
        part, slots, pre, shares = run_experts(tokens, slot[layer], chosen[layer], own_hot, routers[layer], pair, capacity)
        part = part.reshape(n_seq, n_tensor, piece, width)
        saved.append((current, normed_all, qkv, log_total, merged, middle, tokens, shares, slots, pre, qkv_weight, out_weight, pair))

    last_part, last_middle = part, middle

    pair_shards, qkv_grads, out_grads, smalls = ([None] * LAYERS for _ in range(4))
    out_rows = half // n_seq
    for layer in range(LAYERS - 1, -1, -1):
        (layer_in, normed_all, qkv, log_total, merged, middle, tokens, shares, slots, pre, qkv_weight, out_weight, pair) = saved[layer]
        gain_one, gain_two = gains[0, layer], gains[1, layer]
        part, pair_grad, router_grad, *shared = run_experts_back(
            grad_rows.reshape(n_seq, group_rows, width), tokens, slot[layer], shares, own_hot, routers[layer], pair, slots, pre,
            pair_shards[1] if layer == 0 else None
        )
        pair_shards[layer] = lax.psum_scatter(pair_grad, "dp", scatter_dimension=0, tiled=True)[0]
        middle_grad, gain_two_grad, mixed_grad, out_grads[layer] = comm_call(
            split_kernel, "split", 5, 25.0,
            [wide_array(piece, width), wide_array(1, width), low_array(n_seq, piece, head_width),
             low_array(n_tensor, n_dp, n_seq, out_rows, width)],
            [pltpu.VMEM((piece, width), low), pltpu.VMEM((n_seq, piece, head_width), low), pltpu.VMEM((n_seq, piece, width), low)]
            + sum_scratch(piece, width), 13,
            part.reshape(n_seq, n_tensor, piece, width), middle, gain_two, grad, out_weight, merged
        )
        operands = (qkv, seg_row, seg_col, lines[layer], log_total, mixed_grad.reshape(length, head_width))
        operands += (normed_all.reshape(length, width), (n_tensor, n_dp, half, 3 * head_width))
        if layer == 0:
            (down_last,) = shared
            outs = [low_array(n_seq, *pair_shards[1].shape[1:])]
            qkv_grad, band, qkv_grads[layer], up_last = attend_back(*operands, (pair_shards[1],), outs, [], "share", 9, 6)
            input_grad, gain_one_grad = comm_call(
                functools.partial(input_grad_kernel, False), "input_grad_last", 12, 16.0, [wide_array(piece, width), wide_array(1, width)],
                sum_scratch(piece, width), 6, qkv_grad.reshape(n_seq, piece, -1), qkv_weight, layer_in, gain_one, middle_grad
            )
        else:
            outs = [wide_array(piece, width)]
            extra_scratch = [pltpu.VMEM((n_seq, piece, width), low)] + sum_scratch(piece, width)
            qkv_grad, band, qkv_grads[layer], block_output = attend_back(
                *operands, (last_part, last_middle), outs, extra_scratch, "sum", 4, 10
            )
            outs = [wide_array(piece, width), wide_array(1, width), low_array(n_seq, n_tensor, piece, width)]
            grad, gain_one_grad, grad_rows = comm_call(
                functools.partial(input_grad_kernel, True), "input_grad", 7, 32.0, outs, sum_scratch(piece, width), 17,
                qkv_grad.reshape(n_seq, piece, -1), qkv_weight, layer_in, gain_one, middle_grad
            )
        table_grad = jnp.dot(line_hot, band.T, precision=highest_precision)
        table_grad = lax.dynamic_update_slice_in_dim(
            jnp.zeros((bucket_count, HEADS), jnp.float32), table_grad, seq_index * local_heads, 1
        )
        table_grad = padded(table_grad.reshape(n_dp, -1)).reshape(1, width)
        packed = jnp.concatenate([gain_one_grad, gain_two_grad, router_grad, table_grad, jnp.zeros((1, width), jnp.float32)])
        smalls[layer] = packed.reshape(n_tensor, n_seq, n_dp, shard).swapaxes(1, 2)

    def reduce_scratch(plane_first):
        line = pltpu.VMEM((n_dp, half, 3 * head_width), low)
        blocks = pltpu.VMEM((n_dp, n_seq, out_rows, width), low)
        over_dp, over_seq = (pltpu.VMEM((count, out_rows, width), low) for count in (n_dp, n_seq))
        found = [line] * 3 + [pltpu.VMEM((n_tensor, n_seq, half, 3 * head_width), low), blocks]
        if plane_first:
            return found + [over_dp, over_dp, pltpu.VMEM((n_seq, n_dp, out_rows, width), low)]
        return found + [blocks, over_seq, over_seq]

    small_scratch = [pltpu.VMEM((n_dp, n_seq, shard), jnp.float32)] * 3 + [pltpu.VMEM((n_seq, shard), jnp.float32)]
    small_scratch += [pltpu.VMEM((n_seq, n_seq, shard), jnp.float32)]
    qkv_total, *totals = comm_call(
        functools.partial(finish_kernel, LAYERS), "finish", 11, 70.0,
        [wide_array(LAYERS, shard, 3 * width)]
        + [low_array(n_tensor, n_seq, out_rows, width)] * LAYERS + [wide_array(n_tensor, n_seq, shard)] * LAYERS
        + [low_array(n_seq, *pair_shards[0].shape[1:])] * 2,
        reduce_scratch(True) + reduce_scratch(True) + small_scratch * LAYERS,
        LAYERS * (2 * (n_dp - 1) + 19 + n_dp + 4) + 12, *qkv_grads, *out_grads, *smalls, pair_shards[0]
    )
    out_total = jnp.stack(totals[:LAYERS]).astype(jnp.float32).reshape(LAYERS, shard, width)
    small = jnp.stack(totals[LAYERS : 2 * LAYERS]).reshape(LAYERS, n_plane, shard)
    up_first, down_first = totals[2 * LAYERS :]
    router_total = small[:, 2 : 2 + experts].swapaxes(1, 2)
    table_total = small[:, 2 + experts, : bucket_shard * HEADS].reshape(LAYERS, bucket_shard, HEADS)
    up_total = jnp.stack([up_first, up_last]).astype(jnp.float32)
    down_total = jnp.stack([down_first, down_last]).astype(jnp.float32).swapaxes(2, 3)
    return (block_output[None], input_grad[None], small[:, 0], qkv_total, out_total, table_total, small[:, 1], router_total, up_total, down_total)


def solution(mesh):
    in_specs = (
        P(("dp", "tensor"), "seq", None),
        P(("dp", "tensor"), None),
        P(None, "dp", "seq", None),
        P(),
        P(None, "dp"),
        P(None, "dp", None),
        P(None, "dp", None),
        P(None, "dp", None),
        P(None, "dp"),
        P(None, "dp", None),
        P(None, None, "dp", "tensor"),
        P(None, None, "tensor", "dp"),
        P(("dp", "tensor"), "seq", None),
    )
    out_specs = (
        P(("dp", "tensor"), "seq", None),
        P(("dp", "tensor"), "seq", None),
        P(None, "dp"),
        P(None, "dp", None),
        P(None, "dp", None),
        P(None, "dp", None),
        P(None, "dp"),
        P(None, "dp", None),
        P(None, None, "dp", "tensor"),
        P(None, None, "tensor", "dp"),
    )
    return jax.shard_map(body, mesh=mesh, in_specs=in_specs, out_specs=out_specs, check_vma=False)
```

```python
import functools

import jax
import jax.numpy as jnp
from jax import lax
from jax.experimental import pallas as pl
from jax.experimental.pallas import tpu as pltpu
from jax.sharding import PartitionSpec as P

HEADS = 12
LAYERS = 2
epsilon = 1e-06
negative = -1e30
highest_precision = lax.Precision.HIGHEST


def scaled(values, gain_vec):
    return values * lax.rsqrt(jnp.mean(values * values, axis=-1, keepdims=True) + epsilon) * gain_vec


HD = 64
ROWS = 128
NT = (((1,), (1,)), ((), ()))
TN = (((0,), (0,)), ((), ()))


def visit_blocks(length, span, one_block, hook, hooks_at):
    full, count = span // ROWS, length // ROWS

    def step(i, carry):
        start = pl.multiple_of(i * ROWS, ROWS)
        one_block(start, pl.multiple_of(start + ROWS - span, ROWS), span)
        return carry

    for i in range(full - 1):
        if i in hooks_at:
            hook()
        one_block(i * ROWS, 0, (i + 1) * ROWS)
    stops = [full - 1] + [i for i in range(full - 1, count) if i in hooks_at] + [count]
    for low, high in zip(stops, stops[1:]):
        if low in hooks_at:
            hook()
        lax.fori_loop(low, high, step, 0)


def background(tasks):
    tasks = list(tasks)

    def hook():
        tasks[:] = [task for task in tasks if next(task, wires_done) is not wires_done]

    return hook, lambda: run_all(*tasks)


def fill_mask(mask_ref, segr_ref, segc_ref, start, low, width):
    same = segc_ref[pl.ds(start, ROWS), :] == segr_ref[:, pl.ds(low, width)]
    back = lax.broadcasted_iota(jnp.int32, (ROWS, width), 0) + (width - ROWS)
    allowed = same & (back >= lax.broadcasted_iota(jnp.int32, (ROWS, width), 1))
    mask_ref[:, :width] = jnp.where(allowed, 0.0, -1e30)


def fill_slab(slab_ref, line_ref, heads, span):
    for h in range(heads):
        spread = jnp.broadcast_to(line_ref[h : h + 1, :], (ROWS, span))
        slab_ref[h] = pltpu.roll(spread, 0, 1, stride=1, stride_axis=0)


def split_heads(qkv_ref, parts_ref, heads):
    for h in range(3 * heads):
        part = qkv_ref[:, h * HD : (h + 1) * HD]
        parts_ref[h] = part * jnp.bfloat16(0.125) if h < heads else part


def fetch_steps(wires, place, own, whole):
    me, core, near, far, cross = place
    width = whole.shape[-1]
    columns = pl.ds(pl.multiple_of(core * (width // 2), width // 2), width // 2)
    around = [wires.copy(own, whole.at[:, me, :, columns], {"seq": spot}) for spot in (cross, near, far)]
    whole[:, me, :, columns] = own[...]
    yield
    for one in around:
        one.wait_recv()
    block = whole.at[:, :, :, columns]
    onward = wires.copy(block, block, {"tensor": 1 - core})
    yield
    onward.wait_recv()


def attn_fwd_kernel(heads, span, mode, *refs):
    qkv_ref, segr_ref, segc_ref, line_ref = refs[:4]
    place = plane_place()
    me, core, near, far, cross = place
    wires = Wires(*refs[-2:])
    if mode == "fetch":
        own_refs, (out_ref, lse_ref), whole_refs, scratch = refs[4:6], refs[6:8], refs[8:10], refs[10:14]
        greet({"seq": near}, {"seq": far}, {"seq": cross}, {"tensor": 1 - core})
        tasks = [fetch_steps(wires, place, *pair) for pair in zip(own_refs, whole_refs)]
        hooks_at = (6,)
    else:
        rows_ref, out_ref, lse_ref, gathered_ref = refs[4:8]
        scratch = refs[8:12]
        greet(*plane_peers(place))
        gathered_ref[me, core] = rows_ref[...].astype(jnp.bfloat16)
        tasks = [gather_steps(wires, gathered_ref, place, True)]
        hooks_at = (4, 6)
    hook, finish = background(tasks)
    hook()
    parts_ref, mixed_ref, slab_ref, mask_ref = scratch
    length = qkv_ref.shape[0]
    fill_slab(slab_ref, line_ref, heads, span)
    split_heads(qkv_ref, parts_ref, heads)

    def one_block(start, low, width):
        fill_mask(mask_ref, segr_ref, segc_ref, start, low, width)

        def one_head(h, carry):
            q = parts_ref[h, pl.ds(start, ROWS), :]
            k = parts_ref[heads + h, pl.ds(low, width), :]
            v = parts_ref[2 * heads + h, pl.ds(low, width), :]
            s = lax.dot_general(q, k, NT, preferred_element_type=jnp.float32)
            s = s + slab_ref[h, :, span - width :] + mask_ref[:, :width]
            top = jnp.max(s, axis=1, keepdims=True)
            e = jnp.exp(s - top)
            total = jnp.sum(e, axis=1, keepdims=True)
            mixed = jnp.dot(e.astype(jnp.bfloat16), v, preferred_element_type=jnp.float32)
            mixed_ref[h, pl.ds(start, ROWS), :] = (mixed / total).astype(jnp.bfloat16)
            lse_ref[h, pl.ds(start, ROWS), :] = top + jnp.log(total)
            return carry

        lax.fori_loop(0, heads, one_head, 0, unroll=True)

    visit_blocks(length, span, one_block, hook, hooks_at)
    out_ref[...] = jnp.concatenate([mixed_ref[h] for h in range(heads)], axis=1)
    finish()
    wires.finish()


def attn_bwd_kernel(heads, span, mode, *refs):
    qkv_ref, segr_ref, segc_ref, line_ref, lse_ref, grad_ref, normed_ref = refs[:7]
    place = plane_place()
    me, core, near, far, cross = place
    wires = Wires(*refs[-2:])
    if mode == "share":
        shard_ref, out_ref, band_ref, weight_ref, shared_ref = refs[7:12]
        greet({"seq": near}, {"seq": far})
        shared_ref[me] = shard_ref[0]
        tasks = [gather_steps(wires, shared_ref, place, False)]
        refs = refs[12:20]
    else:
        part_ref, base_ref, out_ref, band_ref, weight_ref, total_ref = refs[7:13]
        greet(*plane_peers(place))
        tasks = [plane_sum_steps(wires, place, part_ref, refs[21], refs[22:28], add_to(total_ref, base_ref))]
        refs = refs[13:21]
    hook, finish = background(tasks)
    hook()
    parts_ref, gparts_ref, qgrad_ref, kgrad_ref, vgrad_ref, slab_ref, mask_ref, band_acc = refs
    length = qkv_ref.shape[0]
    fill_slab(slab_ref, line_ref, heads, span)
    split_heads(qkv_ref, parts_ref, heads)
    for h in range(heads):
        gparts_ref[h] = grad_ref[:, h * HD : (h + 1) * HD]
    kgrad_ref[...] = jnp.zeros_like(kgrad_ref)
    vgrad_ref[...] = jnp.zeros_like(vgrad_ref)
    band_acc[...] = jnp.zeros_like(band_acc)

    def one_block(start, low, width):
        fill_mask(mask_ref, segr_ref, segc_ref, start, low, width)

        def one_head(h, carry):
            rows = pl.ds(start, ROWS)
            window = pl.ds(low, width)
            q = parts_ref[h, rows, :]
            k = parts_ref[heads + h, window, :]
            v = parts_ref[2 * heads + h, window, :]
            grad = gparts_ref[h, rows, :]
            s = lax.dot_general(q, k, NT, preferred_element_type=jnp.float32)
            s = s + slab_ref[h, :, span - width :] + mask_ref[:, :width]
            p = jnp.exp(s - lse_ref[h, rows, :])
            dp = lax.dot_general(grad, v, NT, preferred_element_type=jnp.float32)
            inner = jnp.sum(p * dp, axis=1, keepdims=True)
            ds = p * (dp - inner)
            band_acc[h, :, span - width :] += ds
            ds = ds.astype(jnp.bfloat16)
            qgrad = jnp.dot(ds, k, preferred_element_type=jnp.float32)
            qgrad_ref[h, rows, :] = (qgrad * 0.125).astype(jnp.bfloat16)
            kgrad_ref[h, window, :] += lax.dot_general(ds, q, TN, preferred_element_type=jnp.float32)
            vgrad_ref[h, window, :] += lax.dot_general(p.astype(jnp.bfloat16), grad, TN, preferred_element_type=jnp.float32)
            return carry

        lax.fori_loop(0, heads, one_head, 0, unroll=True)

    visit_blocks(length, span, one_block, hook, (5, 7) if mode == "share" else (3, 6))
    parts = [qgrad_ref[h] for h in range(heads)]
    parts += [kgrad_ref[h].astype(jnp.bfloat16) for h in range(heads)]
    parts += [vgrad_ref[h].astype(jnp.bfloat16) for h in range(heads)]
    out_ref[...] = jnp.concatenate(parts, axis=1)
    weight_grad = dot_tn(normed_ref[...], out_ref[...])
    rows = weight_ref.shape[2]
    for at in range(weight_ref.shape[1]):
        for core_at in range(weight_ref.shape[0]):
            first = (at * weight_ref.shape[0] + core_at) * rows
            weight_ref[core_at, at] = weight_grad[first : first + rows].astype(jnp.bfloat16)
    row = lax.broadcasted_iota(jnp.int32, (ROWS, span), 0)
    for h in range(heads):
        acc = band_acc[h]
        bit = 1
        while bit < ROWS:
            acc = jnp.where((row & bit) != 0, pltpu.roll(acc, span - bit, 1), acc)
            bit *= 2
        band_ref[h : h + 1, :] = jnp.sum(acc, axis=0, keepdims=True)
    finish()
    wires.finish()


def vmem(count):
    return [pl.BlockSpec(memory_space=pltpu.VMEM)] * count


def attend_scratch(heads, length, span):
    return [
        pltpu.VMEM((3 * heads, length, HD), jnp.bfloat16),
        pltpu.VMEM((heads, length, HD), jnp.bfloat16),
        pltpu.VMEM((heads, ROWS, span), jnp.float32),
        pltpu.VMEM((ROWS, span), jnp.float32),
    ]


def attend(qkv, seg_row, seg_col, line, extra, extra_outs, mode, number, wire_count):
    length, width = qkv.shape
    heads, span = line.shape
    outs = [low_array(length, heads * HD), wide_array(heads, length, 1)] + extra_outs
    return comm_call(functools.partial(attn_fwd_kernel, heads, span, mode), "attend_" + mode, number, 18.0, outs,
                     attend_scratch(heads, length, span), wire_count, qkv, seg_row, seg_col, line, *extra)


def attend_back(qkv, seg_row, seg_col, line, lse, grad, normed, weight_shape, extra, extra_outs, extra_scratch, mode, number, wire_count):
    length, width = qkv.shape
    heads, span = line.shape
    outs = [low_array(length, width), wide_array(heads, span), low_array(*weight_shape)] + extra_outs
    scratch = [
        pltpu.VMEM((3 * heads, length, HD), jnp.bfloat16),
        pltpu.VMEM((heads, length, HD), jnp.bfloat16),
        pltpu.VMEM((heads, length, HD), jnp.bfloat16),
        pltpu.VMEM((heads, length, HD), jnp.float32),
        pltpu.VMEM((heads, length, HD), jnp.float32),
        pltpu.VMEM((heads, ROWS, span), jnp.float32),
        pltpu.VMEM((ROWS, span), jnp.float32),
        pltpu.VMEM((heads, ROWS, span), jnp.float32),
    ]
    return comm_call(functools.partial(attn_bwd_kernel, heads, span, mode), "attend_back_" + mode, number, 23.0, outs,
                     scratch + extra_scratch, wire_count, qkv, seg_row, seg_col, line, lse, grad, normed, *extra)


MESH_ID = pl.DeviceIdType.MESH


class Wires:
    def __init__(self, send, recv):
        self.send, self.recv, self.next, self.started = send, recv, 0, []

    def copy(self, src, dst, where):
        one = pltpu.make_async_remote_copy(
            src_ref=src, dst_ref=dst, send_sem=self.send.at[self.next], recv_sem=self.recv.at[self.next],
            device_id=where, device_id_type=MESH_ID,
        )
        self.next += 1
        one.start()
        self.started.append(one)
        return one

    def finish(self):
        for one in self.started:
            one.wait_send()


def plane_place():
    me = lax.axis_index("seq")
    core = lax.axis_index("tensor")
    near, far = me + 1 - 2 * lax.rem(me, 2), lax.rem(me + 2, 4)
    cross = lax.rem(near + 2, 4)
    return me, core, near, far, cross


def greet(*places):
    barrier = pltpu.get_barrier_semaphore()
    for where in places:
        pl.semaphore_signal(barrier, inc=1, device_id=where, device_id_type=MESH_ID)
    pl.semaphore_wait(barrier, len(places))


def gather_steps(wires, ref, place, paired):
    me, core, near, far, cross = place
    half = ref.shape[-2] // 2
    to_near, to_far, partner = {"seq": near}, {"seq": far}, {"tensor": 1 - core}

    def part(spot, start, size):
        return ref.at[spot, core, pl.ds(start, size)] if paired else ref.at[spot, pl.ds(start, size)]

    def send(spot, start, size, where):
        block = part(spot, start, size)
        return wires.copy(block, block, where)

    near_top = send(me, 0, half, to_near)
    far_low = send(me, half, half, to_far)
    near_low = send(me, half, half, to_near)
    far_top = send(me, 0, half, to_far)
    inside = [send(me, 0, 2 * half, partner)] if paired else []
    yield
    near_top.wait_recv()
    cross_top = send(near, 0, half, to_far)
    far_low.wait_recv()
    cross_low = send(far, half, half, to_near)
    yield
    near_low.wait_recv()
    inside += [send(near, 0, 2 * half, partner)] if paired else []
    far_top.wait_recv()
    inside += [send(far, 0, 2 * half, partner)] if paired else []
    yield
    cross_top.wait_recv()
    inside += [send(cross, 0, half, partner)] if paired else []
    cross_low.wait_recv()
    inside += [send(cross, half, half, partner)] if paired else []
    yield
    for one in inside:
        one.wait_recv()


def run_all(*tasks):
    tasks = list(tasks)
    while tasks:
        tasks = [task for task in tasks if next(task, wires_done) is not wires_done]


wires_done = object()


def wide(values):
    return values.astype(jnp.float32)


def cross_steps(wires, place, total_of, out_refs, done):
    me, core, near, far, cross = place
    cross_ref, near_ref, far_ref, cross_in, near_in, far_in = out_refs
    half = near_ref.shape[0] // 2
    top, bottom = pl.ds(0, half), pl.ds(half, half)
    cross_ref[...] = total_of(cross).astype(cross_ref.dtype)
    to_near = wires.copy(cross_ref.at[top], cross_in.at[top], {"seq": near})
    to_far = wires.copy(cross_ref.at[bottom], cross_in.at[bottom], {"seq": far})
    near_ref[...] = total_of(near).astype(near_ref.dtype)
    near_one = wires.copy(near_ref.at[top], near_in.at[top], {"seq": near})
    far_ref[...] = total_of(far).astype(far_ref.dtype)
    far_one = wires.copy(far_ref.at[bottom], far_in.at[bottom], {"seq": far})
    yield
    to_near.wait_recv()
    far_ref[top, :] = (wide(far_ref[top, :]) + wide(cross_in[top, :])).astype(far_ref.dtype)
    far_two = wires.copy(far_ref.at[top], far_in.at[top], {"seq": far})
    to_far.wait_recv()
    near_ref[bottom, :] = (wide(near_ref[bottom, :]) + wide(cross_in[bottom, :])).astype(near_ref.dtype)
    near_two = wires.copy(near_ref.at[bottom], near_in.at[bottom], {"seq": near})
    own = total_of(me)
    yield
    for one in (near_one, far_one, far_two, near_two):
        one.wait_recv()
    done(own + wide(near_in[...]) + wide(far_in[...]))


def plane_sum_steps(wires, place, part_ref, partner_in, out_refs, done):
    me, core, near, far, cross = place
    arrivals = {}
    for name, spot in (("cross", cross), ("near", near), ("far", far), ("me", me)):
        arrivals[name] = wires.copy(part_ref.at[spot, 1 - core], partner_in.at[spot], {"tensor": 1 - core})
    order = iter(("cross", "near", "far", "me"))

    def total_of(spot):
        arrivals[next(order)].wait_recv()
        return wide(part_ref[spot, core]) + wide(partner_in[spot])

    yield
    yield from cross_steps(wires, place, total_of, out_refs, done)


def plane_sum(wires, place, part_ref, partner_in, out_refs):
    totals = []
    run_all(plane_sum_steps(wires, place, part_ref, partner_in, out_refs, totals.append))
    return totals[0]


def sum_scratch(piece, width):
    return [pltpu.VMEM((piece, width), jnp.bfloat16)] * 6


def sems(count):
    return [pltpu.SemaphoreType.DMA((count,)), pltpu.SemaphoreType.DMA((count,))]


def plane_peers(place):
    me, core, near, far, cross = place
    return {"seq": near}, {"seq": far}, {"tensor": 1 - core}


def norm_of(values, gain_vec):
    return values * lax.rsqrt(jnp.mean(values * values, axis=-1, keepdims=True) + epsilon) * gain_vec


def norm_back(values, gain_vec, grad):
    inverse = lax.rsqrt(jnp.mean(values * values, axis=-1, keepdims=True) + epsilon)
    unit = values * inverse
    scaled_grad = grad * gain_vec
    gain_grad = jnp.sum(grad * unit, axis=0, keepdims=True)
    return inverse * (scaled_grad - unit * jnp.mean(scaled_grad * unit, axis=-1, keepdims=True)), gain_grad


def dot(left, right):
    return jnp.dot(left, right, preferred_element_type=jnp.float32)


def dot_nt(left, right):
    return lax.dot_general(left, right, NT, preferred_element_type=jnp.float32)


def dot_tn(left, right):
    return lax.dot_general(left, right, TN, preferred_element_type=jnp.float32)


def project_steps(place, x_ref, gain_ref, w_ref, normed_ref, qkv_ref, wires):
    me, core, near, far, cross = place
    normed_ref[me] = norm_of(x_ref[...], gain_ref[...]).astype(jnp.bfloat16)
    task = gather_steps(wires, normed_ref, place, False)
    next(task)
    qkv_ref[me] = dot(normed_ref[me], w_ref[...]).astype(jnp.bfloat16)
    next(task)
    next(task)
    qkv_ref[near] = dot(normed_ref[near], w_ref[...]).astype(jnp.bfloat16)
    qkv_ref[far] = dot(normed_ref[far], w_ref[...]).astype(jnp.bfloat16)
    next(task)
    qkv_ref[cross] = dot(normed_ref[cross], w_ref[...]).astype(jnp.bfloat16)


def add_to(out_ref, base_ref):
    def done(total):
        out_ref[...] = base_ref[...] + total

    return done


def project_kernel(x_ref, gain_ref, w_ref, routes_ref, normed_ref, qkv_ref, routes_all_ref, send, recv):
    place = plane_place()
    me, core, near, far, cross = place
    wires = Wires(send, recv)
    greet({"seq": near}, {"seq": far}, {"seq": cross})
    routes_all_ref[me] = routes_ref[...]
    picks = [wires.copy(routes_ref, routes_all_ref.at[me], {"seq": spot}) for spot in (near, far, cross)]
    project_steps(place, x_ref, gain_ref, w_ref, normed_ref, qkv_ref, wires)
    for one in picks:
        one.wait_recv()
    wires.finish()


def sum_project_kernel(part_ref, base_ref, gain_ref, w_ref, x_ref, normed_ref, qkv_ref, partner_in, *rest):
    out_refs, (send, recv) = rest[:6], rest[6:]
    place = plane_place()
    wires = Wires(send, recv)
    greet(*plane_peers(place))
    x_ref[...] = base_ref[...] + plane_sum(wires, place, part_ref, partner_in, out_refs)
    project_steps(place, x_ref, gain_ref, w_ref, normed_ref, qkv_ref, wires)
    wires.finish()


def merge_kernel(fetch, mixed_ref, base_ref, w_ref, gain_ref, *refs):
    place = plane_place()
    me, core, near, far, cross = place
    if fetch:
        qkv_next, merged_ref, middle_ref, tokens_ref, qkv_all, send, recv = refs
        line_me, targets, sources = dp_peers()
    else:
        merged_ref, middle_ref, tokens_ref, send, recv = refs
        targets = []
    wires = Wires(send, recv)
    greet({"seq": near}, {"seq": far}, {"seq": cross}, {"tensor": 1 - core}, *[{"dp": spot} for spot in targets])
    if fetch:
        lines = line_start(wires, qkv_next, qkv_all, core, line_me, targets)
    copies = [wires.copy(mixed_ref.at[spot], merged_ref.at[me], {"seq": spot}) for spot in (cross, near, far)]
    merged_ref[me] = mixed_ref[me]
    total = base_ref[...] + dot(mixed_ref[me], w_ref[me])
    for spot, one in ((near, copies[1]), (far, copies[2]), (cross, copies[0])):
        one.wait_recv()
        total = total + dot(merged_ref[spot], w_ref[spot])
    middle_ref[...] = total
    tokens_ref[me, core] = norm_of(total, gain_ref[...]).astype(jnp.bfloat16)
    run_all(gather_steps(wires, tokens_ref, place, True))
    if fetch:
        for one in line_forward(wires, qkv_all, core, lines, sources):
            one.wait_recv()
    wires.finish()


def split_kernel(part_ref, middle_ref, gain_ref, grad_ref, w_ref, merged_ref, middle_grad_ref, gain_grad_ref, mixed_grad_ref,
                 weight_ref, out_grad_ref, outgoing, partner_in, *rest):
    out_refs, (send, recv) = rest[:6], rest[6:]
    place = plane_place()
    me, core, near, far, cross = place
    wires = Wires(send, recv)
    greet({"seq": near}, {"seq": far}, {"seq": cross}, {"tensor": 1 - core})
    normed_grad = plane_sum(wires, place, part_ref, partner_in, out_refs)
    part, gain_grad_ref[...] = norm_back(middle_ref[...], gain_ref[...], normed_grad)
    middle_grad = grad_ref[...] + part
    middle_grad_ref[...] = middle_grad
    out_grad_ref[...] = middle_grad.astype(jnp.bfloat16)
    copies = []
    for spot in (cross, near, far):
        outgoing[spot] = dot_nt(out_grad_ref[...], w_ref[spot]).astype(jnp.bfloat16)
        copies.append(wires.copy(outgoing.at[spot], mixed_grad_ref.at[me], {"seq": spot}))
    mixed_grad_ref[me] = dot_nt(out_grad_ref[...], w_ref[me]).astype(jnp.bfloat16)
    cores, count, parts, rows = weight_ref.shape[:4]
    block = merged_ref.shape[2]
    for at in range(merged_ref.shape[0]):
        weight_grad = dot_tn(merged_ref[at], out_grad_ref[...])
        for inner in range(block // rows):
            index = (at * block + inner * rows) // rows
            dp_at, core_at, part_at = index // (cores * parts), index // parts % cores, index % parts
            weight_ref[core_at, dp_at, part_at] = weight_grad[inner * rows : (inner + 1) * rows].astype(jnp.bfloat16)
    for one in copies:
        one.wait_recv()
    wires.finish()


def input_grad_kernel(spread, qkv_grad_ref, w_ref, x_ref, gain_ref, middle_grad_ref, *rest):
    grad_ref, gain_grad_ref = rest[:2]
    rows_ref = rest[2] if spread else None
    rest = rest[3:] if spread else rest[2:]
    out_refs, (send, recv) = rest[:6], rest[6:]
    place = plane_place()
    me, core, near, far, cross = place
    wires = Wires(send, recv)
    greet(*plane_peers(place)[: 3 if spread else 2])
    totals = []
    run_all(cross_steps(wires, place, lambda spot: dot_nt(qkv_grad_ref[spot], w_ref[...]), out_refs, totals.append))
    normed_grad = totals[0]
    part, gain_grad_ref[...] = norm_back(x_ref[...], gain_ref[...], normed_grad)
    grad = middle_grad_ref[...] + part
    grad_ref[...] = grad
    if spread:
        rows_ref[me, core] = grad.astype(jnp.bfloat16)
        run_all(gather_steps(wires, rows_ref, place, True))
    wires.finish()


def comm_call(kernel, name, number, time, outs, scratch, wire_count, *operands):
    return pl.pallas_call(
        kernel,
        out_shape=tuple(outs),
        in_specs=vmem(len(operands)),
        out_specs=tuple(vmem(len(outs))),
        scratch_shapes=scratch + sems(wire_count),
        compiler_params=pltpu.CompilerParams(collective_id=number, has_side_effects=True),
        cost_estimate=cost(time),
        name=name,
    )(*operands)


def cost(time):
    return pl.CostEstimate(flops=0, bytes_accessed=int(time * 3e6), transcendentals=0)


def low_array(*shape):
    return jax.ShapeDtypeStruct(shape, jnp.bfloat16)


def wide_array(*shape):
    return jax.ShapeDtypeStruct(shape, jnp.float32)


def gelu_parts(values):
    square = values * values
    inner = jnp.tanh(values * (0.7978845608028654 + (0.7978845608028654 * 0.044715) * square))
    lift = 0.5 + 0.5 * inner
    slope = lift + (0.5 * values) * (1.0 - inner * inner) * (0.7978845608028654 + (3.0 * 0.7978845608028654 * 0.044715) * square)
    return values * lift, slope


def slot_hot(slot_row, capacity):
    rows = lax.broadcasted_iota(jnp.int32, (capacity, slot_row.shape[1]), 0)
    return (rows == slot_row).astype(jnp.bfloat16)


def one_of(pair_ref, index):
    values = pair_ref[:, index]
    return values.reshape(values.shape[0] * values.shape[1], values.shape[2])


def experts_kernel(tokens_ref, slot_ref, chosen_ref, own_ref, router_ref, pair_ref, part_ref, slots_ref, pre_ref, shares_ref):
    capacity = slots_ref.shape[0]
    tokens = tokens_ref[...]
    logits = jnp.where(chosen_ref[...] > 0, dot_nt(tokens, router_ref[...]), negative)
    raised = jnp.exp(logits - jnp.max(logits, axis=1, keepdims=True))
    shares = raised / jnp.sum(raised, axis=1, keepdims=True)
    shares_ref[...] = shares
    own_share = jnp.sum(shares * own_ref[...], axis=1, keepdims=True)
    hot = slot_hot(slot_ref[...], capacity)
    slots = dot(hot, tokens).astype(jnp.bfloat16)
    slots_ref[...] = slots
    pre = dot(slots, one_of(pair_ref, 0))
    pre_ref[...] = pre.astype(jnp.bfloat16)
    hidden = gelu_parts(pre)[0].astype(jnp.bfloat16)
    result = dot_nt(hidden, one_of(pair_ref, 1)).astype(jnp.bfloat16)
    part_ref[...] = (own_share * dot_tn(hot, result)).astype(jnp.bfloat16)


class Replay(Wires):
    def __init__(self, send, recv, ref, place, stage):
        super().__init__(send, recv)
        self.stage, self.now = stage, 0
        task = gather_steps(self, ref, place, False)
        for self.now in range(1, stage + 1):
            next(task, None)
        if stage == 5:
            self.finish()

    def copy(self, src, dst, where):
        one = pltpu.make_async_remote_copy(
            src_ref=src, dst_ref=dst, send_sem=self.send.at[self.next], recv_sem=self.recv.at[self.next],
            device_id=where, device_id_type=MESH_ID,
        )
        self.next += 1
        if self.now == self.stage:
            one.start()
        self.started.append(one)
        return Held(one, self)


class Held:
    def __init__(self, one, owner):
        self.one, self.owner = one, owner

    def wait_recv(self):
        if self.owner.now == self.owner.stage or self.owner.stage == 5 and self.owner.now > 2:
            self.one.wait_recv()


def experts_back_kernel(rows_ref, tokens_ref, slot_ref, shares_ref, own_ref, router_ref, pair_ref, slots_ref, pre_ref,
                        *refs):
    group, last = pl.program_id(0), pl.num_programs(0) - 1
    if len(refs) > 6:
        shard_ref, part_ref, pair_grad_ref, router_grad_ref, shared_ref, up_acc, down_acc, landing, send, recv = refs

        @pl.when(group == 0)
        def _():
            place = plane_place()
            greet({"seq": place[2]}, {"seq": place[3]})
            landing[place[0]] = shard_ref[1]
            Replay(send, recv, landing, plane_place(), 1)

        @pl.when(group == 2)
        def _():
            Replay(send, recv, landing, plane_place(), 2)

    else:
        part_ref, pair_grad_ref, router_grad_ref, up_acc, down_acc = refs
        shared_ref = None

    @pl.when(group == 0)
    def _():
        up_acc[...] = jnp.zeros_like(up_acc)
        down_acc[...] = jnp.zeros_like(down_acc)
        router_grad_ref[...] = jnp.zeros_like(router_grad_ref)

    capacity = slots_ref.shape[0]
    shares = shares_ref[...]
    own = own_ref[...]
    own_share = jnp.sum(shares * own, axis=1, keepdims=True)
    hot = slot_hot(slot_ref[...], capacity)
    scaled_rows = (own_share * rows_ref[...].astype(jnp.float32)).astype(jnp.bfloat16)
    result_grad = dot(hot, scaled_rows).astype(jnp.bfloat16)
    hidden_grad = dot(result_grad, one_of(pair_ref, 1))
    hidden, slope = gelu_parts(pre_ref[...].astype(jnp.float32))
    pre_grad = (slope * hidden_grad).astype(jnp.bfloat16)
    pair_sum = jnp.sum(hidden * hidden_grad, axis=1, keepdims=True)
    down_acc[...] += dot_tn(result_grad, hidden.astype(jnp.bfloat16))
    up_acc[...] += dot_tn(slots_ref[...], pre_grad)
    slot_grad = dot_nt(pre_grad, one_of(pair_ref, 0)).astype(jnp.bfloat16)
    high = pair_sum.astype(jnp.bfloat16)
    rest = (pair_sum - high.astype(jnp.float32)).astype(jnp.bfloat16)
    token_pair = dot_tn(hot, jnp.concatenate([jnp.broadcast_to(high, (capacity, 128)), jnp.broadcast_to(rest, (capacity, 128))], axis=1))
    token_pair = token_pair[:, :1] + token_pair[:, 128:129]
    logit_grad = (token_pair * (own - shares)).astype(jnp.bfloat16)
    router_grad_ref[...] += dot_tn(logit_grad, tokens_ref[...])
    part_ref[...] = (dot_tn(hot, slot_grad) + dot(logit_grad, router_ref[...])).astype(jnp.bfloat16)

    @pl.when(group == last)
    def _():
        shape = pair_grad_ref.shape[:1] + pair_grad_ref.shape[2:]
        pair_grad_ref[:, 0] = up_acc[...].astype(jnp.bfloat16).reshape(shape)
        pair_grad_ref[:, 1] = down_acc[...].astype(jnp.bfloat16).reshape(shape)

    if shared_ref is not None:

        @pl.when(group == last)
        def _():
            Replay(send, recv, landing, plane_place(), 5)
            shared_ref[...] = landing[...]


def by_group(*shape):
    return pl.BlockSpec((None,) + shape, lambda g: (g,) + (0,) * len(shape))


def held(*shape):
    return pl.BlockSpec(shape, lambda g: (0,) * len(shape), pipeline_mode=pl.Buffered(1))


def run_experts(tokens, slot, chosen, own, router, pair, capacity):
    groups, rows, width = tokens.shape
    experts, wide_ff = router.shape[0], pair.shape[3]
    return pl.pallas_call(
        experts_kernel,
        grid=(groups,),
        out_shape=(low_array(groups, rows, width), low_array(groups, capacity, width), low_array(groups, capacity, wide_ff),
                   wide_array(groups, rows, experts)),
        in_specs=[by_group(rows, width), by_group(1, rows), by_group(rows, experts), held(1, experts), held(experts, width),
                  held(*pair.shape)],
        out_specs=(by_group(rows, width), by_group(capacity, width), by_group(capacity, wide_ff), by_group(rows, experts)),
        compiler_params=pltpu.CompilerParams(dimension_semantics=("arbitrary",)),
        cost_estimate=cost(14.0),
        name="experts",
    )(tokens, slot, chosen, own, router, pair)


def run_experts_back(rows_grad, tokens, slot, shares, own, router, pair, slots, pre, shard=None):
    groups, rows, width = tokens.shape
    experts, wide_ff = router.shape[0], pair.shape[3]
    capacity = slots.shape[1]
    outs = [low_array(groups, rows, width), low_array(*pair.shape), wide_array(experts, width)]
    out_specs = [by_group(rows, width), held(*pair.shape), held(experts, width)]
    in_specs = [by_group(rows, width), by_group(rows, width), by_group(1, rows), by_group(rows, experts), held(1, experts),
                held(experts, width), held(*pair.shape), by_group(capacity, width), by_group(capacity, wide_ff)]
    scratch = [pltpu.VMEM((width, wide_ff), jnp.float32), pltpu.VMEM((width, wide_ff), jnp.float32)]
    operands = [rows_grad, tokens, slot, shares, own, router, pair, slots, pre]
    options = {}
    if shard is not None:
        operands.append(shard)
        in_specs.append(held(*shard.shape))
        outs.append(low_array(4, *shard.shape[1:]))
        out_specs.append(held(4, *shard.shape[1:]))
        scratch += [pltpu.VMEM((4,) + shard.shape[1:], jnp.bfloat16)] + sems(6)
        options = {"collective_id": 13, "has_side_effects": True}
    return pl.pallas_call(
        experts_back_kernel,
        grid=(groups,),
        out_shape=tuple(outs),
        in_specs=in_specs,
        out_specs=tuple(out_specs),
        scratch_shapes=scratch,
        compiler_params=pltpu.CompilerParams(dimension_semantics=("arbitrary",), **options),
        cost_estimate=cost(25.0),
        name="experts_back" if shard is None else "experts_back_share",
    )(*operands)


def dp_peers():
    me, count = lax.axis_index("dp"), lax.axis_size("dp")
    return me, [lax.rem(me + step, count) for step in range(1, count)], [lax.rem(me + count - step, count) for step in range(1, count)]


def line_start(wires, own_ref, all_ref, core, me, targets):
    half = own_ref.at[core]
    copies = [wires.copy(half, all_ref.at[me, core], {"dp": spot}) for spot in targets]
    all_ref[me] = own_ref[...]
    return copies


def line_forward(wires, all_ref, core, copies, sources):
    onward = []
    for one, spot in zip(copies, sources):
        one.wait_recv()
        block = all_ref.at[spot, core]
        onward.append(wires.copy(block, block, {"tensor": 1 - core}))
    return onward


def weights_kernel(small_ref, whole_ref, outs_ref, small_all, qkv_all, qkv_next, one_piece, two_piece, own_ref, send, recv):
    core, place = lax.axis_index("tensor"), lax.axis_index("seq")
    me, targets, sources = dp_peers()
    wires = Wires(send, recv)
    greet(*[{"dp": spot} for spot in targets], {"tensor": 1 - core})
    smalls = [wires.copy(small_ref, small_all.at[me], {"dp": spot}) for spot in targets]
    small_all[me] = small_ref[...]
    layers, rows, columns = whole_ref.shape
    part, parts = columns // 3, lax.axis_size("seq")
    size = part // parts
    for spot in range(parts):

        @pl.when(place == spot)
        def _():
            for layer, target in enumerate((own_ref, qkv_next)):
                pieces = [whole_ref[layer, :, kind * part + spot * size : kind * part + (spot + 1) * size] for kind in range(3)]
                pieces = jnp.concatenate(pieces, axis=1)
                target[0] = pieces[: rows // 2]
                target[1] = pieces[rows // 2 :]

    qkvs = line_start(wires, own_ref, qkv_all, core, me, targets)
    half = one_piece.shape[-1]
    chosen = pl.ds(pl.multiple_of(core * half, half), half)
    for layer, piece in enumerate((one_piece, two_piece)):
        smalls += [wires.copy(outs_ref.at[layer, place, :, chosen], piece.at[me], {"dp": spot}) for spot in targets]
        piece[me] = outs_ref[layer, place, :, chosen]
    onward = line_forward(wires, qkv_all, core, qkvs, sources)
    for one in smalls + onward:
        one.wait_recv()
    wires.finish()


def reduce_steps(wires, place, line, plane_first, q_ref, o_ref, o_out, scratch):
    me, core, near, far, cross = place
    line_me, targets, sources = line
    q_in, q_sum, q_line, q_out, o_in, o_line, o_sum, o_seq = scratch
    others, partner = (cross, near, far), {"tensor": 1 - core}
    q_first = wires.copy(q_ref.at[1 - core], q_in, partner)
    o_first = wires.copy(o_ref.at[1 - core], o_in, partner)
    yield
    q_first.wait_recv()
    q_sum[...] = (wide(q_ref[core]) + wide(q_in[...])).astype(jnp.bfloat16)
    q_copies = [wires.copy(q_sum.at[spot], q_line.at[line_me], {"dp": spot}) for spot in targets]
    q_line[line_me] = q_sum[line_me]
    o_first.wait_recv()
    o_in[...] = (wide(o_ref[core]) + wide(o_in[...])).astype(jnp.bfloat16)
    if plane_first:
        o_copies = [wires.copy(o_in.at[:, spot], o_seq.at[me], {"seq": spot}) for spot in others]
        o_seq[me] = o_in[:, me]
    else:
        o_copies = [wires.copy(o_in.at[spot], o_line.at[line_me], {"dp": spot}) for spot in targets]
        o_line[line_me] = o_in[line_me]
    yield

    def line_total(ref, copies):
        for one in copies:
            one.wait_recv()
        total = wide(ref[0])
        for spot in range(1, len(targets) + 1):
            total = total + wide(ref[spot])
        return total.astype(jnp.bfloat16)

    def spread(out):
        mine = out.at[core, me]
        return (out, [wires.copy(mine, mine, {"seq": spot}) for spot in others], [wires.copy(mine, mine, partner)])

    def plane_total(copies):
        for one in copies:
            one.wait_recv()
        return (wide(o_seq[0]) + wide(o_seq[1]) + wide(o_seq[2]) + wide(o_seq[3])).astype(jnp.bfloat16)

    if plane_first:
        o_sum[...] = plane_total(o_copies)
        next_copies = [wires.copy(o_sum.at[spot], o_line.at[line_me], {"dp": spot}) for spot in targets]
        o_line[line_me] = o_sum[line_me]
        yield
        q_out[core, me] = line_total(q_line, q_copies)
        last = [spread(q_out)]
        yield
        o_out[core, me] = line_total(o_line, next_copies)
    else:
        q_out[core, me] = line_total(q_line, q_copies)
        last = [spread(q_out)]
        yield
        o_sum[...] = line_total(o_line, o_copies)
        next_copies = [wires.copy(o_sum.at[spot], o_seq.at[me], {"seq": spot}) for spot in others]
        o_seq[me] = o_sum[me]
        yield
        o_out[core, me] = plane_total(next_copies)
    last.append(spread(o_out))
    yield
    for out, copies, onward in last:
        for one, spot in zip(copies, others):
            one.wait_recv()
            block = out.at[core, spot]
            onward.append(wires.copy(block, block, partner))
    yield
    for out, copies, onward in last:
        for one in onward:
            one.wait_recv()


def small_steps(wires, place, line, s_ref, s_out, scratch):
    me, core, near, far, cross = place
    line_me, targets, sources = line
    s_in, s_sum, s_line, s_tot, s_seq = scratch
    partner = {"tensor": 1 - core}
    one = wires.copy(s_ref.at[1 - core], s_in, partner)
    yield
    one.wait_recv()
    s_sum[...] = s_ref[core] + s_in[...]
    copies = [wires.copy(s_sum.at[spot], s_line.at[line_me], {"dp": spot}) for spot in targets]
    s_line[line_me] = s_sum[line_me]
    yield
    for one in copies:
        one.wait_recv()
    s_tot[...] = jnp.sum(s_line[...], axis=0)
    copies = [wires.copy(s_tot, s_seq.at[me], {"seq": spot}) for spot in (cross, near, far)]
    s_seq[me] = s_tot[...]
    yield
    for one in copies:
        one.wait_recv()
    s_out[core] = jnp.sum(s_seq[...], axis=0)
    mine = s_out.at[core]
    one = wires.copy(mine, mine, partner)
    yield
    one.wait_recv()


def finish_kernel(layers, *refs):
    def take(number):
        nonlocal refs
        first, refs = refs[:number], refs[number:]
        return first

    q_refs, o_refs, s_refs, (pair_ref,) = take(layers), take(layers), take(layers), take(1)
    (total_ref,), o_outs, s_outs, share_outs = take(1), take(layers), take(layers), take(2)
    scratch = [take(8) for _ in range(layers)]
    small_scratch = [take(5) for _ in range(layers)]
    place, line = plane_place(), dp_peers()
    me, core, near, far, cross = place
    wires = Wires(*refs)
    greet({"seq": near}, {"seq": far}, {"seq": cross}, {"tensor": 1 - core}, *[{"dp": spot} for spot in line[1]])
    reduces = [reduce_steps(wires, place, line, at > 0, *one) for at, one in enumerate(zip(q_refs, o_refs, o_outs, scratch))]
    smalls = [small_steps(wires, place, line, *one) for one in zip(s_refs, s_outs, small_scratch)]
    for task in reduces + smalls:
        next(task)
    for task in reduces:
        next(task)
    shares = []
    for at, dst in enumerate(share_outs):
        dst[me] = pair_ref[at]
        shares.append(gather_steps(wires, dst, place, False))
        next(shares[at])
    run_all(*reduces, *smalls, *shares)
    rows = total_ref.shape[1] // 2
    for layer in range(layers):
        whole = scratch[layer][3]
        size = whole.shape[-1] // 3
        for half in range(2):
            pieces = [whole[half, spot][:, kind * size : (kind + 1) * size] for kind in range(3) for spot in range(4)]
            total_ref[layer, half * rows : (half + 1) * rows, :] = wide(jnp.concatenate(pieces, axis=1))
    wires.finish()

def body(
    block_input,
    segments,
    routes,
    distance_bucket,
    first_gain,
    query_key_value,
    attention_out,
    bias_table,
    second_gain,
    router_weights,
    expert_up,
    expert_down,
    cotangent,
):
    low = jnp.bfloat16
    seq_count, piece, width = block_input.shape
    n_dp, n_seq, n_tensor = (lax.axis_size(name) for name in ("dp", "seq", "tensor"))
    n_plane = n_seq * n_tensor
    length = piece * n_seq
    local_heads = HEADS // n_seq
    head_width = local_heads * HD
    experts = expert_up.shape[1]
    assert seq_count == 1 and experts == n_seq
    shard = width // n_dp
    bucket_count = bias_table.shape[1] * n_dp
    bucket_shard = bias_table.shape[1]
    group_rows = n_tensor * piece
    capacity = group_rows * routes.shape[-1] // experts
    seq_index = lax.axis_index("seq")
    span = ROWS + length // 2


    assert n_seq == 4 and n_tensor == 2
    half = shard // n_tensor

    def padded(values):
        return jnp.pad(values, ((0, 0), (0, shard - values.shape[1])))

    small = jnp.concatenate(
        [
            first_gain,
            second_gain,
            router_weights.swapaxes(1, 2).reshape(-1, shard),
            padded(bias_table.reshape(LAYERS, -1)),
        ]
    )
    small_rows = small.shape[0]
    small = jnp.pad(small, ((0, -small_rows % 16), (0, 0)))
    own_out = attention_out.reshape(LAYERS, n_seq, shard // n_seq, width)
    own_up = lax.dynamic_index_in_dim(expert_up, seq_index, 1, keepdims=False)
    own_down = lax.dynamic_index_in_dim(expert_down, seq_index, 1, keepdims=False).swapaxes(1, 2)

    own_shape = (n_tensor, half, 3 * head_width)
    small_all, qkv_all, qkv_next, *out_pieces = comm_call(
        weights_kernel, "weights", 10, 22.0,
        [low_array(n_dp, *small.shape), low_array(n_dp, *own_shape), low_array(*own_shape)]
        + [low_array(n_dp, shard // n_seq, width // n_tensor)] * LAYERS,
        [pltpu.VMEM(own_shape, low)], 5 * (n_dp - 1), small, query_key_value, own_out
    )
    qkv_weights = [qkv_all]
    own_pair, small_all = lax.optimization_barrier((jnp.stack([own_up, own_down], axis=1), small_all))
    whole_rows = small_all.swapaxes(0, 1).reshape(-1, width)
    gains = whole_rows[: 2 * LAYERS].astype(jnp.float32).reshape(2, LAYERS, 1, width)
    routers = whole_rows[2 * LAYERS : 2 * LAYERS + LAYERS * experts].reshape(LAYERS, experts, width)
    tables = whole_rows[2 * LAYERS + LAYERS * experts : small_rows].reshape(LAYERS, n_dp, shard)[:, :, : bucket_shard * HEADS]
    tables = tables.reshape(LAYERS, bucket_count, HEADS).astype(jnp.float32)
    own_tables = lax.dynamic_slice_in_dim(tables, seq_index * local_heads, local_heads, 2)
    routes_own = routes.reshape(-1, 128)
    seg_row = segments
    seg_col = segments.reshape(length, 1)
    bucket_line = distance_bucket[length // 2 - 1 :: -1][: length // 2]
    bucket_line = jnp.concatenate(
        [jnp.full((1,), -1, jnp.int32), bucket_line, jnp.full((span - 1 - length // 2,), -1, jnp.int32)]
    )
    line_hot = (bucket_line[None, :] == lax.iota(jnp.int32, bucket_count)[:, None]).astype(jnp.float32)
    lines = jnp.einsum("lbh,bs->lhs", own_tables, line_hot, precision=highest_precision)
    strict_upper = (
        lax.iota(jnp.int32, group_rows)[:, None] < lax.iota(jnp.int32, group_rows)[None, :]
    ).astype(low)

    own_hot = (lax.iota(jnp.int32, experts) == seq_index).astype(jnp.float32)[None]

    current = block_input[0]
    grad = cotangent[0]
    saved = []
    for layer in range(LAYERS):
        pair = lax.all_gather(own_pair[layer], "dp", axis=0)
        gain_one, gain_two = gains[0, layer], gains[1, layer]
        qkv_weight = qkv_weights[layer].reshape(width, 3 * head_width)
        outs = [low_array(n_seq, piece, width), low_array(n_seq, piece, 3 * head_width)]
        if layer == 0:
            outs.append(jax.ShapeDtypeStruct((n_seq,) + routes_own.shape, jnp.int32))
            normed_all, qkv, routes_all = comm_call(
                project_kernel, "project", 1, 16.0, outs, [], 9, current, gain_one, qkv_weight, routes_own
            )
        else:
            current, normed_all, qkv = comm_call(
                sum_project_kernel, "sum_project", 2, 32.0, [wide_array(piece, width)] + outs,
                [pltpu.VMEM((n_seq, piece, width), low)] + sum_scratch(piece, width), 16, part, middle, gain_one, qkv_weight
            )
        qkv = qkv.reshape(length, 3 * head_width)
        if layer == 0:
            outs = [low_array(n_dp, *own_out.shape[1:])] * LAYERS
            mixed, log_total, *out_weights = attend(qkv, seg_row, seg_col, lines[layer], out_pieces, outs, "fetch", 6, 8)
        else:
            outs = [low_array(n_seq, n_tensor, piece, width)]
            mixed, log_total, grad_rows = attend(qkv, seg_row, seg_col, lines[layer], (grad,), outs, "gather", 14, 11)
        out_weight = out_weights[layer].reshape(n_seq, head_width, width)
        fetch = layer == 0
        outs = [low_array(n_seq, piece, head_width), wide_array(piece, width), low_array(n_seq, n_tensor, piece, width)]
        outs += [low_array(n_dp, *own_shape)] if fetch else []
        operands = (mixed.reshape(n_seq, piece, head_width), current, out_weight, gain_two) + ((qkv_next,) if fetch else ())
        merged, middle, tokens, *more = comm_call(
            functools.partial(merge_kernel, fetch), "merge_fetch" if fetch else "merge", 15 if fetch else 3, 25.0, outs, [],
            14 + (2 * (n_dp - 1) if fetch else 0), *operands
        )
        qkv_weights += more
        if layer == 0:
            routes_all, tokens = lax.optimization_barrier((routes_all, tokens))
            routes_all = jnp.moveaxis(routes_all.reshape((n_seq,) + routes.shape), 0, 1).reshape(LAYERS, n_seq, group_rows, -1)
            mine = jnp.any(routes_all == seq_index, axis=-1)
            slot = dot(mine.reshape(-1, group_rows).astype(low), strict_upper).astype(jnp.int32).reshape(mine.shape)
            slot = jnp.where(mine & (slot < capacity), slot, -1)[:, :, None]
            chosen = jnp.any(routes_all[..., None] == lax.iota(jnp.int32, experts), axis=3).astype(jnp.float32)
        tokens = tokens.reshape(n_seq, group_rows, width)
        part, slots, pre, shares = run_experts(tokens, slot[layer], chosen[layer], own_hot, routers[layer], pair, capacity)
        part = part.reshape(n_seq, n_tensor, piece, width)
        saved.append((current, normed_all, qkv, log_total, merged, middle, tokens, shares, slots, pre, qkv_weight, out_weight, pair))

    last_part, last_middle = part, middle

    pair_shards, qkv_grads, out_grads, smalls = ([None] * LAYERS for _ in range(4))
    out_rows = half // n_seq
    for layer in range(LAYERS - 1, -1, -1):
        (layer_in, normed_all, qkv, log_total, merged, middle, tokens, shares, slots, pre, qkv_weight, out_weight, pair) = saved[layer]
        gain_one, gain_two = gains[0, layer], gains[1, layer]
        part, pair_grad, router_grad, *shared = run_experts_back(
            grad_rows.reshape(n_seq, group_rows, width), tokens, slot[layer], shares, own_hot, routers[layer], pair, slots, pre,
            pair_shards[1] if layer == 0 else None
        )
        pair_shards[layer] = lax.psum_scatter(pair_grad, "dp", scatter_dimension=0, tiled=True)[0]
        middle_grad, gain_two_grad, mixed_grad, out_grads[layer] = comm_call(
            split_kernel, "split", 5, 25.0,
            [wide_array(piece, width), wide_array(1, width), low_array(n_seq, piece, head_width),
             low_array(n_tensor, n_dp, n_seq, out_rows, width)],
            [pltpu.VMEM((piece, width), low), pltpu.VMEM((n_seq, piece, head_width), low), pltpu.VMEM((n_seq, piece, width), low)]
            + sum_scratch(piece, width), 13,
            part.reshape(n_seq, n_tensor, piece, width), middle, gain_two, grad, out_weight, merged
        )
        operands = (qkv, seg_row, seg_col, lines[layer], log_total, mixed_grad.reshape(length, head_width))
        operands += (normed_all.reshape(length, width), (n_tensor, n_dp, half, 3 * head_width))
        if layer == 0:
            (down_last,) = shared
            outs = [low_array(n_seq, *pair_shards[1].shape[1:])]
            qkv_grad, band, qkv_grads[layer], up_last = attend_back(*operands, (pair_shards[1],), outs, [], "share", 9, 6)
            input_grad, gain_one_grad = comm_call(
                functools.partial(input_grad_kernel, False), "input_grad_last", 12, 16.0, [wide_array(piece, width), wide_array(1, width)],
                sum_scratch(piece, width), 6, qkv_grad.reshape(n_seq, piece, -1), qkv_weight, layer_in, gain_one, middle_grad
            )
        else:
            outs = [wide_array(piece, width)]
            extra_scratch = [pltpu.VMEM((n_seq, piece, width), low)] + sum_scratch(piece, width)
            qkv_grad, band, qkv_grads[layer], block_output = attend_back(
                *operands, (last_part, last_middle), outs, extra_scratch, "sum", 4, 10
            )
            outs = [wide_array(piece, width), wide_array(1, width), low_array(n_seq, n_tensor, piece, width)]
            grad, gain_one_grad, grad_rows = comm_call(
                functools.partial(input_grad_kernel, True), "input_grad", 7, 32.0, outs, sum_scratch(piece, width), 17,
                qkv_grad.reshape(n_seq, piece, -1), qkv_weight, layer_in, gain_one, middle_grad
            )
        table_grad = jnp.dot(line_hot, band.T, precision=highest_precision)
        table_grad = lax.dynamic_update_slice_in_dim(
            jnp.zeros((bucket_count, HEADS), jnp.float32), table_grad, seq_index * local_heads, 1
        )
        table_grad = padded(table_grad.reshape(n_dp, -1)).reshape(1, width)
        packed = jnp.concatenate([gain_one_grad, gain_two_grad, router_grad, table_grad, jnp.zeros((1, width), jnp.float32)])
        smalls[layer] = packed.reshape(n_tensor, n_seq, n_dp, shard).swapaxes(1, 2)

    def reduce_scratch(plane_first):
        line = pltpu.VMEM((n_dp, half, 3 * head_width), low)
        blocks = pltpu.VMEM((n_dp, n_seq, out_rows, width), low)
        over_dp, over_seq = (pltpu.VMEM((count, out_rows, width), low) for count in (n_dp, n_seq))
        found = [line] * 3 + [pltpu.VMEM((n_tensor, n_seq, half, 3 * head_width), low), blocks]
        if plane_first:
            return found + [over_dp, over_dp, pltpu.VMEM((n_seq, n_dp, out_rows, width), low)]
        return found + [blocks, over_seq, over_seq]

    small_scratch = [pltpu.VMEM((n_dp, n_seq, shard), jnp.float32)] * 3 + [pltpu.VMEM((n_seq, shard), jnp.float32)]
    small_scratch += [pltpu.VMEM((n_seq, n_seq, shard), jnp.float32)]
    qkv_total, *totals = comm_call(
        functools.partial(finish_kernel, LAYERS), "finish", 11, 70.0,
        [wide_array(LAYERS, shard, 3 * width)]
        + [low_array(n_tensor, n_seq, out_rows, width)] * LAYERS + [wide_array(n_tensor, n_seq, shard)] * LAYERS
        + [low_array(n_seq, *pair_shards[0].shape[1:])] * 2,
        reduce_scratch(False) + reduce_scratch(True) + small_scratch * LAYERS,
        LAYERS * (2 * (n_dp - 1) + 19 + n_dp + 4) + 12, *qkv_grads, *out_grads, *smalls, pair_shards[0]
    )
    out_total = jnp.stack(totals[:LAYERS]).astype(jnp.float32).reshape(LAYERS, shard, width)
    small = jnp.stack(totals[LAYERS : 2 * LAYERS]).reshape(LAYERS, n_plane, shard)
    up_first, down_first = totals[2 * LAYERS :]
    router_total = small[:, 2 : 2 + experts].swapaxes(1, 2)
    table_total = small[:, 2 + experts, : bucket_shard * HEADS].reshape(LAYERS, bucket_shard, HEADS)
    up_total = jnp.stack([up_first, up_last]).astype(jnp.float32)
    down_total = jnp.stack([down_first, down_last]).astype(jnp.float32).swapaxes(2, 3)
    return (block_output[None], input_grad[None], small[:, 0], qkv_total, out_total, table_total, small[:, 1], router_total, up_total, down_total)


def solution(mesh):
    in_specs = (
        P(("dp", "tensor"), "seq", None),
        P(("dp", "tensor"), None),
        P(None, "dp", "seq", None),
        P(),
        P(None, "dp"),
        P(None, "dp", None),
        P(None, "dp", None),
        P(None, "dp", None),
        P(None, "dp"),
        P(None, "dp", None),
        P(None, None, "dp", "tensor"),
        P(None, None, "tensor", "dp"),
        P(("dp", "tensor"), "seq", None),
    )
    out_specs = (
        P(("dp", "tensor"), "seq", None),
        P(("dp", "tensor"), "seq", None),
        P(None, "dp"),
        P(None, "dp", None),
        P(None, "dp", None),
        P(None, "dp", None),
        P(None, "dp"),
        P(None, "dp", None),
        P(None, None, "dp", "tensor"),
        P(None, None, "tensor", "dp"),
    )
    return jax.shard_map(body, mesh=mesh, in_specs=in_specs, out_specs=out_specs, check_vma=False)
```
